32 devices in a mesh: graph: 8 (over z, x), mp: 4 (over y, core).
Axes of the slice: x: 2, y: 2, z: 4, core: 2. Of those that a mesh axis runs over, the one named last changes fastest.
Arguments:
- edge_state: bfloat16 [4096, 1536], P('graph', 'mp'), may hold values from -6 to 6
- down_weight: bfloat16 [1536, 384], P('mp'), may hold values from -0.15625 to 0.15625
- basis: float32 [42, 131072], P(None, ('graph', 'mp')), may hold values from -6 to 6
- basis_weight: float32 [42, 384], replicated, may hold values from -1 to 1
- up_weight: bfloat16 [384, 1536], P(None, 'mp'), may hold values from -0.3125 to 0.3125
- dense_weight: bfloat16 [3, 2, 1536, 1536], P(None, None, None, 'mp'), may hold values from -0.15625 to 0.15625
- send_rows: int32 [8, 32, 64], P('graph', 'mp'), may hold values from 0 to 512, as said below
- trip_in: int32 [131072], P(('graph', 'mp')), may hold values from 0 to 511, as said below
- trip_out: int32 [131072], P(('graph', 'mp')), may hold values from 0 to 511, as said below
- trip_live: int32 [131072], P(('graph', 'mp')), may hold values from 0 to 1, as said below
- edge_atom: int32 [4096], P('graph'), may hold values from 0 to 255
Outputs:
- edge_out: bfloat16 [4096, 1536], P('graph', 'mp')
- atom_out: bfloat16 [256, 1536], P('graph', 'mp')
The draws below stay inside these ranges and needn't reach their ends.
Inputs may be any that keep to these rules, and one draw needn't show every extreme that they name: `send_rows`: entry [s, m * 8 + g, c] is a row among the 512 edges of graph index s listed in slot c for the device at graph index g and mp index m, or 512 for an empty slot; used slots come first in each list, and some device has every list full. `trip_in`: A slot s * 64 + c of the triplet's own device whose list entry from graph index s is used. `trip_out`: A slot s * 64 + c of the triplet's own device whose list entry from graph index s is used. `trip_live`: on each device the real triplets come first; some device has no padding.
All inputs are finite; a program needn't handle non-finite values.
Results may differ from the reference program's by a relative error of at most 0.014.
Values may be sent and summed in bfloat16 or wider, within the bound.
A program may use at most 128 MiB of HBM per device.

```python
import jax
import jax.numpy as jnp
from jax import lax

D = 1536
TRIP = 384
NSBF = 42
TILE = 128
LAYERS = 3
EDGE_DEV = 512
CAP = 64
TILES_DEV = 32
EDGES = 4096
ATOMS = 256
TRIPLETS = 131072
N_GRAPH = 8
N_MP = 4


def list_counts(key):
    count_key = jax.random.fold_in(key, 1701)
    counts = jax.random.randint(count_key, (N_GRAPH * N_MP, N_GRAPH), 1, CAP + 1)
    return counts.at[0].set(CAP)


def draw_send_rows(key, part):
    counts = list_counts(key)
    shaped = counts.reshape(N_GRAPH, N_MP, N_GRAPH).transpose(2, 1, 0).reshape(N_GRAPH, N_MP * N_GRAPH)
    start_rows = jax.random.randint(jax.random.fold_in(key, 2203), (N_GRAPH, N_MP * N_GRAPH), 0, EDGE_DEV)
    position = jnp.arange(CAP, dtype=jnp.int32)
    rows = (start_rows[:, :, None] + position) % EDGE_DEV
    return jnp.where(position < shaped[:, :, None], rows, EDGE_DEV).astype(jnp.int32)


def slot_draw(key, salt):
    counts = list_counts(key)
    per_device = TILES_DEV * TILE
    source = jax.random.randint(jax.random.fold_in(key, salt), (N_GRAPH * N_MP, per_device), 0, N_GRAPH)
    raw = jax.random.randint(jax.random.fold_in(key, salt + 1), (N_GRAPH * N_MP, per_device), 0, 1048576)
    limit = jnp.take_along_axis(counts, source, axis=1)
    return (source * CAP + raw % limit).reshape(-1).astype(jnp.int32)


def draw_trip_in(key, part):
    return slot_draw(key, 3301)


def draw_trip_out(key, part):
    return slot_draw(key, 4409)


def draw_trip_live(key, part):
    per_device = TILES_DEV * TILE
    live_count = jax.random.randint(jax.random.fold_in(key, 5507), (N_GRAPH * N_MP,), per_device // 4, per_device + 1)
    live_count = live_count.at[0].set(per_device)
    position = jnp.arange(per_device, dtype=jnp.int32)
    return (position[None, :] < live_count[:, None]).reshape(-1).astype(jnp.int32)


def place_ends(result, stream_key, smallest, largest):
    shape = result.shape
    place = [jax.random.randint(jax.random.fold_in(stream_key, axis), (), 0, shape[axis]) for axis in range(len(shape))]
    result = result.at[tuple(place)].set(smallest)
    longest = shape.index(max(shape))
    place[longest] = (place[longest] + 1) % shape[longest]
    return result.at[tuple(place)].set(largest)


def levels(key, shape, split, smallest, high):
    def one(dim, blocks):
        draws = jax.random.uniform(jax.random.fold_in(jax.random.fold_in(key, 6), dim), (blocks,), jnp.float32, smallest / len(split), high / len(split))
        return jnp.repeat(jnp.exp(draws), shape[dim] // blocks).reshape((-1,) + (1,) * (len(shape) - dim - 1))

    loudness = one(*split[0])
    for cut in split[1:]:
        loudness = loudness * one(*cut)
    return loudness


def normal_values(key, shape, deviation, most, pieces=(), kind=jnp.bfloat16):
    factor_of = levels(key, shape, pieces, -0.22, 0.18) if pieces else 1.0
    entries = jax.random.normal(key, shape, jnp.float32) * deviation * factor_of
    return jnp.minimum(jnp.maximum(entries, -most), most).astype(kind)


def setup_inputs(seed: int = 0) -> dict:
    streams_of = jax.random.split(jax.random.key(seed), 12)
    edge_state = normal_values(streams_of[0], (EDGES, D), 1.0, 6.0, ((0, 8), (1, 4)))
    down_weight = normal_values(streams_of[1], (D, TRIP), D ** -0.5, 0.15625, ((0, 4),))
    basis = normal_values(streams_of[2], (NSBF, TRIPLETS), 1.0, 6.0, ((1, 32),), jnp.float32)
    basis_weight = normal_values(streams_of[3], (NSBF, TRIP), NSBF ** -0.5, 1.0, (), jnp.float32)
    up_weight = normal_values(streams_of[4], (TRIP, D), TRIP ** -0.5, 0.3125, ((1, 4),))
    dense_weight = normal_values(streams_of[5], (LAYERS, 2, D, D), D ** -0.5, 0.15625, ((3, 4),))
    send_rows = draw_send_rows(jax.random.fold_in(streams_of[11], 71), 0)
    trip_in = draw_trip_in(jax.random.fold_in(streams_of[11], 71), 0)
    trip_out = draw_trip_out(jax.random.fold_in(streams_of[11], 71), 0)
    trip_live = draw_trip_live(jax.random.fold_in(streams_of[11], 71), 0)
    edge_atom = place_ends(jax.random.randint(streams_of[10], (EDGES,), 0, ATOMS), jax.random.fold_in(streams_of[10], 1), 0, ATOMS - 1).astype(jnp.int32)
    return {"edge_state": edge_state, "down_weight": down_weight, "basis": basis, "basis_weight": basis_weight, "up_weight": up_weight, "dense_weight": dense_weight, "send_rows": send_rows, "trip_in": trip_in, "trip_out": trip_out, "trip_live": trip_live, "edge_atom": edge_atom}


inv_root_two = 0.7071067811865476
atom_scale = 0.2


def reference(edge_state, down_weight, basis, basis_weight, up_weight, dense_weight, send_rows, trip_in, trip_out, trip_live, edge_atom):
    projected = jnp.dot(edge_state, down_weight, preferred_element_type=jnp.float32).astype(jnp.bfloat16)
    per_device = TILES_DEV * TILE
    slot_count = N_GRAPH * CAP
    sources = (jnp.arange(N_GRAPH, dtype=jnp.int32) * EDGE_DEV)[:, None]

    def visit(carry, device):
        graph_index = device // N_MP
        mp_index = device % N_MP
        row_lists = lax.dynamic_index_in_dim(send_rows, (mp_index * N_GRAPH + graph_index).astype(jnp.int32), 1, keepdims=False)
        valid_flat = (row_lists < EDGE_DEV).reshape(-1)
        global_rows = (sources + jnp.minimum(row_lists, EDGE_DEV - 1)).reshape(-1).astype(jnp.int32)
        received = jnp.where(valid_flat[:, None], jnp.take(projected, global_rows, axis=0), jnp.zeros((), jnp.bfloat16))
        offset = (device * per_device).astype(jnp.int32)
        basis_part = lax.dynamic_slice_in_dim(basis, offset, per_device, 1)
        in_part = lax.dynamic_slice_in_dim(trip_in, offset, per_device, 0)
        out_part = lax.dynamic_slice_in_dim(trip_out, offset, per_device, 0)
        live_part = lax.dynamic_slice_in_dim(trip_live, offset, per_device, 0)
        angle_coef = lax.dot_general(basis_part, basis_weight, (((0,), (0,)), ((), ())), precision=lax.Precision.HIGHEST, preferred_element_type=jnp.float32)
        trip_values = jnp.take(received, in_part, axis=0).astype(jnp.float32) * angle_coef * live_part[:, None].astype(jnp.float32)
        slot_sums = jax.ops.segment_sum(trip_values, out_part, num_segments=slot_count).astype(jnp.bfloat16)
        contrib = jnp.where(valid_flat[:, None], slot_sums.astype(jnp.float32), jnp.zeros((), jnp.float32))
        carry = carry.at[global_rows].add(contrib)
        return carry, None

    edge_update, _ = lax.scan(visit, jnp.zeros((EDGES, TRIP), jnp.float32), jnp.arange(N_GRAPH * N_MP, dtype=jnp.int32))
    update_rows = edge_update.astype(jnp.bfloat16)
    hidden = edge_state.astype(jnp.float32) + jnp.dot(update_rows, up_weight, preferred_element_type=jnp.float32)
    for layer_index in range(LAYERS):
        inner = jax.nn.silu(jnp.dot(hidden.astype(jnp.bfloat16), dense_weight[layer_index, 0], preferred_element_type=jnp.float32)).astype(jnp.bfloat16)
        outer = jax.nn.silu(jnp.dot(inner, dense_weight[layer_index, 1], preferred_element_type=jnp.float32))
        hidden = (hidden + outer) * inv_root_two
    atom_sum = jax.ops.segment_sum(hidden, edge_atom, num_segments=ATOMS)
    atom_out = jax.nn.silu(atom_scale * atom_sum).astype(jnp.bfloat16)
    edge_out = (hidden + jnp.take(atom_out, edge_atom, axis=0).astype(jnp.float32)).astype(jnp.bfloat16)
    return (edge_out, atom_out)
```

```python
import functools

import jax
import jax.numpy as jnp
from jax import lax
from jax.experimental import pallas as pl
from jax.experimental.pallas import tpu as pltpu
from jax.sharding import PartitionSpec as P

ATOM_DEV = 32
CHUNKS = 4

inv_root_two = 0.7071067811865476
atom_scale = 0.2

MESH = pl.DeviceIdType.MESH
bf16 = jnp.bfloat16
f32 = jnp.float32


def scope(name):
    return jax.named_scope(name)


def silu(v):
    return v / (1.0 + jnp.exp(-v))


def flip(index, bit):
    return index + bit - 2 * bit * ((index // bit) % 2)


def one_hot(rows, ids):
    shape = (rows, ids.shape[1])
    return jnp.where(lax.broadcasted_iota(jnp.int32, shape, 0) == ids, 1.0, 0.0).astype(bf16)


def dot(a, b, ca=1, cb=0):
    return lax.dot_general(a, b, (((ca,), (cb,)), ((), ())), preferred_element_type=f32)


def halves(v):
    high = v.astype(bf16)
    return high, (v - high.astype(f32)).astype(bf16)


def gather_plan(mp):
    plan, held, bit = [], [0], mp // 2
    while bit >= 1:
        plan += [(bit, off) for off in held]
        held += [bit ^ off for off in held]
        bit //= 2
    return plan, held


def kernel(
    graph, mp, tile,
    state_hbm, down_hbm, basis_hbm, bw_hbm, up_hbm, dense_hbm, lists_hbm, in_hbm, out_hbm, live_hbm, atom_hbm,
    edge_out_ref, atom_out_ref,
    state_ref, down_ref, basis_ref, bw_ref, up_ref, lists_ref, in_ref, out_ref, live_ref, atom_ref, load_sem,
    weight, weight_sem,
    part_a, got_a, sum_a, more_a, full_a,
    part_b, got_b, sum_b, more_b, full_b,
    red_send, red_recv,
    to_a, from_a, to_b, from_b, xc_send, xc_recv,
    list_hot, basis_stack, bw_stack, angle, slots, in_hot, out_hot,
    acts, hidden, act_send, act_recv,
    atoms_own, atoms_to, atoms_from, table,
):
    g = lax.axis_index("graph")
    m = lax.axis_index("mp")
    rows, width = state_ref.shape
    trip = down_ref.shape[1]
    layers = weight.shape[0] // 2
    cap = lists_ref.shape[2]
    slot_total = graph * cap
    pieces, lane = to_a.shape[0], to_a.shape[2]
    kept = in_hot is not None
    triplets = in_ref.shape[1]
    atoms = graph * ATOM_DEV
    half = rows // 2
    bits = [1 << i for i in range(mp.bit_length() - 1)]
    stages = len(bits)
    size = rows // CHUNKS

    barrier = pltpu.get_barrier_semaphore()

    def greet(k, _):
        pl.semaphore_signal(barrier, inc=1, device_id={"graph": (g + k) % graph}, device_id_type=MESH)
        return 0

    lax.fori_loop(1, graph, greet, 0)
    for bit in bits:
        pl.semaphore_signal(barrier, inc=1, device_id={"mp": flip(m, bit)}, device_id_type=MESH)

    hbm = [state_hbm, down_hbm, lists_hbm, in_hbm, out_hbm, live_hbm, basis_hbm, bw_hbm, up_hbm, atom_hbm]
    here_refs = [state_ref, down_ref, lists_ref, in_ref, out_ref, live_ref, basis_ref, bw_ref, up_ref, atom_ref]
    loads = [pltpu.make_async_copy(a, b, load_sem.at[i]) for i, (a, b) in enumerate(zip(hbm, here_refs))]
    for load in loads:
        load.start()
    state_in, down_in, lists_in, in_in, out_in, live_in, basis_in, bw_in, up_in, atom_in = loads

    def mp_copy(src, dst, which, j, stage, bit):
        return pltpu.make_async_remote_copy(
            src_ref=src, dst_ref=dst, send_sem=red_send.at[which, j, stage], recv_sem=red_recv.at[which, j, stage],
            device_id={"mp": flip(m, bit)}, device_id_type=MESH)

    mine = pl.ds(pl.multiple_of((m % 2) * half, half), half)
    other = pl.ds(pl.multiple_of(half - (m % 2) * half, half), half)

    class Sum:
        def __init__(self, which, part, got, summed, more, full):
            self.which, self.part, self.got = which, part, got
            self.summed, self.more, self.full = summed, more, full

        def first(self, j):
            return mp_copy(self.part.at[j, other], self.got.at[j], self.which, j, 0, 1)

        def step(self, j, b):
            return mp_copy(self.summed.at[j, b], self.more.at[j, b], self.which, j, 1 + b, bits[1 + b])

        def last(self, j):
            at = self.full.at[j, mine]
            return mp_copy(at, at, self.which, j, stages, 1)

        def into(self, j):
            self.first(j).start()

        def across(self, j):
            self.first(j).wait_recv()
            total = self.part[j, mine].astype(f32) + self.got[j].astype(f32)
            if stages > 1:
                self.summed[j, 0] = total.astype(bf16)
                self.step(j, 0).start()
            else:
                self.full[j, mine] = total.astype(bf16)

        def home(self, j):
            for b in range(stages - 1):
                self.step(j, b).wait_recv()
                total = self.summed[j, b].astype(f32) + self.more[j, b].astype(f32)
                if b + 2 < stages:
                    self.summed[j, b + 1] = total.astype(bf16)
                    self.step(j, b + 1).start()
                else:
                    self.full[j, mine] = total.astype(bf16)
            self.last(j).start()

        def done(self, j):
            self.last(j).wait_recv()

        def drain(self):
            for j in range(pieces):
                self.first(j).wait_send()
                for b in range(stages - 1):
                    self.step(j, b).wait_send()
                self.last(j).wait_send()

    sum0 = Sum(0, part_a, got_a, sum_a, more_a, full_a)
    sum1 = Sum(1, part_b, got_b, sum_b, more_b, full_b)

    def exchange(which, src_at, dst_at, whole):
        def copy(k):
            peer = (g + k) % graph
            return pltpu.make_async_remote_copy(
                src_ref=src_at(peer), dst_ref=dst_at(g), send_sem=xc_send.at[which], recv_sem=xc_recv.at[which],
                device_id={"graph": peer}, device_id_type=MESH)

        def start(k, _):
            copy(k).start()
            return 0

        total = pltpu.make_async_remote_copy(
            src_ref=whole, dst_ref=whole, send_sem=xc_send.at[which], recv_sem=xc_recv.at[which],
            device_id={"graph": (g + 1) % graph}, device_id_type=MESH)
        return (lambda: lax.fori_loop(1, graph, start, 0)), total.wait_recv, total.wait_send

    def block(ref, size):
        return lambda i: ref.at[pl.ds(pl.multiple_of(i * size, size), size)]

    def piece(ref, j, size):
        return lambda i: ref.at[j, pl.ds(pl.multiple_of(i * size, size), size)]

    def tiles(step):
        def one(i, _):
            step(pl.ds(pl.multiple_of(i * tile, tile), tile))
            return 0

        lax.fori_loop(0, triplets // tile, one, 0)

    def in_part(at):
        return one_hot(slot_total, in_ref[:, at])

    def out_part(at):
        return one_hot(slot_total, jnp.where(live_ref[:, at] > 0, out_ref[:, at], -1))

    state_in.wait()
    down_in.wait()
    with scope("s_proj"):
        projected = dot(state_ref[...], down_ref[...]).astype(bf16)
        for j in range(pieces):
            part_a[j] = projected[:, j * lane:(j + 1) * lane]
    with scope("s_barrier"):
        pl.semaphore_wait(barrier, graph - 1 + len(bits))
    for j in range(pieces):
        sum0.into(j)
    load = pltpu.make_async_copy(dense_hbm, weight, weight_sem)
    load.start()

    lists_in.wait()
    with scope("s_hots"):
        for i in range(graph):
            list_hot[:, i * cap:(i + 1) * cap] = one_hot(rows, lists_ref[0, i:i + 1, :])
        in_in.wait()
        if kept:
            def keep_in(at):
                in_hot[:, at] = in_part(at)

            tiles(keep_in)
    with scope("s_across"):
        for j in range(pieces):
            sum0.across(j)
    out_in.wait()
    live_in.wait()
    if kept:
        def keep_out(at):
            out_hot[:, at] = out_part(at)

        with scope("s_outhot"):
            tiles(keep_out)

    basis_in.wait()
    bw_in.wait()
    depth = basis_ref.shape[0]
    pad = basis_stack.shape[0] // 3
    with scope("s_angles"):
        bw_high, bw_low = halves(bw_ref[...])
        bw_stack[...] = jnp.zeros_like(bw_stack)
        bw_stack[0:depth] = bw_high
        bw_stack[pad:pad + depth] = bw_high
        bw_stack[2 * pad:2 * pad + depth] = bw_low

        def angles(at):
            high, low = halves(basis_ref[:, at])
            basis_stack[:, at] = jnp.zeros((3 * pad, tile), bf16)
            basis_stack[0:depth, at] = high
            basis_stack[pad:pad + depth, at] = low
            basis_stack[2 * pad:2 * pad + depth, at] = high
            angle[:, at] = dot(bw_stack[...], basis_stack[:, at], 0, 0)

        tiles(angles)

    step_rows = min(slot_total, 512)
    own = pl.ds(pl.multiple_of(g * cap, cap), cap)
    span = pl.ds(0, slot_total - cap)
    going = [exchange(j, piece(to_a, j, cap), piece(from_a, j, cap), from_a.at[j, span]) for j in range(pieces)]
    back = [exchange(pieces + j, piece(to_b, j, cap), piece(from_b, j, cap), from_b.at[j, span])
            for j in range(pieces)]

    def pick_piece(j):
        def pick(i, _):
            at = pl.ds(pl.multiple_of(i * step_rows, step_rows), step_rows)
            to_a[j, at, :] = dot(list_hot[:, at], full_a[j], 0, 0).astype(bf16)
            return 0

        sum0.done(j)
        lax.fori_loop(0, slot_total // step_rows, pick, 0)
        going[j][0]()
        from_a[j, own] = to_a[j, own]

    with scope("s_home"):
        sum0.home(0)
    with scope("s_home1"):
        for j in range(1, pieces):
            sum0.home(j)
            pick_piece(j - 1)
        pick_piece(pieces - 1)
    sum0.drain()

    for j in range(pieces):
        with scope("s_gowait%d" % j):
            going[j][1]()
        slots[...] = jnp.zeros_like(slots)
        received = from_a[j].astype(f32).T.astype(bf16)

        def trips(at):
            source = in_hot[:, at] if kept else in_part(at)
            value = dot(received, source) * angle[j * lane:(j + 1) * lane, at]
            target = out_hot[:, at] if kept else out_part(at)
            slots[...] += dot(target, value.astype(bf16), 1, 1)

        with scope("s_trips%d" % j):
            tiles(trips)
        to_b[j] = slots[...].astype(bf16)
        back[j][0]()
        from_b[j, own] = to_b[j, own]

    up_in.wait()

    def add_up(j):
        rest = dot(full_b[j], up_ref[j * lane:(j + 1) * lane, :])
        hidden[...] = (state_ref[...].astype(f32) if j == 0 else hidden[...]) + rest

    for j in range(pieces):
        with scope("s_backwait%d" % j):
            back[j][1]()
        part_b[j] = dot(list_hot[...], from_b[j]).astype(bf16)
        sum1.into(j)
        if j + 1 < pieces:
            sum1.across(j)
    with scope("s_sum1"):
        if pieces > 1:
            sum1.home(0)
        sum1.across(pieces - 1)
        for j in range(1 if pieces > 1 else 0, pieces):
            sum1.home(j)
            if j >= 1:
                sum1.done(j - 1)
                add_up(j - 1)
        sum1.done(pieces - 1)

    plan, held = gather_plan(mp)
    order = [h * (CHUNKS // 2) + i for i in range(CHUNKS // 2) for h in (0, 1)]

    def other_of(off):
        index = m
        for bit in bits:
            if off & bit:
                index = flip(index, bit)
        return index

    def act_copy(layer, parity, c, which):
        bit, off = plan[which]
        at = acts.at[layer, other_of(off), pl.ds(c * size, size)]
        return pltpu.make_async_remote_copy(
            src_ref=at, dst_ref=at,
            send_sem=act_send.at[parity, c, which], recv_sem=act_recv.at[parity, c, which],
            device_id={"mp": flip(m, bit)}, device_id_type=MESH)

    local = [i for i, (bit, off) in enumerate(plan) if off == 0]
    relayed = [i for i, (bit, off) in enumerate(plan) if off != 0]
    brings = {bit ^ off: i for i, (bit, off) in enumerate(plan)}
    relays_from = sorted({brings[plan[i][1]] for i in relayed})

    def send(layer, parity, c):
        for i in local:
            act_copy(layer, parity, c, i).start()

    def relay(layer, parity, c):
        for i in relayed:
            first = brings[plan[i][1]]
            if [j for j in relayed if brings[plan[j][1]] == first][0] == i:
                act_copy(layer, parity, c, first).wait_recv()
            act_copy(layer, parity, c, i).start()

    def finish(layer, parity, c):
        for i in range(len(plan)):
            if i not in relays_from:
                act_copy(layer, parity, c, i).wait_recv()

    def sent(layer, parity, c):
        for i in range(len(plan)):
            act_copy(layer, parity, c, i).wait_send()

    last_up = (pieces - 1) * lane
    with scope("s_begin"):
        for c in order:
            at = pl.ds(c * size, size)
            before = hidden[at, :] if pieces > 1 else state_ref[at, :].astype(f32)
            first = before + dot(full_b[pieces - 1, at], up_ref[last_up:last_up + lane, :])
            hidden[at, :] = first
            acts[0, m, at, :] = first.astype(bf16)
            send(0, 0, c)
        sum1.drain()
        load.wait()
        for j in range(pieces):
            going[j][2]()
            back[j][2]()
    with scope("s_relay0"):
        relay(0, 0, order[0])

    def layer_step(l, _):
        for inside in range(2):
            k = 2 * l + inside
            for spot, c in enumerate(order):
                at = pl.ds(c * size, size)
                if spot + 1 < CHUNKS:
                    relay(k, inside, order[spot + 1])
                elif inside == 0:
                    relay(k + 1, 1, order[0])
                else:
                    @pl.when(l + 1 < layers)
                    def _():
                        relay(k + 1, 0, order[0])
                finish(k, inside, c)
                total = None
                for off in held:
                    index = other_of(off)
                    term = dot(acts[k, index, at, :], weight[k, pl.ds(pl.multiple_of(index * width, width), width), :])
                    total = term if total is None else total + term
                value = silu(total)
                if inside == 0:
                    @pl.when(l > 0)
                    def _():
                        sent(k - 1, 1, c)

                    acts[k + 1, m, at, :] = value.astype(bf16)
                    send(k + 1, 1, c)
                else:
                    value = (hidden[at, :] + value) * inv_root_two
                    hidden[at, :] = value

                    @pl.when(l + 1 < layers)
                    def _():
                        sent(k - 1, 0, c)
                        acts[k + 1, m, at, :] = value.astype(bf16)
                        send(k + 1, 0, c)
        return 0

    with scope("s_layers"):
        lax.fori_loop(0, layers, layer_step, 0)

    atom_in.wait()
    atom_rows = min(atoms, 256)

    def collect(i, _):
        at = pl.ds(pl.multiple_of(i * atom_rows, atom_rows), atom_rows)
        ids = one_hot(atom_rows, atom_ref[...] - i * atom_rows)
        high, low = halves(hidden[...])
        total = dot(ids, high) + dot(ids, low)
        atoms_own[at, :] = total
        atoms_to[at, :] = total.astype(bf16)
        return 0

    with scope("s_collect"):
        lax.fori_loop(0, atoms // atom_rows, collect, 0)
    atom_span = pl.ds(0, atoms - ATOM_DEV)
    start, wait, wait_sent = exchange(
        2 * pieces, block(atoms_to, ATOM_DEV), block(atoms_from, ATOM_DEV), atoms_from.at[atom_span])
    start()
    here = pl.ds(pl.multiple_of(g * ATOM_DEV, ATOM_DEV), ATOM_DEV)
    atoms_from[here] = jnp.zeros((ATOM_DEV, width), bf16)
    for c in range(CHUNKS):
        sent(2 * layers - 2, 0, c)
        sent(2 * layers - 1, 1, c)
    with scope("s_atomwait"):
        wait()

    def add(i, total):
        return total + atoms_from[pl.ds(pl.multiple_of(i * ATOM_DEV, ATOM_DEV), ATOM_DEV)].astype(f32)

    total = lax.fori_loop(0, graph, add, atoms_own[here])
    mine_out = silu(atom_scale * total).astype(bf16)
    table[here] = mine_out
    start2, wait2, wait_sent2 = exchange(
        2 * pieces + 1, lambda peer: block(table, ATOM_DEV)(g), block(table, ATOM_DEV), table.at[atom_span])
    start2()
    atom_out_ref[...] = mine_out
    wait_sent()
    with scope("s_atomwait2"):
        wait2()

    def spread(i, _):
        at = pl.ds(pl.multiple_of(i * atom_rows, atom_rows), atom_rows)
        hidden[...] += dot(one_hot(atom_rows, atom_ref[...] - i * atom_rows), table[at, :], 0, 0)
        return 0

    with scope("s_spread"):
        lax.fori_loop(0, atoms // atom_rows, spread, 0)
        edge_out_ref[...] = hidden[...].astype(bf16)
    wait_sent2()


def hand_on(edge_ref, atom_ref, edge_out_ref, atom_out_ref):
    edge_out_ref[...] = edge_ref[...]
    atom_out_ref[...] = atom_ref[...]


def local(graph, mp, edge_state, down_weight, basis, basis_weight, up_weight, dense_weight,
          send_rows, trip_in, trip_out, trip_live, edge_atom):
    rows, width = edge_state.shape
    trip = down_weight.shape[1]
    slot_total = graph * send_rows.shape[2]
    triplets = trip_in.shape[0]
    maps = dense_weight.shape[0] * dense_weight.shape[1]
    tile = 2048 if slot_total <= 512 else 128
    atoms = graph * ATOM_DEV
    stages = mp.bit_length()
    extra = max(stages - 2, 1)
    half = rows // 2
    vmem = pltpu.VMEM
    pieces = trip // 128 if trip % 128 == 0 else 1
    lane = trip // pieces
    pad = -(-basis.shape[0] // 16) * 16
    hot_bytes = 2 * 2 * slot_total * triplets
    hots = [vmem((slot_total, triplets), bf16)] * 2 if hot_bytes <= 2 ** 24 else [None, None]
    reduce_bufs = [
        vmem((pieces, rows, lane), bf16), vmem((pieces, half, lane), bf16), vmem((pieces, extra, half, lane), bf16),
        vmem((pieces, extra, half, lane), bf16), vmem((pieces, rows, lane), bf16),
    ]
    dma = pltpu.SemaphoreType.DMA
    spec = pl.BlockSpec(memory_space=pltpu.VMEM)
    operands = [
        edge_state, down_weight, basis, basis_weight, up_weight,
        dense_weight.reshape((maps,) + dense_weight.shape[2:]),
        send_rows, trip_in.reshape(1, triplets), trip_out.reshape(1, triplets),
        trip_live.reshape(1, triplets), edge_atom.reshape(1, rows),
    ]
    inputs = [vmem(a.shape, a.dtype) for i, a in enumerate(operands) if i != 5]
    body = functools.partial(kernel, graph, mp, tile)
    before = [
        *inputs, dma((len(inputs),)),
        vmem((maps,) + dense_weight.shape[2:], bf16), dma(()),
        *reduce_bufs, *reduce_bufs,
        dma((2, pieces, stages)), dma((2, pieces, stages)),
        *[vmem((pieces, slot_total, lane), bf16)] * 4,
        dma((2 * pieces + 2,)), dma((2 * pieces + 2,)),
        vmem((rows, slot_total), bf16), vmem((3 * pad, triplets), bf16), vmem((3 * pad, trip), bf16),
        vmem((trip, triplets), f32), vmem((slot_total, lane), f32),
    ]
    if hots[0] is None:
        hots, kept_body, at = [], body, len(operands) + 2 + len(before)
        body = lambda *refs: kept_body(*refs[:at], None, None, *refs[at:])
    outs = pl.pallas_call(
        body,
        out_shape=(
            jax.ShapeDtypeStruct((rows, width), bf16),
            jax.ShapeDtypeStruct((ATOM_DEV, width), bf16),
        ),
        in_specs=[pl.BlockSpec(memory_space=pl.ANY)] * len(operands),
        out_specs=(spec, spec),
        scratch_shapes=[
            *before, *hots,
            vmem((maps, mp, rows, width), bf16), vmem((rows, width), f32),
            dma((2, CHUNKS, mp - 1)), dma((2, CHUNKS, mp - 1)),
            vmem((atoms, width), f32), vmem((atoms, width), bf16), vmem((atoms, width), bf16),
            vmem((atoms, width), bf16),
        ],
        compiler_params=pltpu.CompilerParams(
            collective_id=0, has_side_effects=True, vmem_limit_bytes=64000 * 1024
        ),
        name="edge_block",
    )(*operands)
    return pl.pallas_call(
        hand_on,
        out_shape=tuple(jax.ShapeDtypeStruct(o.shape, o.dtype) for o in outs),
        in_specs=[spec] * 2,
        out_specs=(spec, spec),
        name="hand_on",
    )(*outs)


def solution(mesh):
    in_specs = (
        P("graph", "mp"),
        P("mp", None),
        P(None, ("graph", "mp")),
        P(),
        P(None, "mp"),
        P(None, None, None, "mp"),
        P("graph", "mp", None),
        P(("graph", "mp")),
        P(("graph", "mp")),
        P(("graph", "mp")),
        P("graph"),
    )
    out_specs = (P("graph", "mp"), P("graph", "mp"))
    body = functools.partial(local, mesh.shape["graph"], mesh.shape["mp"])
    return jax.shard_map(body, mesh=mesh, in_specs=in_specs, out_specs=out_specs, check_vma=False)
```

```python
import functools

import jax
import jax.numpy as jnp
from jax import lax
from jax.experimental import pallas as pl
from jax.experimental.pallas import tpu as pltpu
from jax.sharding import PartitionSpec as P

ATOM_DEV = 32
CHUNKS = 4

inv_root_two = 0.7071067811865476
atom_scale = 0.2

MESH = pl.DeviceIdType.MESH
bf16 = jnp.bfloat16
f32 = jnp.float32


def scope(name):
    return jax.named_scope(name)


def silu(v):
    return v / (1.0 + jnp.exp(-v))


def flip(index, bit):
    return index + bit - 2 * bit * ((index // bit) % 2)


def one_hot(rows, ids):
    shape = (rows, ids.shape[1])
    return jnp.where(lax.broadcasted_iota(jnp.int32, shape, 0) == ids, 1.0, 0.0).astype(bf16)


def dot(a, b, ca=1, cb=0):
    return lax.dot_general(a, b, (((ca,), (cb,)), ((), ())), preferred_element_type=f32)


def halves(v):
    high = v.astype(bf16)
    return high, (v - high.astype(f32)).astype(bf16)


def gather_plan(mp):
    plan, held, bit = [], [0], mp // 2
    while bit >= 1:
        plan += [(bit, off) for off in held]
        held += [bit ^ off for off in held]
        bit //= 2
    return plan, held


def kernel(
    graph, mp, tile,
    state_hbm, down_hbm, basis_hbm, bw_hbm, up_hbm, dense_hbm, lists_hbm, in_hbm, out_hbm, live_hbm, atom_hbm,
    edge_out_ref, atom_out_ref,
    down_ref, basis_ref, bw_ref, lists_ref, in_ref, out_ref, live_ref, atom_ref, load_sem,
    states, ups, early_send, early_recv,
    weight, weight_sem,
    part_a, got_a, sum_a, more_a, full_a,
    part_b, got_b, sum_b, more_b, full_b,
    red_send, red_recv,
    to_a, from_a, to_b, from_b, xc_send, xc_recv,
    list_hot, basis_stack, bw_stack, angle, slots, in_hot, out_hot,
    acts, partial, hidden, act_send, act_recv,
    atoms_own, atoms_to, atoms_from, table,
):
    g = lax.axis_index("graph")
    m = lax.axis_index("mp")
    rows, width = hidden.shape
    trip = down_ref.shape[1]
    layers = weight.shape[0] // 2
    cap = lists_ref.shape[2]
    slot_total = graph * cap
    pieces, lane = to_a.shape[0], to_a.shape[2]
    kept = in_hot is not None
    triplets = in_ref.shape[1]
    atoms = graph * ATOM_DEV
    half = rows // 2
    bits = [1 << i for i in range(mp.bit_length() - 1)]
    stages = len(bits)
    size = rows // CHUNKS

    barrier = pltpu.get_barrier_semaphore()

    def greet(k, _):
        pl.semaphore_signal(barrier, inc=1, device_id={"graph": (g + k) % graph}, device_id_type=MESH)
        return 0

    lax.fori_loop(1, graph, greet, 0)
    for bit in bits:
        pl.semaphore_signal(barrier, inc=1, device_id={"mp": flip(m, bit)}, device_id_type=MESH)

    hbm = [state_hbm, down_hbm, lists_hbm, in_hbm, out_hbm, live_hbm, basis_hbm, bw_hbm, up_hbm, atom_hbm]
    here_refs = [
        states.at[m], down_ref, lists_ref, in_ref, out_ref, live_ref, basis_ref, bw_ref, ups.at[m], atom_ref]
    loads = [pltpu.make_async_copy(a, b, load_sem.at[i]) for i, (a, b) in enumerate(zip(hbm, here_refs))]
    for load in loads:
        load.start()
    state_in, down_in, lists_in, in_in, out_in, live_in, basis_in, bw_in, up_in, atom_in = loads

    def mp_copy(src, dst, which, j, stage, bit):
        return pltpu.make_async_remote_copy(
            src_ref=src, dst_ref=dst, send_sem=red_send.at[which, j, stage], recv_sem=red_recv.at[which, j, stage],
            device_id={"mp": flip(m, bit)}, device_id_type=MESH)

    mine = pl.ds(pl.multiple_of((m % 2) * half, half), half)
    other = pl.ds(pl.multiple_of(half - (m % 2) * half, half), half)

    plan, held = gather_plan(mp)

    def other_of(off):
        index = m
        for bit in bits:
            if off & bit:
                index = flip(index, bit)
        return index

    local = [i for i, (bit, off) in enumerate(plan) if off == 0]
    relayed = [i for i, (bit, off) in enumerate(plan) if off != 0]
    brings = {bit ^ off: i for i, (bit, off) in enumerate(plan)}
    relays_from = sorted({brings[plan[i][1]] for i in relayed})

    def early(which, i):
        bit, off = plan[i]
        at = (states, ups)[which].at[other_of(off)]
        return pltpu.make_async_remote_copy(
            src_ref=at, dst_ref=at, send_sem=early_send.at[which, i], recv_sem=early_recv.at[which, i],
            device_id={"mp": flip(m, bit)}, device_id_type=MESH)

    def early_relay(which):
        for i in relayed:
            first = brings[plan[i][1]]
            if [j for j in relayed if brings[plan[j][1]] == first][0] == i:
                early(which, first).wait_recv()
            early(which, i).start()

    def early_finish(which):
        for i in range(len(plan)):
            if i not in relays_from:
                early(which, i).wait_recv()

    class Sum:
        def __init__(self, which, part, got, summed, more, full):
            self.which, self.part, self.got = which, part, got
            self.summed, self.more, self.full = summed, more, full

        def first(self, j):
            return mp_copy(self.part.at[j, other], self.got.at[j], self.which, j, 0, 1)

        def step(self, j, b):
            return mp_copy(self.summed.at[j, b], self.more.at[j, b], self.which, j, 1 + b, bits[1 + b])

        def last(self, j):
            at = self.full.at[j, mine]
            return mp_copy(at, at, self.which, j, stages, 1)

        def into(self, j):
            self.first(j).start()

        def across(self, j):
            self.first(j).wait_recv()
            total = self.part[j, mine].astype(f32) + self.got[j].astype(f32)
            if stages > 1:
                self.summed[j, 0] = total.astype(bf16)
                self.step(j, 0).start()
            else:
                self.full[j, mine] = total.astype(bf16)

        def home(self, j):
            for b in range(stages - 1):
                self.step(j, b).wait_recv()
                total = self.summed[j, b].astype(f32) + self.more[j, b].astype(f32)
                if b + 2 < stages:
                    self.summed[j, b + 1] = total.astype(bf16)
                    self.step(j, b + 1).start()
                else:
                    self.full[j, mine] = total.astype(bf16)
            self.last(j).start()

        def done(self, j):
            self.last(j).wait_recv()

        def drain(self):
            for j in range(pieces):
                self.first(j).wait_send()
                for b in range(stages - 1):
                    self.step(j, b).wait_send()
                self.last(j).wait_send()

    sum0 = Sum(0, part_a, got_a, sum_a, more_a, full_a)
    sum1 = Sum(1, part_b, got_b, sum_b, more_b, full_b)

    def exchange(which, src_at, dst_at, whole):
        def copy(k):
            peer = (g + k) % graph
            return pltpu.make_async_remote_copy(
                src_ref=src_at(peer), dst_ref=dst_at(g), send_sem=xc_send.at[which], recv_sem=xc_recv.at[which],
                device_id={"graph": peer}, device_id_type=MESH)

        def start(k, _):
            copy(k).start()
            return 0

        total = pltpu.make_async_remote_copy(
            src_ref=whole, dst_ref=whole, send_sem=xc_send.at[which], recv_sem=xc_recv.at[which],
            device_id={"graph": (g + 1) % graph}, device_id_type=MESH)
        return (lambda: lax.fori_loop(1, graph, start, 0)), total.wait_recv, total.wait_send

    def block(ref, size):
        return lambda i: ref.at[pl.ds(pl.multiple_of(i * size, size), size)]

    def piece(ref, j, size):
        return lambda i: ref.at[j, pl.ds(pl.multiple_of(i * size, size), size)]

    def tiles(step):
        def one(i, _):
            step(pl.ds(pl.multiple_of(i * tile, tile), tile))
            return 0

        lax.fori_loop(0, triplets // tile, one, 0)

    def in_part(at):
        return one_hot(slot_total, in_ref[:, at])

    def out_part(at):
        return one_hot(slot_total, jnp.where(live_ref[:, at] > 0, out_ref[:, at], -1))

    state_in.wait()
    down_in.wait()
    with scope("s_proj"):
        projected = dot(states[m], down_ref[...]).astype(bf16)
        for j in range(pieces):
            part_a[j] = projected[:, j * lane:(j + 1) * lane]
    with scope("s_barrier"):
        pl.semaphore_wait(barrier, graph - 1 + len(bits))
    for j in range(pieces):
        sum0.into(j)
    load = pltpu.make_async_copy(dense_hbm, weight, weight_sem)
    load.start()

    lists_in.wait()
    with scope("s_hots"):
        for i in range(graph):
            list_hot[:, i * cap:(i + 1) * cap] = one_hot(rows, lists_ref[0, i:i + 1, :])
        in_in.wait()
        if kept:
            def keep_in(at):
                in_hot[:, at] = in_part(at)

            tiles(keep_in)
    with scope("s_across"):
        for j in range(pieces):
            sum0.across(j)
    up_in.wait()
    for which in range(2):
        for i in local[:1]:
            early(which, i).start()
    out_in.wait()
    live_in.wait()
    if kept:
        def keep_out(at):
            out_hot[:, at] = out_part(at)

        with scope("s_outhot"):
            tiles(keep_out)

    basis_in.wait()
    bw_in.wait()
    depth = basis_ref.shape[0]
    pad = basis_stack.shape[0] // 3
    with scope("s_angles"):
        bw_high, bw_low = halves(bw_ref[...])
        bw_stack[...] = jnp.zeros_like(bw_stack)
        bw_stack[0:depth] = bw_high
        bw_stack[pad:pad + depth] = bw_high
        bw_stack[2 * pad:2 * pad + depth] = bw_low

        def angles(at):
            high, low = halves(basis_ref[:, at])
            basis_stack[:, at] = jnp.zeros((3 * pad, tile), bf16)
            basis_stack[0:depth, at] = high
            basis_stack[pad:pad + depth, at] = low
            basis_stack[2 * pad:2 * pad + depth, at] = high
            angle[:, at] = dot(bw_stack[...], basis_stack[:, at], 0, 0)

        tiles(angles)

    step_rows = min(slot_total, 512)
    own = pl.ds(pl.multiple_of(g * cap, cap), cap)
    span = pl.ds(0, slot_total - cap)
    going = [exchange(j, piece(to_a, j, cap), piece(from_a, j, cap), from_a.at[j, span]) for j in range(pieces)]
    back = [exchange(pieces + j, piece(to_b, j, cap), piece(from_b, j, cap), from_b.at[j, span])
            for j in range(pieces)]

    def pick_piece(j):
        def pick(i, _):
            at = pl.ds(pl.multiple_of(i * step_rows, step_rows), step_rows)
            to_a[j, at, :] = dot(list_hot[:, at], full_a[j], 0, 0).astype(bf16)
            return 0

        sum0.done(j)
        lax.fori_loop(0, slot_total // step_rows, pick, 0)
        going[j][0]()
        from_a[j, own] = to_a[j, own]

    with scope("s_home"):
        sum0.home(0)
    with scope("s_home1"):
        for j in range(1, pieces):
            sum0.home(j)
            pick_piece(j - 1)
        pick_piece(pieces - 1)
    for which in range(2):
        for i in local[1:]:
            early(which, i).start()
    sum0.drain()

    for j in range(pieces):
        with scope("s_gowait%d" % j):
            going[j][1]()
        slots[...] = jnp.zeros_like(slots)
        received = from_a[j].astype(f32).T.astype(bf16)

        def trips(at):
            source = in_hot[:, at] if kept else in_part(at)
            value = dot(received, source) * angle[j * lane:(j + 1) * lane, at]
            target = out_hot[:, at] if kept else out_part(at)
            slots[...] += dot(target, value.astype(bf16), 1, 1)

        with scope("s_trips%d" % j):
            tiles(trips)
        to_b[j] = slots[...].astype(bf16)
        back[j][0]()
        from_b[j, own] = to_b[j, own]
    with scope("s_early0"):
        early_relay(0)

    def add_up(j):
        for index in range(mp):
            rest = dot(full_b[j], ups[index, j * lane:(j + 1) * lane, :])
            partial[index] = (states[index].astype(f32) if j == 0 else partial[index]) + rest

    for j in range(pieces):
        with scope("s_backwait%d" % j):
            back[j][1]()
        part_b[j] = dot(list_hot[...], from_b[j]).astype(bf16)
        sum1.into(j)
        if j == 0:
            with scope("s_early1"):
                early_relay(1)
        if j + 1 < pieces:
            sum1.across(j)
    with scope("s_sum1"):
        if pieces > 1:
            sum1.home(0)
        sum1.across(pieces - 1)
        early_finish(0)
        early_finish(1)
        for j in range(1 if pieces > 1 else 0, pieces):
            sum1.home(j)
            if j >= 1:
                sum1.done(j - 1)
                add_up(j - 1)
        sum1.done(pieces - 1)

    order = [h * (CHUNKS // 2) + i for i in range(CHUNKS // 2) for h in (0, 1)]

    def act_copy(layer, parity, c, which):
        bit, off = plan[which]
        at = acts.at[layer, other_of(off), pl.ds(c * size, size)]
        return pltpu.make_async_remote_copy(
            src_ref=at, dst_ref=at,
            send_sem=act_send.at[parity, c, which], recv_sem=act_recv.at[parity, c, which],
            device_id={"mp": flip(m, bit)}, device_id_type=MESH)

    def send(layer, parity, c):
        for i in local:
            act_copy(layer, parity, c, i).start()

    def relay(layer, parity, c):
        for i in relayed:
            first = brings[plan[i][1]]
            if [j for j in relayed if brings[plan[j][1]] == first][0] == i:
                act_copy(layer, parity, c, first).wait_recv()
            act_copy(layer, parity, c, i).start()

    def finish(layer, parity, c):
        for i in range(len(plan)):
            if i not in relays_from:
                act_copy(layer, parity, c, i).wait_recv()

    def sent(layer, parity, c):
        for i in range(len(plan)):
            act_copy(layer, parity, c, i).wait_send()

    def product(k, at):
        total = None
        for off in held:
            index = other_of(off)
            term = dot(acts[k, index, at, :], weight[k, pl.ds(pl.multiple_of(index * width, width), width), :])
            total = term if total is None else total + term
        return silu(total)

    last_up = (pieces - 1) * lane
    load.wait()
    with scope("s_begin"):
        for c in order:
            at = pl.ds(c * size, size)
            for index in range(mp):
                before = partial[index, at] if pieces > 1 else states[index, at].astype(f32)
                first = before + dot(full_b[pieces - 1, at], ups[index, last_up:last_up + lane, :])
                partial[index, at] = first
                acts[0, index, at, :] = first.astype(bf16)
            hidden[at, :] = partial[m, at]
            acts[1, m, at, :] = product(0, at).astype(bf16)
            send(1, 1, c)
        sum1.drain()
        for j in range(pieces):
            going[j][2]()
            back[j][2]()
        for which in range(2):
            for i in range(len(plan)):
                early(which, i).wait_send()
    with scope("s_relay1"):
        relay(1, 1, order[0])

    def half_step(l, inside, first):
        k = 2 * l + inside
        for spot, c in enumerate(order):
            at = pl.ds(c * size, size)
            if spot + 1 < CHUNKS:
                relay(k, inside, order[spot + 1])
            elif inside == 0:
                relay(k + 1, 1, order[0])
            elif not first or layers > 1:
                @pl.when(l + 1 < layers)
                def _():
                    relay(k + 1, 0, order[0])
            finish(k, inside, c)
            value = product(k, at)
            if inside == 0:
                sent(k - 1, 1, c)
                acts[k + 1, m, at, :] = value.astype(bf16)
                send(k + 1, 1, c)
            else:
                value = (hidden[at, :] + value) * inv_root_two
                hidden[at, :] = value

                @pl.when(l + 1 < layers)
                def _():
                    if not first:
                        sent(k - 1, 0, c)
                    acts[k + 1, m, at, :] = value.astype(bf16)
                    send(k + 1, 0, c)

    def layer_step(l, _):
        half_step(l, 0, False)
        half_step(l, 1, False)
        return 0

    with scope("s_layers"):
        half_step(0, 1, True)
        lax.fori_loop(1, layers, layer_step, 0)

    atom_in.wait()
    atom_rows = min(atoms, 256)
    parts, part_lane = table.shape[0], table.shape[2]
    here = pl.ds(pl.multiple_of(g * ATOM_DEV, ATOM_DEV), ATOM_DEV)
    atom_span = pl.ds(0, atoms - ATOM_DEV)
    gathers = [exchange(2 * pieces + p, piece(atoms_to, p, ATOM_DEV), piece(atoms_from, p, ATOM_DEV),
                        atoms_from.at[p, atom_span]) for p in range(parts)]
    spreads = [exchange(2 * pieces + parts + p, lambda peer, p=p: piece(table, p, ATOM_DEV)(g),
                        piece(table, p, ATOM_DEV), table.at[p, atom_span]) for p in range(parts)]

    def columns(p):
        return slice(p * part_lane, (p + 1) * part_lane)

    with scope("s_collect"):
        for p in range(parts):
            def collect(i, _):
                at = pl.ds(pl.multiple_of(i * atom_rows, atom_rows), atom_rows)
                ids = one_hot(atom_rows, atom_ref[...] - i * atom_rows)
                high, low = halves(hidden[:, columns(p)])
                total = dot(ids, high) + dot(ids, low)
                atoms_own[p, at] = total
                atoms_to[p, at] = total.astype(bf16)
                return 0

            lax.fori_loop(0, atoms // atom_rows, collect, 0)
            gathers[p][0]()
    for p in range(parts):
        atoms_from[p, here] = jnp.zeros((ATOM_DEV, part_lane), bf16)
    for c in range(CHUNKS):
        if layers > 1:
            sent(2 * layers - 2, 0, c)
        sent(2 * layers - 1, 1, c)
    for p in range(parts):
        with scope("s_atomwait%d" % p):
            gathers[p][1]()

        def add(i, total):
            return total + atoms_from[p, pl.ds(pl.multiple_of(i * ATOM_DEV, ATOM_DEV), ATOM_DEV)].astype(f32)

        total = lax.fori_loop(0, graph, add, atoms_own[p, here])
        mine_out = silu(atom_scale * total).astype(bf16)
        table[p, here] = mine_out
        spreads[p][0]()
        atom_out_ref[:, columns(p)] = mine_out
    for p in range(parts):
        gathers[p][2]()
    for p in range(parts):
        with scope("s_spreadwait%d" % p):
            spreads[p][1]()

        def spread(i, total):
            at = pl.ds(pl.multiple_of(i * atom_rows, atom_rows), atom_rows)
            return total + dot(one_hot(atom_rows, atom_ref[...] - i * atom_rows), table[p, at], 0, 0)

        total = lax.fori_loop(0, atoms // atom_rows, spread, hidden[:, columns(p)])
        edge_out_ref[:, columns(p)] = total.astype(bf16)
    for p in range(parts):
        spreads[p][2]()


def hand_on(edge_ref, atom_ref, edge_out_ref, atom_out_ref, sem):
    edge = pltpu.make_async_copy(edge_ref, edge_out_ref, sem.at[0])
    atom = pltpu.make_async_copy(atom_ref, atom_out_ref, sem.at[1])
    edge.start()
    atom.start()
    edge.wait()
    atom.wait()


def local(graph, mp, edge_state, down_weight, basis, basis_weight, up_weight, dense_weight,
          send_rows, trip_in, trip_out, trip_live, edge_atom):
    rows, width = edge_state.shape
    trip = down_weight.shape[1]
    slot_total = graph * send_rows.shape[2]
    triplets = trip_in.shape[0]
    maps = dense_weight.shape[0] * dense_weight.shape[1]
    tile = 2048 if slot_total <= 512 else 128
    atoms = graph * ATOM_DEV
    stages = mp.bit_length()
    extra = max(stages - 2, 1)
    half = rows // 2
    vmem = pltpu.VMEM
    pieces = trip // 128 if trip % 128 == 0 else 1
    lane = trip // pieces
    pad = -(-basis.shape[0] // 16) * 16
    hot_bytes = 2 * 2 * slot_total * triplets
    hots = [vmem((slot_total, triplets), bf16)] * 2 if hot_bytes <= 2 ** 24 else [None, None]
    reduce_bufs = [
        vmem((pieces, rows, lane), bf16), vmem((pieces, half, lane), bf16), vmem((pieces, extra, half, lane), bf16),
        vmem((pieces, extra, half, lane), bf16), vmem((pieces, rows, lane), bf16),
    ]
    dma = pltpu.SemaphoreType.DMA
    spec = pl.BlockSpec(memory_space=pltpu.VMEM)
    operands = [
        edge_state, down_weight, basis, basis_weight, up_weight,
        dense_weight.reshape((maps,) + dense_weight.shape[2:]),
        send_rows, trip_in.reshape(1, triplets), trip_out.reshape(1, triplets),
        trip_live.reshape(1, triplets), edge_atom.reshape(1, rows),
    ]
    inputs = [vmem(a.shape, a.dtype) for i, a in enumerate(operands) if i not in (0, 4, 5)]
    parts = width // 128 if width % 128 == 0 else 1
    atom_buf = (parts, atoms, width // parts)
    body = functools.partial(kernel, graph, mp, tile)
    before = [
        *inputs, dma((len(inputs) + 2,)),
        vmem((mp, rows, width), bf16), vmem((mp, trip, width), bf16), dma((2, mp - 1)), dma((2, mp - 1)),
        vmem((maps,) + dense_weight.shape[2:], bf16), dma(()),
        *reduce_bufs, *reduce_bufs,
        dma((2, pieces, stages)), dma((2, pieces, stages)),
        *[vmem((pieces, slot_total, lane), bf16)] * 4,
        dma((2 * pieces + 2 * parts,)), dma((2 * pieces + 2 * parts,)),
        vmem((rows, slot_total), bf16), vmem((3 * pad, triplets), bf16), vmem((3 * pad, trip), bf16),
        vmem((trip, triplets), f32), vmem((slot_total, lane), f32),
    ]
    if hots[0] is None:
        hots, kept_body, at = [], body, len(operands) + 2 + len(before)
        body = lambda *refs: kept_body(*refs[:at], None, None, *refs[at:])
    outs = pl.pallas_call(
        body,
        out_shape=(
            pltpu.VMEM((rows, width), bf16),
            pltpu.VMEM((ATOM_DEV, width), bf16),
        ),
        in_specs=[pl.BlockSpec(memory_space=pl.ANY)] * len(operands),
        out_specs=(spec, spec),
        scratch_shapes=[
            *before, *hots,
            vmem((maps, mp, rows, width), bf16), vmem((mp, rows, width), f32), vmem((rows, width), f32),
            dma((2, CHUNKS, mp - 1)), dma((2, CHUNKS, mp - 1)),
            vmem(atom_buf, f32), vmem(atom_buf, bf16), vmem(atom_buf, bf16), vmem(atom_buf, bf16),
        ],
        compiler_params=pltpu.CompilerParams(
            collective_id=0, has_side_effects=True, vmem_limit_bytes=64000 * 1024
        ),
        name="edge_block",
    )(*operands)
    outs = [pltpu.with_memory_space_constraint(o, pltpu.VMEM) for o in outs]
    return pl.pallas_call(
        hand_on,
        out_shape=tuple(jax.ShapeDtypeStruct(o.shape, o.dtype) for o in outs),
        in_specs=[spec] * 2,
        out_specs=[pl.BlockSpec(memory_space=pl.ANY)] * 2,
        scratch_shapes=[dma((2,))],
        name="hand_on",
    )(*outs)


def solution(mesh):
    in_specs = (
        P("graph", "mp"),
        P("mp", None),
        P(None, ("graph", "mp")),
        P(),
        P(None, "mp"),
        P(None, None, None, "mp"),
        P("graph", "mp", None),
        P(("graph", "mp")),
        P(("graph", "mp")),
        P(("graph", "mp")),
        P("graph"),
    )
    out_specs = (P("graph", "mp"), P("graph", "mp"))
    body = functools.partial(local, mesh.shape["graph"], mesh.shape["mp"])
    return jax.shard_map(body, mesh=mesh, in_specs=in_specs, out_specs=out_specs, check_vma=False)
```

```python
import functools

import jax
import jax.numpy as jnp
from jax import lax
from jax.experimental import pallas as pl
from jax.experimental.pallas import tpu as pltpu
from jax.sharding import PartitionSpec as P

ATOM_DEV = 32

inv_root_two = 0.7071067811865476
atom_scale = 0.2

MESH = pl.DeviceIdType.MESH
bf16 = jnp.bfloat16
f32 = jnp.float32


def scope(name):
    return jax.named_scope(name)


def silu(v):
    return v / (1.0 + jnp.exp(-v))


def flip(index, bit):
    return index + bit - 2 * bit * ((index // bit) % 2)


def one_hot(rows, ids):
    shape = (rows, ids.shape[1])
    return jnp.where(lax.broadcasted_iota(jnp.int32, shape, 0) == ids, 1.0, 0.0).astype(bf16)


def dot(a, b, ca=1, cb=0):
    return lax.dot_general(a, b, (((ca,), (cb,)), ((), ())), preferred_element_type=f32)


def halves(v):
    high = v.astype(bf16)
    return high, (v - high.astype(f32)).astype(bf16)


def chunks_of(half):
    quarter = half // 4
    return (0, quarter, 3 * quarter), (quarter, 2 * quarter, quarter)


def gather_plan(mp):
    plan, held, bit = [], [0], mp // 2
    while bit >= 1:
        plan += [(bit, off) for off in held]
        held += [bit ^ off for off in held]
        bit //= 2
    return plan, held


def kernel(
    graph, mp, tile,
    state_hbm, down_hbm, basis_hbm, bw_hbm, up_hbm, dense_hbm, lists_hbm, in_hbm, out_hbm, live_hbm, atom_hbm,
    edge_out_ref, atom_out_ref,
    down_ref, basis_ref, bw_ref, lists_ref, in_ref, out_ref, live_ref, atom_ref, load_sem,
    states, ups, early_send, early_recv,
    weight, weight_sem,
    part_a, got_a, sum_a, more_a, full_a,
    part_b, got_b, sum_b, more_b, full_b,
    red_send, red_recv,
    to_a, from_a, to_b, from_b, xc_send, xc_recv,
    list_hot, basis_stack, bw_stack, angle, slots, in_hot, out_hot,
    acts, partial, hidden, act_send, act_recv,
    atoms_own, atoms_to, atoms_from, table,
):
    g = lax.axis_index("graph")
    m = lax.axis_index("mp")
    rows, width = hidden.shape
    trip = down_ref.shape[1]
    layers = weight.shape[0] // 2
    cap = lists_ref.shape[2]
    slot_total = graph * cap
    pieces, lane = to_a.shape[0], to_a.shape[2]
    kept = in_hot is not None
    triplets = in_ref.shape[1]
    atoms = graph * ATOM_DEV
    half = rows // 2
    bits = [1 << i for i in range(mp.bit_length() - 1)]
    stages = len(bits)

    barrier = pltpu.get_barrier_semaphore()

    def greet(k, _):
        pl.semaphore_signal(barrier, inc=1, device_id={"graph": (g + k) % graph}, device_id_type=MESH)
        return 0

    lax.fori_loop(1, graph, greet, 0)
    for bit in bits:
        pl.semaphore_signal(barrier, inc=1, device_id={"mp": flip(m, bit)}, device_id_type=MESH)

    hbm = [state_hbm, down_hbm, lists_hbm, in_hbm, out_hbm, live_hbm, basis_hbm, bw_hbm, up_hbm, atom_hbm]
    here_refs = [
        states.at[m], down_ref, lists_ref, in_ref, out_ref, live_ref, basis_ref, bw_ref, ups.at[m], atom_ref]
    loads = [pltpu.make_async_copy(a, b, load_sem.at[i]) for i, (a, b) in enumerate(zip(hbm, here_refs))]
    for load in loads:
        load.start()
    state_in, down_in, lists_in, in_in, out_in, live_in, basis_in, bw_in, up_in, atom_in = loads

    def mp_copy(src, dst, which, j, stage, bit):
        return pltpu.make_async_remote_copy(
            src_ref=src, dst_ref=dst, send_sem=red_send.at[which, stage], recv_sem=red_recv.at[which, j, stage],
            device_id={"mp": flip(m, bit)}, device_id_type=MESH)

    mine = pl.ds(pl.multiple_of((m % 2) * half, half), half)
    other = pl.ds(pl.multiple_of(half - (m % 2) * half, half), half)

    plan, held = gather_plan(mp)

    def other_of(off):
        index = m
        for bit in bits:
            if off & bit:
                index = flip(index, bit)
        return index

    local = [i for i, (bit, off) in enumerate(plan) if off == 0]
    relayed = [i for i, (bit, off) in enumerate(plan) if off != 0]
    brings = {bit ^ off: i for i, (bit, off) in enumerate(plan)}
    relays_from = sorted({brings[plan[i][1]] for i in relayed})

    def early(which, i):
        bit, off = plan[i]
        at = (states, ups)[which].at[other_of(off)]
        return pltpu.make_async_remote_copy(
            src_ref=at, dst_ref=at, send_sem=early_send.at[which], recv_sem=early_recv.at[which, i],
            device_id={"mp": flip(m, bit)}, device_id_type=MESH)

    def early_sent(which):
        at = (states, ups)[which].at[pl.ds(0, mp - 1)]
        pltpu.make_async_remote_copy(
            src_ref=at, dst_ref=at, send_sem=early_send.at[which], recv_sem=early_recv.at[which, 0],
            device_id={"mp": flip(m, 1)}, device_id_type=MESH).wait_send()

    def early_relay(which):
        for i in relayed:
            first = brings[plan[i][1]]
            if [j for j in relayed if brings[plan[j][1]] == first][0] == i:
                early(which, first).wait_recv()
            early(which, i).start()

    def early_finish(which):
        for i in range(len(plan)):
            if i not in relays_from:
                early(which, i).wait_recv()

    class Sum:
        def __init__(self, which, part, got, summed, more, full):
            self.which, self.part, self.got = which, part, got
            self.summed, self.more, self.full = summed, more, full

        def first(self, j):
            return mp_copy(self.part.at[j, other], self.got.at[j], self.which, j, 0, 1)

        def step(self, j, b):
            return mp_copy(self.summed.at[j, b], self.more.at[j, b], self.which, j, 1 + b, bits[1 + b])

        def last(self, j):
            at = self.full.at[j, mine]
            return mp_copy(at, at, self.which, j, stages, 1)

        def into(self, j):
            self.first(j).start()

        def across(self, j):
            self.first(j).wait_recv()
            total = self.part[j, mine].astype(f32) + self.got[j].astype(f32)
            if stages > 1:
                self.summed[j, 0] = total.astype(bf16)
                self.step(j, 0).start()
            else:
                self.full[j, mine] = total.astype(bf16)

        def home(self, j):
            for b in range(stages - 1):
                self.step(j, b).wait_recv()
                total = self.summed[j, b].astype(f32) + self.more[j, b].astype(f32)
                if b + 2 < stages:
                    self.summed[j, b + 1] = total.astype(bf16)
                    self.step(j, b + 1).start()
                else:
                    self.full[j, mine] = total.astype(bf16)
            self.last(j).start()

        def done(self, j):
            self.last(j).wait_recv()

        def drain(self):
            for stage in range(stages + 1):
                mp_copy(self.got, self.got, self.which, 0, stage, 1).wait_send()

    sum0 = Sum(0, part_a, got_a, sum_a, more_a, full_a)
    sum1 = Sum(1, part_b, got_b, sum_b, more_b, full_b)

    def peer_of(k):
        if graph & (graph - 1):
            return (g + k) % graph
        return sum(bit * ((g // bit + k // bit) % 2) for bit in (1 << i for i in range(graph.bit_length() - 1)))

    peers = [peer_of(k) for k in range(graph - 1, 0, -1)] if graph <= 8 else None

    def arrived(whole, group, which):
        return pltpu.make_async_remote_copy(
            src_ref=whole, dst_ref=whole, send_sem=xc_send.at[group], recv_sem=xc_recv.at[which],
            device_id={"graph": (g + 1) % graph}, device_id_type=MESH)

    def exchange(group, which, src_at, dst_at, whole):
        def to(peer):
            pltpu.make_async_remote_copy(
                src_ref=src_at(peer), dst_ref=dst_at(g), send_sem=xc_send.at[group], recv_sem=xc_recv.at[which],
                device_id={"graph": peer}, device_id_type=MESH).start()

        def one(i, _):
            to(peer_of(graph - 1 - i))
            return 0

        def start():
            if peers is None:
                lax.fori_loop(0, graph - 1, one, 0)
            else:
                for peer in peers:
                    to(peer)

        return start, arrived(whole, group, which).wait_recv

    def block(ref, size):
        return lambda i: ref.at[pl.ds(pl.multiple_of(i * size, size), size)]

    def piece(ref, j, size):
        return lambda i: ref.at[j, pl.ds(pl.multiple_of(i * size, size), size)]

    def tiles(step):
        def one(i, _):
            step(pl.ds(pl.multiple_of(i * tile, tile), tile))
            return 0

        lax.fori_loop(0, triplets // tile, one, 0)

    def in_part(at):
        return one_hot(slot_total, in_ref[:, at])

    def out_part(at):
        return one_hot(slot_total, jnp.where(live_ref[:, at] > 0, out_ref[:, at], -1))

    state_in.wait()
    down_in.wait()
    with scope("s_proj"):
        projected = dot(states[m], down_ref[...]).astype(bf16)
        for j in range(pieces):
            part_a[j] = projected[:, j * lane:(j + 1) * lane]
    with scope("s_barrier"):
        pl.semaphore_wait(barrier, graph - 1 + len(bits))
    for j in range(pieces):
        sum0.into(j)
    load = pltpu.make_async_copy(dense_hbm, weight, weight_sem)
    load.start()

    lists_in.wait()
    with scope("s_hots"):
        for i in range(graph):
            list_hot[:, i * cap:(i + 1) * cap] = one_hot(rows, lists_ref[0, i:i + 1, :])
        in_in.wait()
        if kept:
            def keep_in(at):
                in_hot[:, at] = in_part(at)

            tiles(keep_in)
    with scope("s_across"):
        for j in range(pieces):
            sum0.across(j)
    up_in.wait()
    for which in range(2):
        for i in local[:1]:
            early(which, i).start()
    out_in.wait()
    live_in.wait()
    if kept:
        def keep_out(at):
            out_hot[:, at] = out_part(at)

        with scope("s_outhot"):
            tiles(keep_out)

    basis_in.wait()
    bw_in.wait()
    depth = basis_ref.shape[0]
    pad = basis_stack.shape[0] // 3
    with scope("s_angles"):
        bw_high, bw_low = halves(bw_ref[...])
        bw_stack[...] = jnp.zeros_like(bw_stack)
        bw_stack[0:depth] = bw_high
        bw_stack[pad:pad + depth] = bw_high
        bw_stack[2 * pad:2 * pad + depth] = bw_low

        def angles(at):
            high, low = halves(basis_ref[:, at])
            basis_stack[:, at] = jnp.zeros((3 * pad, tile), bf16)
            basis_stack[0:depth, at] = high
            basis_stack[pad:pad + depth, at] = low
            basis_stack[2 * pad:2 * pad + depth, at] = high
            angle[:, at] = dot(bw_stack[...], basis_stack[:, at], 0, 0)

        tiles(angles)

    step_rows = min(slot_total, 512)
    own = pl.ds(pl.multiple_of(g * cap, cap), cap)
    span = pl.ds(0, slot_total - cap)
    going = [exchange(0, j, piece(to_a, j, cap), piece(from_a, j, cap), from_a.at[j, span]) for j in range(pieces)]
    back = [exchange(1, pieces + j, piece(to_b, j, cap), piece(from_b, j, cap), from_b.at[j, span])
            for j in range(pieces)]

    def pick_piece(j):
        def pick(i, _):
            at = pl.ds(pl.multiple_of(i * step_rows, step_rows), step_rows)
            to_a[j, at, :] = dot(list_hot[:, at], full_a[j], 0, 0).astype(bf16)
            return 0

        sum0.done(j)
        lax.fori_loop(0, slot_total // step_rows, pick, 0)
        going[j][0]()
        from_a[j, own] = to_a[j, own]

    with scope("s_home"):
        sum0.home(0)
    with scope("s_home1"):
        for j in range(1, pieces):
            sum0.home(j)
            pick_piece(j - 1)
        pick_piece(pieces - 1)
    for which in range(2):
        for i in local[1:]:
            early(which, i).start()
    sum0.drain()

    for j in range(pieces):
        with scope("s_gowait%d" % j):
            going[j][1]()
        slots[...] = jnp.zeros_like(slots)
        received = from_a[j].astype(f32).T.astype(bf16)

        def trips(at):
            source = in_hot[:, at] if kept else in_part(at)
            value = dot(received, source) * angle[j * lane:(j + 1) * lane, at]
            target = out_hot[:, at] if kept else out_part(at)
            slots[...] += dot(target, value.astype(bf16), 1, 1)

        with scope("s_trips%d" % j):
            tiles(trips)
        to_b[j] = slots[...].astype(bf16)
        back[j][0]()
        from_b[j, own] = to_b[j, own]
    with scope("s_early0"):
        early_relay(0)

    def add_up(j):
        for index in range(mp):
            rest = dot(full_b[j], ups[index, j * lane:(j + 1) * lane, :])
            partial[index] = (states[index].astype(f32) if j == 0 else partial[index]) + rest

    for j in range(pieces):
        with scope("s_backwait%d" % j):
            back[j][1]()
        part_b[j] = dot(list_hot[...], from_b[j]).astype(bf16)
        sum1.into(j)
        if j == 0:
            with scope("s_early1"):
                early_relay(1)
        if j + 1 < pieces:
            sum1.across(j)
    with scope("s_sum1"):
        for j in range(pieces - 2):
            sum1.home(j)
        sum1.across(pieces - 1)
        early_finish(0)
        early_finish(1)
        if pieces > 1:
            sum1.home(pieces - 2)
        for j in range(pieces - 1):
            sum1.done(j)
            add_up(j)
        with scope("s_lasthome"):
            sum1.home(pieces - 1)

    starts, sizes = chunks_of(half)
    order = [(h, t) for t in range(len(sizes)) for h in (0, 1)]

    def chunk(c):
        side, t = c
        start = side * half + starts[t]
        return pl.ds(start if isinstance(side, int) else pl.multiple_of(start, half // 4), sizes[t])

    def chunk_id(c):
        return c[0] * len(sizes) + c[1]

    def act_copy(layer, parity, c, which):
        bit, off = plan[which]
        at = acts.at[layer, other_of(off), chunk(c)]
        return pltpu.make_async_remote_copy(
            src_ref=at, dst_ref=at,
            send_sem=act_send.at[parity, chunk_id(c)], recv_sem=act_recv.at[parity, chunk_id(c), which],
            device_id={"mp": flip(m, bit)}, device_id_type=MESH)

    def send(layer, parity, c):
        for i in local:
            act_copy(layer, parity, c, i).start()

    def relay(layer, parity, c):
        for i in relayed:
            first = brings[plan[i][1]]
            if [j for j in relayed if brings[plan[j][1]] == first][0] == i:
                act_copy(layer, parity, c, first).wait_recv()
            act_copy(layer, parity, c, i).start()

    def finish(layer, parity, c):
        for i in range(len(plan)):
            if i not in relays_from:
                act_copy(layer, parity, c, i).wait_recv()

    def sent(layer, parity, c):
        at = acts.at[layer, pl.ds(0, mp - 1), chunk(c)]
        pltpu.make_async_remote_copy(
            src_ref=at, dst_ref=at, send_sem=act_send.at[parity, chunk_id(c)], recv_sem=act_recv.at[parity, chunk_id(c), 0],
            device_id={"mp": flip(m, 1)}, device_id_type=MESH).wait_send()

    def product(k, at):
        total = None
        for off in held:
            index = other_of(off)
            term = dot(acts[k, index, at, :], weight[k, pl.ds(pl.multiple_of(index * width, width), width), :])
            total = term if total is None else total + term
        return silu(total)

    last_up = (pieces - 1) * lane
    load.wait()
    with scope("s_begin"):
        for spot in range(len(order)):
            c = (m % 2 if spot % 2 == 0 else 1 - m % 2), spot // 2
            at = chunk(c)
            if spot == 1:
                sum1.done(pieces - 1)
            for index in range(mp):
                before = partial[index, at] if pieces > 1 else states[index, at].astype(f32)
                first = before + dot(full_b[pieces - 1, at], ups[index, last_up:last_up + lane, :])
                partial[index, at] = first
                acts[0, index, at, :] = first.astype(bf16)
            hidden[at, :] = partial[m, at]
            acts[1, m, at, :] = product(0, at).astype(bf16)
            send(1, 1, c)
        sum1.drain()
        arrived(from_a.at[:, span], 0, 0).wait_send()
        arrived(from_b.at[:, span], 1, 0).wait_send()
        for which in range(2):
            early_sent(which)
    with scope("s_relay1"):
        relay(1, 1, order[0])

    def half_step(l, inside, first):
        k = 2 * l + inside
        for spot, c in enumerate(order):
            at = chunk(c)
            if spot + 1 < len(order):
                relay(k, inside, order[spot + 1])
            elif inside == 0:
                relay(k + 1, 1, order[0])
            elif not first or layers > 1:
                @pl.when(l + 1 < layers)
                def _():
                    relay(k + 1, 0, order[0])
            finish(k, inside, c)
            value = product(k, at)
            if inside == 0:
                sent(k - 1, 1, c)
                acts[k + 1, m, at, :] = value.astype(bf16)
                send(k + 1, 1, c)
            else:
                value = (hidden[at, :] + value) * inv_root_two
                hidden[at, :] = value

                @pl.when(l + 1 < layers)
                def _():
                    if not first:
                        sent(k - 1, 0, c)
                    acts[k + 1, m, at, :] = value.astype(bf16)
                    send(k + 1, 0, c)

    def layer_step(l, _):
        half_step(l, 0, False)
        half_step(l, 1, False)
        return 0

    with scope("s_layers"):
        half_step(0, 1, True)
        lax.fori_loop(1, layers, layer_step, 0)

    atom_in.wait()
    atom_rows = min(atoms, 256)
    parts, part_lane = table.shape[0], table.shape[2]
    here = pl.ds(pl.multiple_of(g * ATOM_DEV, ATOM_DEV), ATOM_DEV)
    atom_span = pl.ds(0, atoms - ATOM_DEV)
    gathers = [exchange(2, 2 * pieces + p, piece(atoms_to, p, ATOM_DEV), piece(atoms_from, p, ATOM_DEV),
                        atoms_from.at[p, atom_span]) for p in range(parts)]
    spreads = [exchange(3, 2 * pieces + parts + p, lambda peer, p=p: piece(table, p, ATOM_DEV)(g),
                        piece(table, p, ATOM_DEV), table.at[p, atom_span]) for p in range(parts)]

    def columns(p):
        return slice(p * part_lane, (p + 1) * part_lane)

    with scope("s_collect"):
        def collect(i, _):
            at = pl.ds(pl.multiple_of(i * atom_rows, atom_rows), atom_rows)
            ids = one_hot(atom_rows, atom_ref[...] - i * atom_rows)
            high, low = halves(hidden[...])
            total = dot(ids, high) + dot(ids, low)
            for p in range(parts):
                atoms_own[p, at] = total[:, columns(p)]
                atoms_to[p, at] = total[:, columns(p)].astype(bf16)
            return 0

        lax.fori_loop(0, atoms // atom_rows, collect, 0)
        for p in range(parts):
            gathers[p][0]()
    for p in range(parts):
        atoms_from[p, here] = jnp.zeros((ATOM_DEV, part_lane), bf16)
    for c in order:
        if layers > 1:
            sent(2 * layers - 2, 0, c)
        sent(2 * layers - 1, 1, c)
    for p in range(parts):
        with scope("s_atomwait%d" % p):
            gathers[p][1]()

        def add(i, total):
            return total + atoms_from[p, pl.ds(pl.multiple_of(i * ATOM_DEV, ATOM_DEV), ATOM_DEV)].astype(f32)

        total = lax.fori_loop(0, graph, add, atoms_own[p, here])
        mine_out = silu(atom_scale * total).astype(bf16)
        table[p, here] = mine_out
        spreads[p][0]()
        atom_out_ref[:, columns(p)] = mine_out
    arrived(atoms_from.at[:, atom_span], 2, 0).wait_send()
    for p in range(parts):
        with scope("s_spreadwait%d" % p):
            spreads[p][1]()

        def spread(i, total):
            at = pl.ds(pl.multiple_of(i * atom_rows, atom_rows), atom_rows)
            return total + dot(one_hot(atom_rows, atom_ref[...] - i * atom_rows), table[p, at], 0, 0)

        total = lax.fori_loop(0, atoms // atom_rows, spread, hidden[:, columns(p)])
        edge_out_ref[:, columns(p)] = total.astype(bf16)
    arrived(table.at[:, atom_span], 3, 0).wait_send()


def hand_on(edge_ref, atom_ref, edge_out_ref, atom_out_ref, sem):
    edge = pltpu.make_async_copy(edge_ref, edge_out_ref, sem.at[0])
    atom = pltpu.make_async_copy(atom_ref, atom_out_ref, sem.at[1])
    edge.start()
    atom.start()
    edge.wait()
    atom.wait()


def local(graph, mp, edge_state, down_weight, basis, basis_weight, up_weight, dense_weight,
          send_rows, trip_in, trip_out, trip_live, edge_atom):
    rows, width = edge_state.shape
    trip = down_weight.shape[1]
    slot_total = graph * send_rows.shape[2]
    triplets = trip_in.shape[0]
    maps = dense_weight.shape[0] * dense_weight.shape[1]
    tile = 2048 if slot_total <= 512 else 128
    atoms = graph * ATOM_DEV
    chunks = 2 * len(chunks_of(rows // 2)[1])
    stages = mp.bit_length()
    extra = max(stages - 2, 1)
    half = rows // 2
    vmem = pltpu.VMEM
    pieces = trip // 128 if trip % 128 == 0 else 1
    lane = trip // pieces
    pad = -(-basis.shape[0] // 16) * 16
    hot_bytes = 2 * 2 * slot_total * triplets
    hots = [vmem((slot_total, triplets), bf16)] * 2 if hot_bytes <= 2 ** 24 else [None, None]
    reduce_bufs = [
        vmem((pieces, rows, lane), bf16), vmem((pieces, half, lane), bf16), vmem((pieces, extra, half, lane), bf16),
        vmem((pieces, extra, half, lane), bf16), vmem((pieces, rows, lane), bf16),
    ]
    dma = pltpu.SemaphoreType.DMA
    spec = pl.BlockSpec(memory_space=pltpu.VMEM)
    operands = [
        edge_state, down_weight, basis, basis_weight, up_weight,
        dense_weight.reshape((maps,) + dense_weight.shape[2:]),
        send_rows, trip_in.reshape(1, triplets), trip_out.reshape(1, triplets),
        trip_live.reshape(1, triplets), edge_atom.reshape(1, rows),
    ]
    inputs = [vmem(a.shape, a.dtype) for i, a in enumerate(operands) if i not in (0, 4, 5)]
    parts = width // 128 if width % 128 == 0 else 1
    atom_buf = (parts, atoms, width // parts)
    body = functools.partial(kernel, graph, mp, tile)
    before = [
        *inputs, dma((len(inputs) + 2,)),
        vmem((mp, rows, width), bf16), vmem((mp, trip, width), bf16), dma((2,)), dma((2, mp - 1)),
        vmem((maps,) + dense_weight.shape[2:], bf16), dma(()),
        *reduce_bufs, *reduce_bufs,
        dma((2, stages)), dma((2, pieces, stages)),
        *[vmem((pieces, slot_total, lane), bf16)] * 4,
        dma((4,)), dma((2 * pieces + 2 * parts,)),
        vmem((rows, slot_total), bf16), vmem((3 * pad, triplets), bf16), vmem((3 * pad, trip), bf16),
        vmem((trip, triplets), f32), vmem((slot_total, lane), f32),
    ]
    if hots[0] is None:
        hots, kept_body, at = [], body, len(operands) + 2 + len(before)
        body = lambda *refs: kept_body(*refs[:at], None, None, *refs[at:])
    outs = pl.pallas_call(
        body,
        out_shape=(
            pltpu.VMEM((rows, width), bf16),
            pltpu.VMEM((ATOM_DEV, width), bf16),
        ),
        in_specs=[pl.BlockSpec(memory_space=pl.ANY)] * len(operands),
        out_specs=(spec, spec),
        scratch_shapes=[
            *before, *hots,
            vmem((maps, mp, rows, width), bf16), vmem((mp, rows, width), f32), vmem((rows, width), f32),
            dma((2, chunks)), dma((2, chunks, mp - 1)),
            vmem(atom_buf, f32), vmem(atom_buf, bf16), vmem(atom_buf, bf16), vmem(atom_buf, bf16),
        ],
        compiler_params=pltpu.CompilerParams(
            collective_id=0, has_side_effects=True, vmem_limit_bytes=64000 * 1024
        ),
        name="edge_block",
    )(*operands)
    outs = [pltpu.with_memory_space_constraint(o, pltpu.VMEM) for o in outs]
    return pl.pallas_call(
        hand_on,
        out_shape=tuple(jax.ShapeDtypeStruct(o.shape, o.dtype) for o in outs),
        in_specs=[spec] * 2,
        out_specs=[pl.BlockSpec(memory_space=pl.ANY)] * 2,
        scratch_shapes=[dma((2,))],
        name="hand_on",
    )(*outs)


def solution(mesh):
    in_specs = (
        P("graph", "mp"),
        P("mp", None),
        P(None, ("graph", "mp")),
        P(),
        P(None, "mp"),
        P(None, None, None, "mp"),
        P("graph", "mp", None),
        P(("graph", "mp")),
        P(("graph", "mp")),
        P(("graph", "mp")),
        P("graph"),
    )
    out_specs = (P("graph", "mp"), P("graph", "mp"))
    body = functools.partial(local, mesh.shape["graph"], mesh.shape["mp"])
    return jax.shard_map(body, mesh=mesh, in_specs=in_specs, out_specs=out_specs, check_vma=False)
```

```python
import functools

import jax
import jax.numpy as jnp
from jax import lax
from jax.experimental import pallas as pl
from jax.experimental.pallas import tpu as pltpu
from jax.sharding import PartitionSpec as P

ATOM_DEV = 32

inv_root_two = 0.7071067811865476
atom_scale = 0.2

MESH = pl.DeviceIdType.MESH
bf16 = jnp.bfloat16
f32 = jnp.float32


def scope(name):
    return jax.named_scope(name)


def silu(v):
    return v / (1.0 + jnp.exp(-v))


def flip(index, bit):
    return index + bit - 2 * bit * ((index // bit) % 2)


def one_hot(rows, ids):
    shape = (rows, ids.shape[1])
    return jnp.where(lax.broadcasted_iota(jnp.int32, shape, 0) == ids, 1.0, 0.0).astype(bf16)


def dot(a, b, ca=1, cb=0):
    return lax.dot_general(a, b, (((ca,), (cb,)), ((), ())), preferred_element_type=f32)


def halves(v):
    high = v.astype(bf16)
    return high, (v - high.astype(f32)).astype(bf16)


def chunks_of(half):
    return (0, half // 2), (half // 2, half // 2)


def gather_plan(mp):
    plan, held, bit = [], [0], mp // 2
    while bit >= 1:
        plan += [(bit, off) for off in held]
        held += [bit ^ off for off in held]
        bit //= 2
    return plan, held


def kernel(
    graph, mp, tile,
    state_hbm, down_hbm, basis_hbm, bw_hbm, up_hbm, dense_hbm, lists_hbm, in_hbm, out_hbm, live_hbm, atom_hbm,
    edge_out_ref, atom_out_ref,
    down_ref, basis_ref, bw_ref, lists_ref, in_ref, out_ref, live_ref, atom_ref, load_sem,
    states, ups, early_send, early_recv,
    weight, weight_sem, opposite, feed_send, feed_y, feed_far, feed_near, core_send, core_recv,
    part_a, got_a, sum_a, more_a, full_a,
    part_b, got_b, sum_b, more_b, full_b,
    red_send, red_recv,
    to_a, from_a, to_b, from_b, xc_send, xc_recv,
    list_hot, basis_stack, bw_stack, angle, slots, in_hot, out_hot,
    acts, partial, hidden, act_send, act_recv,
    atoms_own, atoms_to, atoms_from, table,
):
    g = lax.axis_index("graph")
    m = lax.axis_index("mp")
    rows, width = hidden.shape
    trip = down_ref.shape[1]
    layers = weight.shape[0] // 2
    cap = lists_ref.shape[2]
    slot_total = graph * cap
    pieces, lane = to_a.shape[0], to_a.shape[2]
    kept = in_hot is not None
    triplets = in_ref.shape[1]
    atoms = graph * ATOM_DEV
    half = rows // 2
    bits = [1 << i for i in range(mp.bit_length() - 1)]
    stages = len(bits)

    barrier = pltpu.get_barrier_semaphore()

    def greet(k, _):
        pl.semaphore_signal(barrier, inc=1, device_id={"graph": (g + k) % graph}, device_id_type=MESH)
        return 0

    lax.fori_loop(1, graph, greet, 0)
    for bit in bits:
        pl.semaphore_signal(barrier, inc=1, device_id={"mp": flip(m, bit)}, device_id_type=MESH)

    hbm = [state_hbm, down_hbm, lists_hbm, in_hbm, out_hbm, live_hbm, basis_hbm, bw_hbm, up_hbm, atom_hbm]
    here_refs = [
        states.at[m], down_ref, lists_ref, in_ref, out_ref, live_ref, basis_ref, bw_ref, ups.at[m], atom_ref]
    loads = [pltpu.make_async_copy(a, b, load_sem.at[i]) for i, (a, b) in enumerate(zip(hbm, here_refs))]
    for load in loads:
        load.start()
    state_in, down_in, lists_in, in_in, out_in, live_in, basis_in, bw_in, up_in, atom_in = loads

    def mp_copy(src, dst, which, j, stage, bit):
        return pltpu.make_async_remote_copy(
            src_ref=src, dst_ref=dst, send_sem=red_send.at[which, stage], recv_sem=red_recv.at[which, j, stage],
            device_id={"mp": flip(m, bit)}, device_id_type=MESH)

    mine = pl.ds(pl.multiple_of((m % 2) * half, half), half)
    other = pl.ds(pl.multiple_of(half - (m % 2) * half, half), half)

    plan, held = gather_plan(mp)

    def other_of(off):
        index = m
        for bit in bits:
            if off & bit:
                index = flip(index, bit)
        return index

    local = [i for i, (bit, off) in enumerate(plan) if off == 0]
    relayed = [i for i, (bit, off) in enumerate(plan) if off != 0]
    brings = {bit ^ off: i for i, (bit, off) in enumerate(plan)}
    relays_from = sorted({brings[plan[i][1]] for i in relayed})

    def early(which, i):
        bit, off = plan[i]
        at = (states, ups)[which].at[other_of(off)]
        return pltpu.make_async_remote_copy(
            src_ref=at, dst_ref=at, send_sem=early_send.at[which], recv_sem=early_recv.at[which, i],
            device_id={"mp": flip(m, bit)}, device_id_type=MESH)

    def early_sent(which):
        at = (states, ups)[which].at[pl.ds(0, mp - 1)]
        pltpu.make_async_remote_copy(
            src_ref=at, dst_ref=at, send_sem=early_send.at[which], recv_sem=early_recv.at[which, 0],
            device_id={"mp": flip(m, 1)}, device_id_type=MESH).wait_send()

    def early_relay(which):
        for i in relayed:
            first = brings[plan[i][1]]
            if [j for j in relayed if brings[plan[j][1]] == first][0] == i:
                early(which, first).wait_recv()
            early(which, i).start()

    def early_finish(which):
        for i in range(len(plan)):
            if i not in relays_from:
                early(which, i).wait_recv()

    across_y = flip(m, mp // 2)
    feeds = layers - 1
    eighth = weight.shape[1] // 8
    mine8 = g % 8

    def xor(a, k):
        for bit in (1, 2, 4):
            if k & bit:
                a = flip(a, bit)
        return a

    def part8(e):
        return pl.ds(pl.multiple_of(e * eighth, eighth), eighth)

    def feed_copy(src, f, e, sem, device):
        return pltpu.make_async_remote_copy(
            src_ref=src, dst_ref=opposite.at[f, part8(e)], send_sem=feed_send.at[f], recv_sem=sem,
            device_id=device, device_id_type=MESH)

    def enter(f):
        return feed_copy(weight.at[2 * (f + 1), part8(mine8)], f, mine8, feed_y.at[f], {"mp": across_y})

    def hop(f):
        return feed_copy(opposite.at[f, part8(mine8)], f, mine8, feed_far.at[f], {"graph": xor(g, 4)})

    def near(f, far):
        e = xor(mine8, 4 * far)
        return [feed_copy(opposite.at[f, part8(e)], f, e, feed_near.at[f, far], {"graph": xor(g, k)}) for k in (3, 2, 1)]

    def feed_spread(f):
        enter(f).wait_recv()
        hop(f).start()
        for copy in near(f, 0):
            copy.start()

    def feed_rest(f):
        hop(f).wait_recv()
        for copy in near(f, 1):
            copy.start()

    def feed_ready(f):
        at = opposite.at[f, pl.ds(0, 3 * eighth)]
        for far in range(2):
            pltpu.make_async_remote_copy(
                src_ref=at, dst_ref=at, send_sem=feed_send.at[f], recv_sem=feed_near.at[f, far],
                device_id={"mp": across_y}, device_id_type=MESH).wait_recv()

    def feed_sent():
        for f in range(feeds):
            at = opposite.at[f]
            pltpu.make_async_remote_copy(
                src_ref=at, dst_ref=at, send_sem=feed_send.at[f], recv_sem=feed_near.at[f, 0],
                device_id={"mp": across_y}, device_id_type=MESH).wait_send()

    class Sum:
        def __init__(self, which, part, got, summed, more, full):
            self.which, self.part, self.got = which, part, got
            self.summed, self.more, self.full = summed, more, full

        def first(self, j):
            return mp_copy(self.part.at[j, other], self.got.at[j], self.which, j, 0, 1)

        def step(self, j, b):
            return mp_copy(self.summed.at[j, b], self.more.at[j, b], self.which, j, 1 + b, bits[1 + b])

        def last(self, j):
            at = self.full.at[j, mine]
            return mp_copy(at, at, self.which, j, stages, 1)

        def into(self, j):
            self.first(j).start()

        def across(self, j):
            self.first(j).wait_recv()
            total = self.part[j, mine].astype(f32) + self.got[j].astype(f32)
            if stages > 1:
                self.summed[j, 0] = total.astype(bf16)
                self.step(j, 0).start()
            else:
                self.full[j, mine] = total.astype(bf16)

        def home(self, j):
            for b in range(stages - 1):
                self.step(j, b).wait_recv()
                total = self.summed[j, b].astype(f32) + self.more[j, b].astype(f32)
                if b + 2 < stages:
                    self.summed[j, b + 1] = total.astype(bf16)
                    self.step(j, b + 1).start()
                else:
                    self.full[j, mine] = total.astype(bf16)
            self.last(j).start()

        def done(self, j):
            self.last(j).wait_recv()

        def drain(self):
            for stage in range(stages + 1):
                mp_copy(self.got, self.got, self.which, 0, stage, 1).wait_send()

    sum0 = Sum(0, part_a, got_a, sum_a, more_a, full_a)
    sum1 = Sum(1, part_b, got_b, sum_b, more_b, full_b)

    def peer_of(k):
        if graph & (graph - 1):
            return (g + k) % graph
        return sum(bit * ((g // bit + k // bit) % 2) for bit in (1 << i for i in range(graph.bit_length() - 1)))

    peers = [peer_of(k) for k in range(graph - 1, 0, -1)] if graph <= 8 else None

    def arrived(whole, group, which):
        return pltpu.make_async_remote_copy(
            src_ref=whole, dst_ref=whole, send_sem=xc_send.at[group], recv_sem=xc_recv.at[which],
            device_id={"graph": (g + 1) % graph}, device_id_type=MESH)

    def exchange(group, which, src_at, dst_at, whole):
        def to(peer):
            pltpu.make_async_remote_copy(
                src_ref=src_at(peer), dst_ref=dst_at(g), send_sem=xc_send.at[group], recv_sem=xc_recv.at[which],
                device_id={"graph": peer}, device_id_type=MESH).start()

        def one(i, _):
            to(peer_of(graph - 1 - i))
            return 0

        def start():
            if peers is None:
                lax.fori_loop(0, graph - 1, one, 0)
            else:
                for peer in peers:
                    to(peer)

        return start, arrived(whole, group, which).wait_recv

    def block(ref, size):
        return lambda i: ref.at[pl.ds(pl.multiple_of(i * size, size), size)]

    def piece(ref, j, size):
        return lambda i: ref.at[j, pl.ds(pl.multiple_of(i * size, size), size)]

    def tiles(step):
        def one(i, _):
            step(pl.ds(pl.multiple_of(i * tile, tile), tile))
            return 0

        lax.fori_loop(0, triplets // tile, one, 0)

    def in_part(at):
        return one_hot(slot_total, in_ref[:, at])

    def out_part(at):
        return one_hot(slot_total, jnp.where(live_ref[:, at] > 0, out_ref[:, at], -1))

    state_in.wait()
    down_in.wait()
    with scope("s_proj"):
        projected = dot(states[m], down_ref[...]).astype(bf16)
        for j in range(pieces):
            part_a[j] = projected[:, j * lane:(j + 1) * lane]
    with scope("s_barrier"):
        pl.semaphore_wait(barrier, graph - 1 + len(bits))
    for j in range(pieces):
        sum0.into(j)
    load = pltpu.make_async_copy(dense_hbm, weight, weight_sem)
    load.start()

    lists_in.wait()
    with scope("s_hots"):
        for i in range(graph):
            list_hot[:, i * cap:(i + 1) * cap] = one_hot(rows, lists_ref[0, i:i + 1, :])
        in_in.wait()
        if kept:
            def keep_in(at):
                in_hot[:, at] = in_part(at)

            tiles(keep_in)
    with scope("s_across"):
        for j in range(pieces):
            sum0.across(j)
    up_in.wait()
    early(0, local[0]).start()
    out_in.wait()
    live_in.wait()
    if kept:
        def keep_out(at):
            out_hot[:, at] = out_part(at)

        with scope("s_outhot"):
            tiles(keep_out)

    basis_in.wait()
    bw_in.wait()
    depth = basis_ref.shape[0]
    pad = basis_stack.shape[0] // 3
    with scope("s_angles"):
        bw_high, bw_low = halves(bw_ref[...])
        bw_stack[...] = jnp.zeros_like(bw_stack)
        bw_stack[0:depth] = bw_high
        bw_stack[pad:pad + depth] = bw_high
        bw_stack[2 * pad:2 * pad + depth] = bw_low

        def angles(at):
            high, low = halves(basis_ref[:, at])
            basis_stack[:, at] = jnp.zeros((3 * pad, tile), bf16)
            basis_stack[0:depth, at] = high
            basis_stack[pad:pad + depth, at] = low
            basis_stack[2 * pad:2 * pad + depth, at] = high
            angle[:, at] = dot(bw_stack[...], basis_stack[:, at], 0, 0)

        tiles(angles)

    load.wait()
    if feeds:
        enter(0).start()
    early(1, local[0]).start()
    step_rows = min(slot_total, 512)
    own = pl.ds(pl.multiple_of(g * cap, cap), cap)
    span = pl.ds(0, slot_total - cap)
    going = [exchange(0, j, piece(to_a, j, cap), piece(from_a, j, cap), from_a.at[j, span]) for j in range(pieces)]
    back = [exchange(1, pieces + j, piece(to_b, j, cap), piece(from_b, j, cap), from_b.at[j, span])
            for j in range(pieces)]

    def pick_piece(j):
        def pick(i, _):
            at = pl.ds(pl.multiple_of(i * step_rows, step_rows), step_rows)
            to_a[j, at, :] = dot(list_hot[:, at], full_a[j], 0, 0).astype(bf16)
            return 0

        sum0.done(j)
        lax.fori_loop(0, slot_total // step_rows, pick, 0)
        going[j][0]()
        from_a[j, own] = to_a[j, own]

    with scope("s_home"):
        sum0.home(0)
    with scope("s_home1"):
        for j in range(1, pieces):
            sum0.home(j)
            pick_piece(j - 1)
        pick_piece(pieces - 1)
    for which in range(2):
        for i in local[1:]:
            early(which, i).start()
    sum0.drain()

    for j in range(pieces):
        with scope("s_gowait%d" % j):
            going[j][1]()
        slots[...] = jnp.zeros_like(slots)
        received = from_a[j].astype(f32).T.astype(bf16)

        def trips(at):
            source = in_hot[:, at] if kept else in_part(at)
            value = dot(received, source) * angle[j * lane:(j + 1) * lane, at]
            target = out_hot[:, at] if kept else out_part(at)
            slots[...] += dot(target, value.astype(bf16), 1, 1)

        with scope("s_trips%d" % j):
            tiles(trips)
        to_b[j] = slots[...].astype(bf16)
        back[j][0]()
        from_b[j, own] = to_b[j, own]
    with scope("s_early0"):
        early_relay(0)

    def add_up(j):
        for index in range(mp):
            rest = dot(full_b[j], ups[index, j * lane:(j + 1) * lane, :])
            partial[index] = (states[index].astype(f32) if j == 0 else partial[index]) + rest

    for j in range(pieces):
        with scope("s_backwait%d" % j):
            back[j][1]()
        part_b[j] = dot(list_hot[...], from_b[j]).astype(bf16)
        sum1.into(j)
        if j + 1 < pieces:
            sum1.across(j)
    with scope("s_sum1"):
        for j in range(pieces - 2):
            sum1.home(j)
        sum1.across(pieces - 1)
        with scope("s_early1"):
            early_relay(1)
        with scope("s_feedspread"):
            if feeds:
                feed_spread(0)
            for f in range(1, feeds):
                enter(f).start()
        early_finish(0)
        early_finish(1)
        if pieces > 1:
            sum1.home(pieces - 2)
        for j in range(pieces - 1):
            sum1.done(j)
            add_up(j)
        with scope("s_lasthome"):
            sum1.home(pieces - 1)

    starts, sizes = chunks_of(half)
    order = [(h, t) for t in range(len(sizes)) for h in (0, 1)]

    def chunk(c):
        side, t = c
        start = side * half + starts[t]
        return pl.ds(start if isinstance(side, int) else pl.multiple_of(start, half // 2), sizes[t])

    def chunk_id(c):
        return c[0] * len(sizes) + c[1]

    def act_copy(layer, parity, c, which):
        bit, off = plan[which]
        at = acts.at[layer - 1, other_of(off), chunk(c)]
        return pltpu.make_async_remote_copy(
            src_ref=at, dst_ref=at,
            send_sem=act_send.at[parity, chunk_id(c)], recv_sem=act_recv.at[parity, chunk_id(c), which],
            device_id={"mp": flip(m, bit)}, device_id_type=MESH)

    def send(layer, parity, c):
        for i in local:
            act_copy(layer, parity, c, i).start()

    def relay(layer, parity, c):
        for i in relayed:
            first = brings[plan[i][1]]
            if [j for j in relayed if brings[plan[j][1]] == first][0] == i:
                act_copy(layer, parity, c, first).wait_recv()
            act_copy(layer, parity, c, i).start()

    def finish(layer, parity, c):
        for i in range(len(plan)):
            if i not in relays_from:
                act_copy(layer, parity, c, i).wait_recv()

    def sent(layer, parity, c):
        at = acts.at[layer - 1, pl.ds(0, mp - 1), chunk(c)]
        pltpu.make_async_remote_copy(
            src_ref=at, dst_ref=at, send_sem=act_send.at[parity, chunk_id(c)], recv_sem=act_recv.at[parity, chunk_id(c), 0],
            device_id={"mp": flip(m, 1)}, device_id_type=MESH).wait_send()

    def product(k, at, held_weight):
        total = None
        for off in held:
            index = other_of(off)
            term = dot(acts[k - 1, index, at, :], held_weight[pl.ds(pl.multiple_of(index * width, width), width), :])
            total = term if total is None else total + term
        return silu(total)

    def core_copy(layer, c, i):
        at = acts.at[layer - 1, (m, across_y)[i], chunk(c)]
        return pltpu.make_async_remote_copy(
            src_ref=at, dst_ref=at, send_sem=core_send.at[chunk_id(c)], recv_sem=core_recv.at[chunk_id(c), i],
            device_id={"mp": flip(m, 1)}, device_id_type=MESH)

    def core_sent(layer, c):
        at = acts.at[layer - 1, pl.ds(0, 2), chunk(c)]
        pltpu.make_async_remote_copy(
            src_ref=at, dst_ref=at, send_sem=core_send.at[chunk_id(c)], recv_sem=core_recv.at[chunk_id(c), 0],
            device_id={"mp": flip(m, 1)}, device_id_type=MESH).wait_send()

    last_up = (pieces - 1) * lane
    with scope("s_begin"):
        for spot in range(len(order)):
            c = (m % 2 if spot % 2 == 0 else 1 - m % 2), spot // 2
            at = chunk(c)
            if spot == 1:
                sum1.done(pieces - 1)
            total = None
            for index in range(mp):
                before = partial[index, at] if pieces > 1 else states[index, at].astype(f32)
                first = before + dot(full_b[pieces - 1, at], ups[index, last_up:last_up + lane, :])
                partial[index, at] = first
                term = dot(first.astype(bf16), weight[0, index * width:(index + 1) * width, :])
                total = term if total is None else total + term
            hidden[at, :] = partial[m, at]
            acts[0, m, at, :] = silu(total).astype(bf16)
            send(1, 0, c)
        sum1.drain()
        arrived(from_a.at[:, span], 0, 0).wait_send()
        arrived(from_b.at[:, span], 1, 0).wait_send()
        for which in range(2):
            early_sent(which)
    def update(k, c):
        at = chunk(c)
        value = (hidden[at, :] + product(k, at, weight.at[k])) * inv_root_two
        hidden[at, :] = value
        return value.astype(bf16)

    with scope("s_layer0"):
        relay(1, 0, order[0])
        for spot, c in enumerate(order):
            with scope("s_l0fin%d" % spot):
                finish(1, 0, c)
            value = update(1, c)
            if layers > 1:
                acts[1, m, chunk(c), :] = value
                send(2, 1, c)
            if spot + 1 < len(order):
                with scope("s_l0rel%d" % spot):
                    relay(1, 0, order[spot + 1])
            if spot == 0:
                with scope("s_feedrest0"):
                    if feeds:
                        feed_rest(0)
                    for f in range(1, feeds):
                        feed_spread(f)
        with scope("s_feedrest1"):
            for f in range(1, feeds):
                feed_rest(f)
        if layers > 1:
            relay(2, 1, order[0])

    def layer_step(l, _):
        k, parity, f = 2 * l, l % 2, l - 1

        def second(c):
            for i in range(2):
                core_copy(k + 1, c, i).wait_recv()
            value = update(k + 1, c)

            @pl.when(l + 1 < layers)
            def _():
                sent(k, 1 - parity, c)
                acts[k + 1, m, chunk(c), :] = value
                send(k + 2, 1 - parity, c)

        with scope("s_feedwait"):
            feed_ready(f)
        for spot, c in enumerate(order):
            at = chunk(c)
            with scope("s_fin%d" % spot):
                finish(k, parity, c)

            @pl.when(l > 1)
            def _():
                core_sent(k - 1, c)

            acts[k, m, at, :] = product(k, at, weight.at[k]).astype(bf16)
            core_copy(k + 1, c, 0).start()
            with scope("s_rel%d" % spot):
                if spot + 1 < len(order):
                    relay(k, parity, order[spot + 1])
            acts[k, across_y, at, :] = product(k, at, opposite.at[f]).astype(bf16)
            core_copy(k + 1, c, 1).start()
            if spot >= 1:
                with scope("s_second%d" % spot):
                    second(order[spot - 1])

        @pl.when(l + 1 < layers)
        def _():
            with scope("s_relnext"):
                relay(k + 2, 1 - parity, order[0])

        with scope("s_second_last"):
            second(order[-1])
        return 0

    with scope("s_layers"):
        lax.fori_loop(1, layers, layer_step, 0)

    atom_in.wait()
    atom_rows = min(atoms, 256)
    parts, part_lane = table.shape[0], table.shape[2]
    here = pl.ds(pl.multiple_of(g * ATOM_DEV, ATOM_DEV), ATOM_DEV)
    atom_span = pl.ds(0, atoms - ATOM_DEV)
    gathers = [exchange(2, 2 * pieces + p, piece(atoms_to, p, ATOM_DEV), piece(atoms_from, p, ATOM_DEV),
                        atoms_from.at[p, atom_span]) for p in range(parts)]
    spreads = [exchange(3, 2 * pieces + parts + p, lambda peer, p=p: piece(table, p, ATOM_DEV)(g),
                        piece(table, p, ATOM_DEV), table.at[p, atom_span]) for p in range(parts)]

    def columns(p):
        return slice(p * part_lane, (p + 1) * part_lane)

    with scope("s_collect"):
        def collect(i, _):
            at = pl.ds(pl.multiple_of(i * atom_rows, atom_rows), atom_rows)
            ids = one_hot(atom_rows, atom_ref[...] - i * atom_rows)
            high, low = halves(hidden[...])
            total = dot(ids, high) + dot(ids, low)
            for p in range(parts):
                atoms_own[p, at] = total[:, columns(p)]
                atoms_to[p, at] = total[:, columns(p)].astype(bf16)
            return 0

        lax.fori_loop(0, atoms // atom_rows, collect, 0)
        for p in range(parts):
            gathers[p][0]()
    for p in range(parts):
        atoms_from[p, here] = jnp.zeros((ATOM_DEV, part_lane), bf16)
    for c in order:
        sent(1, (layers - 1) % 2, c)
        if layers > 1:
            sent(1, layers % 2, c)
            core_sent(1, c)
    feed_sent()
    for p in range(parts):
        with scope("s_atomwait%d" % p):
            gathers[p][1]()

        def add(i, total):
            return total + atoms_from[p, pl.ds(pl.multiple_of(i * ATOM_DEV, ATOM_DEV), ATOM_DEV)].astype(f32)

        total = lax.fori_loop(0, graph, add, atoms_own[p, here])
        mine_out = silu(atom_scale * total).astype(bf16)
        table[p, here] = mine_out
        spreads[p][0]()
        atom_out_ref[:, columns(p)] = mine_out
    arrived(atoms_from.at[:, atom_span], 2, 0).wait_send()
    for p in range(parts):
        with scope("s_spreadwait%d" % p):
            spreads[p][1]()

        def spread(i, total):
            at = pl.ds(pl.multiple_of(i * atom_rows, atom_rows), atom_rows)
            return total + dot(one_hot(atom_rows, atom_ref[...] - i * atom_rows), table[p, at], 0, 0)

        total = lax.fori_loop(0, atoms // atom_rows, spread, hidden[:, columns(p)])
        edge_out_ref[:, columns(p)] = total.astype(bf16)
    arrived(table.at[:, atom_span], 3, 0).wait_send()


def hand_on(edge_ref, atom_ref, edge_out_ref, atom_out_ref, sem):
    edge = pltpu.make_async_copy(edge_ref, edge_out_ref, sem.at[0])
    atom = pltpu.make_async_copy(atom_ref, atom_out_ref, sem.at[1])
    edge.start()
    atom.start()
    edge.wait()
    atom.wait()


def local(graph, mp, edge_state, down_weight, basis, basis_weight, up_weight, dense_weight,
          send_rows, trip_in, trip_out, trip_live, edge_atom):
    rows, width = edge_state.shape
    trip = down_weight.shape[1]
    slot_total = graph * send_rows.shape[2]
    triplets = trip_in.shape[0]
    maps = dense_weight.shape[0] * dense_weight.shape[1]
    tile = 2048 if slot_total <= 512 else 128
    atoms = graph * ATOM_DEV
    feeds = max(dense_weight.shape[0] - 1, 1)
    chunks = 2 * len(chunks_of(rows // 2)[1])
    stages = mp.bit_length()
    extra = max(stages - 2, 1)
    half = rows // 2
    vmem = pltpu.VMEM
    pieces = trip // 128 if trip % 128 == 0 else 1
    lane = trip // pieces
    pad = -(-basis.shape[0] // 16) * 16
    hot_bytes = 2 * 2 * slot_total * triplets
    hots = [vmem((slot_total, triplets), bf16)] * 2 if hot_bytes <= 2 ** 24 else [None, None]
    reduce_bufs = [
        vmem((pieces, rows, lane), bf16), vmem((pieces, half, lane), bf16), vmem((pieces, extra, half, lane), bf16),
        vmem((pieces, extra, half, lane), bf16), vmem((pieces, rows, lane), bf16),
    ]
    dma = pltpu.SemaphoreType.DMA
    spec = pl.BlockSpec(memory_space=pltpu.VMEM)
    operands = [
        edge_state, down_weight, basis, basis_weight, up_weight,
        dense_weight.reshape((maps,) + dense_weight.shape[2:]),
        send_rows, trip_in.reshape(1, triplets), trip_out.reshape(1, triplets),
        trip_live.reshape(1, triplets), edge_atom.reshape(1, rows),
    ]
    inputs = [vmem(a.shape, a.dtype) for i, a in enumerate(operands) if i not in (0, 4, 5)]
    parts = width // 128 if width % 128 == 0 else 1
    atom_buf = (parts, atoms, width // parts)
    body = functools.partial(kernel, graph, mp, tile)
    before = [
        *inputs, dma((len(inputs) + 2,)),
        vmem((mp, rows, width), bf16), vmem((mp, trip, width), bf16), dma((2,)), dma((2, mp - 1)),
        vmem((maps,) + dense_weight.shape[2:], bf16), dma(()),
        vmem((feeds,) + dense_weight.shape[2:], bf16), dma((feeds,)), dma((feeds,)), dma((feeds,)), dma((feeds, 2)),
        dma((chunks,)), dma((chunks, 2)),
        *reduce_bufs, *reduce_bufs,
        dma((2, stages)), dma((2, pieces, stages)),
        *[vmem((pieces, slot_total, lane), bf16)] * 4,
        dma((4,)), dma((2 * pieces + 2 * parts,)),
        vmem((rows, slot_total), bf16), vmem((3 * pad, triplets), bf16), vmem((3 * pad, trip), bf16),
        vmem((trip, triplets), f32), vmem((slot_total, lane), f32),
    ]
    if hots[0] is None:
        hots, kept_body, at = [], body, len(operands) + 2 + len(before)
        body = lambda *refs: kept_body(*refs[:at], None, None, *refs[at:])
    outs = pl.pallas_call(
        body,
        out_shape=(
            pltpu.VMEM((rows, width), bf16),
            pltpu.VMEM((ATOM_DEV, width), bf16),
        ),
        in_specs=[pl.BlockSpec(memory_space=pl.ANY)] * len(operands),
        out_specs=(spec, spec),
        scratch_shapes=[
            *before, *hots,
            vmem((maps - 1, mp, rows, width), bf16), vmem((mp, rows, width), f32), vmem((rows, width), f32),
            dma((2, chunks)), dma((2, chunks, mp - 1)),
            vmem(atom_buf, f32), vmem(atom_buf, bf16), vmem(atom_buf, bf16), vmem(atom_buf, bf16),
        ],
        compiler_params=pltpu.CompilerParams(
            collective_id=0, has_side_effects=True, vmem_limit_bytes=64000 * 1024
        ),
        name="edge_block",
    )(*operands)
    outs = [pltpu.with_memory_space_constraint(o, pltpu.VMEM) for o in outs]
    return pl.pallas_call(
        hand_on,
        out_shape=tuple(jax.ShapeDtypeStruct(o.shape, o.dtype) for o in outs),
        in_specs=[spec] * 2,
        out_specs=[pl.BlockSpec(memory_space=pl.ANY)] * 2,
        scratch_shapes=[dma((2,))],
        name="hand_on",
    )(*outs)


def solution(mesh):
    in_specs = (
        P("graph", "mp"),
        P("mp", None),
        P(None, ("graph", "mp")),
        P(),
        P(None, "mp"),
        P(None, None, None, "mp"),
        P("graph", "mp", None),
        P(("graph", "mp")),
        P(("graph", "mp")),
        P(("graph", "mp")),
        P("graph"),
    )
    out_specs = (P("graph", "mp"), P("graph", "mp"))
    body = functools.partial(local, mesh.shape["graph"], mesh.shape["mp"])
    return jax.shard_map(body, mesh=mesh, in_specs=in_specs, out_specs=out_specs, check_vma=False)
```

```python
import functools

import jax
import jax.numpy as jnp
from jax import lax
from jax.experimental import pallas as pl
from jax.experimental.pallas import tpu as pltpu
from jax.sharding import PartitionSpec as P

ATOM_DEV = 32

inv_root_two = 0.7071067811865476
atom_scale = 0.2

MESH = pl.DeviceIdType.MESH
bf16 = jnp.bfloat16
f32 = jnp.float32


def scope(name):
    return jax.named_scope(name)


def silu(v):
    return v / (1.0 + jnp.exp(-v))


def flip(index, bit):
    return index + bit - 2 * bit * ((index // bit) % 2)


def one_hot(rows, ids):
    shape = (rows, ids.shape[1])
    return jnp.where(lax.broadcasted_iota(jnp.int32, shape, 0) == ids, 1.0, 0.0).astype(bf16)


def dot(a, b, ca=1, cb=0):
    return lax.dot_general(a, b, (((ca,), (cb,)), ((), ())), preferred_element_type=f32)


def halves(v):
    high = v.astype(bf16)
    return high, (v - high.astype(f32)).astype(bf16)


def chunks_of(half):
    return (0, half // 2), (half // 2, half // 2)


def gather_plan(mp):
    plan, held, bit = [], [0], mp // 2
    while bit >= 1:
        plan += [(bit, off) for off in held]
        held += [bit ^ off for off in held]
        bit //= 2
    return plan, held


def kernel(
    graph, mp, tile,
    state_hbm, down_hbm, basis_hbm, bw_hbm, up_hbm, dense_hbm, lists_hbm, in_hbm, out_hbm, live_hbm, atom_hbm,
    edge_out_ref, atom_out_ref,
    down_ref, basis_ref, bw_ref, lists_ref, in_ref, out_ref, live_ref, atom_ref, load_sem,
    states, ups, early_send, early_recv, up_send, up_recv,
    weight, weight_sem, opposite, feed_send, feed_y, feed_far, near_recv, core_send, core_recv,
    part_a, got_a, sum_a, more_a, full_a,
    part_b, got_b, sum_b, more_b, full_b,
    red_send, red_recv,
    to_a, from_a, to_b, from_b, xc_send, xc_recv,
    list_hot, basis_stack, bw_stack, angle, slots, in_hot, out_hot,
    acts, partial, hidden, act_send, act_recv,
    atoms_own, atoms_to, atoms_from, table,
):
    g = lax.axis_index("graph")
    m = lax.axis_index("mp")
    rows, width = hidden.shape
    trip = down_ref.shape[1]
    layers = weight.shape[0] // 2
    cap = lists_ref.shape[2]
    slot_total = graph * cap
    pieces, lane = to_a.shape[0], to_a.shape[2]
    kept = in_hot is not None
    triplets = in_ref.shape[1]
    atoms = graph * ATOM_DEV
    half = rows // 2
    bits = [1 << i for i in range(mp.bit_length() - 1)]
    stages = len(bits)

    barrier = pltpu.get_barrier_semaphore()

    def greet(k, _):
        pl.semaphore_signal(barrier, inc=1, device_id={"graph": (g + k) % graph}, device_id_type=MESH)
        return 0

    lax.fori_loop(1, graph, greet, 0)
    for bit in bits:
        pl.semaphore_signal(barrier, inc=1, device_id={"mp": flip(m, bit)}, device_id_type=MESH)

    hbm = [state_hbm, down_hbm, lists_hbm, in_hbm, out_hbm, live_hbm, basis_hbm, bw_hbm, up_hbm, atom_hbm]
    here_refs = [
        states.at[m], down_ref, lists_ref, in_ref, out_ref, live_ref, basis_ref, bw_ref, ups.at[m], atom_ref]
    loads = [pltpu.make_async_copy(a, b, load_sem.at[i]) for i, (a, b) in enumerate(zip(hbm, here_refs))]
    for load in loads:
        load.start()
    state_in, down_in, lists_in, in_in, out_in, live_in, basis_in, bw_in, up_in, atom_in = loads

    def mp_copy(src, dst, which, j, stage, bit):
        return pltpu.make_async_remote_copy(
            src_ref=src, dst_ref=dst, send_sem=red_send.at[which, stage], recv_sem=red_recv.at[which, j, stage],
            device_id={"mp": flip(m, bit)}, device_id_type=MESH)

    mine = pl.ds(pl.multiple_of((m % 2) * half, half), half)
    other = pl.ds(pl.multiple_of(half - (m % 2) * half, half), half)

    plan, held = gather_plan(mp)

    def other_of(off):
        index = m
        for bit in bits:
            if off & bit:
                index = flip(index, bit)
        return index

    local = [i for i, (bit, off) in enumerate(plan) if off == 0]
    relayed = [i for i, (bit, off) in enumerate(plan) if off != 0]
    brings = {bit ^ off: i for i, (bit, off) in enumerate(plan)}
    relays_from = sorted({brings[plan[i][1]] for i in relayed})

    across_y = flip(m, mp // 2)

    def early(which, i):
        bit, off = plan[i]
        at = (states, ups)[which].at[other_of(off)]
        return pltpu.make_async_remote_copy(
            src_ref=at, dst_ref=at, send_sem=early_send.at[which], recv_sem=early_recv.at[which, i],
            device_id={"mp": flip(m, bit)}, device_id_type=MESH)

    trip_half = trip // 2
    up_rows = pl.ds(pl.multiple_of((g % 2) * trip_half, trip_half), trip_half)

    def up_copy(i):
        at = ups.at[(m, across_y)[i], up_rows]
        return pltpu.make_async_remote_copy(
            src_ref=at, dst_ref=at, send_sem=up_send, recv_sem=up_recv.at[i],
            device_id=({"mp": across_y}, {"graph": flip(g, 1)})[i], device_id_type=MESH)

    def up_beside():
        up_copy(0).wait_recv()
        up_copy(1).start()

    def up_home():
        up_copy(1).wait_recv()
        for i in relayed:
            early(1, i).start()

    def early_sent(which):
        at = (states, ups)[which].at[pl.ds(0, mp - 1 - which)]
        pltpu.make_async_remote_copy(
            src_ref=at, dst_ref=at, send_sem=early_send.at[which], recv_sem=early_recv.at[which, 0],
            device_id={"mp": flip(m, 1)}, device_id_type=MESH).wait_send()

    def early_relay(which):
        for i in relayed:
            first = brings[plan[i][1]]
            if [j for j in relayed if brings[plan[j][1]] == first][0] == i:
                early(which, first).wait_recv()
            early(which, i).start()

    def early_finish(which):
        for i in range(len(plan)):
            if i not in relays_from:
                early(which, i).wait_recv()

    feeds = layers - 1
    eighth = weight.shape[1] // 8
    mine8 = g % 8

    def xor(a, k):
        for bit in (1, 2, 4):
            if k & bit:
                a = flip(a, bit)
        return a

    def part8(e):
        return pl.ds(pl.multiple_of(e * eighth, eighth), eighth)

    def feed_copy(src, f, e, sem, device):
        return pltpu.make_async_remote_copy(
            src_ref=src, dst_ref=opposite.at[f, part8(e)], send_sem=feed_send.at[f], recv_sem=sem,
            device_id=device, device_id_type=MESH)

    def enter(f, far):
        e = xor(mine8, 4 * far)
        return feed_copy(weight.at[2 * (f + 1), part8(e)], f, e, feed_y.at[f, far], {"mp": across_y})

    def hop(f):
        return feed_copy(opposite.at[f, part8(mine8)], f, mine8, feed_far.at[f], {"graph": xor(g, 4)})

    def near(f, far, k):
        e = xor(mine8, 4 * far)
        return feed_copy(opposite.at[f, part8(e)], f, e, near_recv.at[f, far, k - 1], {"graph": xor(g, k)})

    def corner(f, far):
        came, goes = (2, 1) if far == 0 else (1, 2)
        e = xor(mine8, 4 * far + came)
        return feed_copy(opposite.at[f, part8(e)], f, e, near_recv.at[f, far, 2], {"graph": xor(g, goes)})

    def feed_corner(f, far):
        near(f, far, 2 if far == 0 else 1).wait_recv()
        corner(f, far).start()

    def feed_ready(f):
        for far in range(2):
            near(f, far, 1 if far == 0 else 2).wait_recv()
            corner(f, far).wait_recv()

    def feed_sent():
        for f in range(feeds):
            at = opposite.at[f]
            pltpu.make_async_remote_copy(
                src_ref=at, dst_ref=at, send_sem=feed_send.at[f], recv_sem=near_recv.at[f, 0, 0],
                device_id={"mp": across_y}, device_id_type=MESH).wait_send()

    class Sum:
        def __init__(self, which, part, got, summed, more, full):
            self.which, self.part, self.got = which, part, got
            self.summed, self.more, self.full = summed, more, full

        def first(self, j):
            return mp_copy(self.part.at[j, other], self.got.at[j], self.which, j, 0, 1)

        def step(self, j, b):
            return mp_copy(self.summed.at[j, b], self.more.at[j, b], self.which, j, 1 + b, bits[1 + b])

        def last(self, j):
            at = self.full.at[j, mine]
            return mp_copy(at, at, self.which, j, stages, 1)

        def into(self, j):
            self.first(j).start()

        def across(self, j):
            self.first(j).wait_recv()
            total = self.part[j, mine].astype(f32) + self.got[j].astype(f32)
            if stages > 1:
                self.summed[j, 0] = total.astype(bf16)
                self.step(j, 0).start()
            else:
                self.full[j, mine] = total.astype(bf16)

        def home(self, j):
            for b in range(stages - 1):
                self.step(j, b).wait_recv()
                total = self.summed[j, b].astype(f32) + self.more[j, b].astype(f32)
                if b + 2 < stages:
                    self.summed[j, b + 1] = total.astype(bf16)
                    self.step(j, b + 1).start()
                else:
                    self.full[j, mine] = total.astype(bf16)
            self.last(j).start()

        def done(self, j):
            self.last(j).wait_recv()

        def drain(self):
            for stage in range(stages + 1):
                mp_copy(self.got, self.got, self.which, 0, stage, 1).wait_send()

    sum0 = Sum(0, part_a, got_a, sum_a, more_a, full_a)
    sum1 = Sum(1, part_b, got_b, sum_b, more_b, full_b)

    def peer_of(k):
        if graph & (graph - 1):
            return (g + k) % graph
        return sum(bit * ((g // bit + k // bit) % 2) for bit in (1 << i for i in range(graph.bit_length() - 1)))

    peers = [peer_of(k) for k in range(graph - 1, 0, -1)] if graph <= 8 else None

    def arrived(whole, group, which):
        return pltpu.make_async_remote_copy(
            src_ref=whole, dst_ref=whole, send_sem=xc_send.at[group], recv_sem=xc_recv.at[which],
            device_id={"graph": (g + 1) % graph}, device_id_type=MESH)

    def exchange(group, which, src_at, dst_at, whole):
        def to(peer):
            pltpu.make_async_remote_copy(
                src_ref=src_at(peer), dst_ref=dst_at(g), send_sem=xc_send.at[group], recv_sem=xc_recv.at[which],
                device_id={"graph": peer}, device_id_type=MESH).start()

        def one(i, _):
            to(peer_of(graph - 1 - i))
            return 0

        def start():
            if peers is None:
                lax.fori_loop(0, graph - 1, one, 0)
            else:
                for peer in peers:
                    to(peer)

        return start, arrived(whole, group, which).wait_recv

    def block(ref, size):
        return lambda i: ref.at[pl.ds(pl.multiple_of(i * size, size), size)]

    def piece(ref, j, size):
        return lambda i: ref.at[j, pl.ds(pl.multiple_of(i * size, size), size)]

    def tiles(step):
        def one(i, _):
            step(pl.ds(pl.multiple_of(i * tile, tile), tile))
            return 0

        lax.fori_loop(0, triplets // tile, one, 0)

    def in_part(at):
        return one_hot(slot_total, in_ref[:, at])

    def out_part(at):
        return one_hot(slot_total, jnp.where(live_ref[:, at] > 0, out_ref[:, at], -1))

    state_in.wait()
    down_in.wait()
    with scope("s_proj"):
        projected = dot(states[m], down_ref[...]).astype(bf16)
        for j in range(pieces):
            part_a[j] = projected[:, j * lane:(j + 1) * lane]
    with scope("s_barrier"):
        pl.semaphore_wait(barrier, graph - 1 + len(bits))
    for j in range(pieces):
        sum0.into(j)
    load = pltpu.make_async_copy(dense_hbm, weight, weight_sem)
    load.start()

    lists_in.wait()
    with scope("s_hots"):
        for i in range(graph):
            list_hot[:, i * cap:(i + 1) * cap] = one_hot(rows, lists_ref[0, i:i + 1, :])
        in_in.wait()
        if kept:
            def keep_in(at):
                in_hot[:, at] = in_part(at)

            tiles(keep_in)
    with scope("s_across"):
        for j in range(pieces):
            sum0.across(j)
    up_in.wait()
    early(0, local[0]).start()
    out_in.wait()
    live_in.wait()
    if kept:
        def keep_out(at):
            out_hot[:, at] = out_part(at)

        with scope("s_outhot"):
            tiles(keep_out)

    basis_in.wait()
    bw_in.wait()
    depth = basis_ref.shape[0]
    pad = basis_stack.shape[0] // 3
    with scope("s_angles"):
        bw_high, bw_low = halves(bw_ref[...])
        bw_stack[...] = jnp.zeros_like(bw_stack)
        bw_stack[0:depth] = bw_high
        bw_stack[pad:pad + depth] = bw_high
        bw_stack[2 * pad:2 * pad + depth] = bw_low

        def angles(at):
            high, low = halves(basis_ref[:, at])
            basis_stack[:, at] = jnp.zeros((3 * pad, tile), bf16)
            basis_stack[0:depth, at] = high
            basis_stack[pad:pad + depth, at] = low
            basis_stack[2 * pad:2 * pad + depth, at] = high
            angle[:, at] = dot(bw_stack[...], basis_stack[:, at], 0, 0)

        tiles(angles)

    load.wait()
    if feeds:
        enter(0, 0).start()
    up_copy(0).start()
    for f in range(1, feeds):
        enter(f, 0).start()
    step_rows = min(slot_total, 512)
    own = pl.ds(pl.multiple_of(g * cap, cap), cap)
    span = pl.ds(0, slot_total - cap)
    going = [exchange(0, j, piece(to_a, j, cap), piece(from_a, j, cap), from_a.at[j, span]) for j in range(pieces)]
    back = [exchange(1, pieces + j, piece(to_b, j, cap), piece(from_b, j, cap), from_b.at[j, span])
            for j in range(pieces)]

    def pick_piece(j):
        def pick(i, _):
            at = pl.ds(pl.multiple_of(i * step_rows, step_rows), step_rows)
            to_a[j, at, :] = dot(list_hot[:, at], full_a[j], 0, 0).astype(bf16)
            return 0

        sum0.done(j)
        lax.fori_loop(0, slot_total // step_rows, pick, 0)
        going[j][0]()
        from_a[j, own] = to_a[j, own]

    with scope("s_home"):
        sum0.home(0)
    with scope("s_home1"):
        for j in range(1, pieces):
            sum0.home(j)
            pick_piece(j - 1)
        pick_piece(pieces - 1)
    for which in range(2):
        for i in local[1:]:
            early(which, i).start()
    sum0.drain()

    for j in range(pieces):
        with scope("s_gowait%d" % j):
            going[j][1]()
        slots[...] = jnp.zeros_like(slots)
        received = from_a[j].astype(f32).T.astype(bf16)

        def trips(at):
            source = in_hot[:, at] if kept else in_part(at)
            value = dot(received, source) * angle[j * lane:(j + 1) * lane, at]
            target = out_hot[:, at] if kept else out_part(at)
            slots[...] += dot(target, value.astype(bf16), 1, 1)

        with scope("s_trips%d" % j):
            tiles(trips)
        to_b[j] = slots[...].astype(bf16)
        back[j][0]()
        from_b[j, own] = to_b[j, own]
    with scope("s_early0"):
        early_relay(0)
    with scope("s_upbeside"):
        up_beside()

    def add_up(j):
        for index in range(mp):
            rest = dot(full_b[j], ups[index, j * lane:(j + 1) * lane, :])
            partial[index] = (states[index].astype(f32) if j == 0 else partial[index]) + rest

    for j in range(pieces):
        with scope("s_backwait%d" % j):
            back[j][1]()
        part_b[j] = dot(list_hot[...], from_b[j]).astype(bf16)
        sum1.into(j)
        if j + 1 < pieces:
            sum1.across(j)
    with scope("s_sum1"):
        sum1.across(pieces - 1)
        with scope("s_early1"):
            up_home()
        with scope("s_feedspread"):
            if feeds:
                enter(0, 0).wait_recv()
                near(0, 0, 2).start()
                near(0, 0, 1).start()
                hop(0).start()
        for j in range(pieces - 2):
            sum1.home(j)
        early_finish(0)
        early_finish(1)
        if pieces > 1:
            sum1.home(pieces - 2)
        for j in range(pieces - 1):
            sum1.done(j)
            add_up(j)
        with scope("s_lasthome"):
            sum1.home(pieces - 1)

    starts, sizes = chunks_of(half)
    order = [(h, t) for t in range(len(sizes)) for h in (0, 1)]

    def chunk(c):
        side, t = c
        start = side * half + starts[t]
        return pl.ds(start if isinstance(side, int) else pl.multiple_of(start, half // 2), sizes[t])

    def chunk_id(c):
        return c[0] * len(sizes) + c[1]

    def act_copy(layer, parity, c, which):
        bit, off = plan[which]
        at = acts.at[layer - 1, other_of(off), chunk(c)]
        return pltpu.make_async_remote_copy(
            src_ref=at, dst_ref=at,
            send_sem=act_send.at[parity, chunk_id(c)], recv_sem=act_recv.at[parity, chunk_id(c), which],
            device_id={"mp": flip(m, bit)}, device_id_type=MESH)

    def send(layer, parity, c):
        for i in local:
            act_copy(layer, parity, c, i).start()

    def relay(layer, parity, c):
        for i in relayed:
            first = brings[plan[i][1]]
            if [j for j in relayed if brings[plan[j][1]] == first][0] == i:
                act_copy(layer, parity, c, first).wait_recv()
            act_copy(layer, parity, c, i).start()

    def finish(layer, parity, c):
        for i in range(len(plan)):
            if i not in relays_from:
                act_copy(layer, parity, c, i).wait_recv()

    def sent(layer, parity, c):
        at = acts.at[layer - 1, pl.ds(0, mp - 1), chunk(c)]
        pltpu.make_async_remote_copy(
            src_ref=at, dst_ref=at, send_sem=act_send.at[parity, chunk_id(c)], recv_sem=act_recv.at[parity, chunk_id(c), 0],
            device_id={"mp": flip(m, 1)}, device_id_type=MESH).wait_send()

    def product(k, at, held_weight):
        total = None
        for off in held:
            index = other_of(off)
            term = dot(acts[k - 1, index, at, :], held_weight[pl.ds(pl.multiple_of(index * width, width), width), :])
            total = term if total is None else total + term
        return silu(total)

    def core_copy(layer, c, i):
        at = acts.at[layer - 1, (m, across_y)[i], chunk(c)]
        return pltpu.make_async_remote_copy(
            src_ref=at, dst_ref=at, send_sem=core_send.at[chunk_id(c)], recv_sem=core_recv.at[chunk_id(c), i],
            device_id={"mp": flip(m, 1)}, device_id_type=MESH)

    def core_sent(layer, c):
        at = acts.at[layer - 1, pl.ds(0, 2), chunk(c)]
        pltpu.make_async_remote_copy(
            src_ref=at, dst_ref=at, send_sem=core_send.at[chunk_id(c)], recv_sem=core_recv.at[chunk_id(c), 0],
            device_id={"mp": flip(m, 1)}, device_id_type=MESH).wait_send()

    last_up = (pieces - 1) * lane
    with scope("s_begin"):
        for spot in range(len(order)):
            c = (m % 2 if spot % 2 == 0 else 1 - m % 2), spot // 2
            at = chunk(c)
            if spot == 1:
                sum1.done(pieces - 1)
            if spot == 3 and feeds:
                with scope("s_corner00"):
                    feed_corner(0, 0)
                    for f in range(1, feeds):
                        enter(f, 0).wait_recv()
                        near(f, 0, 2).start()
            total = None
            for index in range(mp):
                before = partial[index, at] if pieces > 1 else states[index, at].astype(f32)
                first = before + dot(full_b[pieces - 1, at], ups[index, last_up:last_up + lane, :])
                partial[index, at] = first
                term = dot(first.astype(bf16), weight[0, index * width:(index + 1) * width, :])
                total = term if total is None else total + term
            hidden[at, :] = partial[m, at]
            acts[0, m, at, :] = silu(total).astype(bf16)
            send(1, 0, c)
        sum1.drain()
        arrived(from_a.at[:, span], 0, 0).wait_send()
        arrived(from_b.at[:, span], 1, 0).wait_send()
        for which in range(2):
            early_sent(which)
        pltpu.make_async_remote_copy(
            src_ref=ups.at[m], dst_ref=ups.at[m], send_sem=up_send, recv_sem=up_recv.at[0],
            device_id={"mp": across_y}, device_id_type=MESH).wait_send()
    def update(k, c):
        at = chunk(c)
        value = (hidden[at, :] + product(k, at, weight.at[k])) * inv_root_two
        hidden[at, :] = value
        return value.astype(bf16)

    with scope("s_layer0"):
        with scope("s_feedrest0"):
            for f in range(1, feeds):
                enter(f, 1).start()
            if feeds:
                hop(0).wait_recv()
                near(0, 1, 1).start()
                near(0, 1, 2).start()
        with scope("s_l0rel"):
            relay(1, 0, order[0])
        for spot, c in enumerate(order):
            with scope("s_l0fin%d" % spot):
                finish(1, 0, c)
            with scope("s_l0rel%d" % spot):
                if spot + 1 < len(order):
                    relay(1, 0, order[spot + 1])
            value = update(1, c)
            if layers > 1:
                acts[1, m, chunk(c), :] = value
                send(2, 1, c)
            with scope("s_l0feed%d" % spot):
                if spot == 1 and feeds:
                    feed_corner(0, 1)
                    for f in range(1, feeds):
                        near(f, 0, 1).start()
                if spot == 2:
                    for f in range(1, feeds):
                        feed_corner(f, 0)
        if layers > 1:
            with scope("s_l1rel"):
                relay(2, 1, order[0])
        with scope("s_feedrest1"):
            for f in range(1, feeds):
                enter(f, 1).wait_recv()
                near(f, 1, 1).start()
                near(f, 1, 2).start()

    def layer_step(l, _):
        k, parity, f = 2 * l, l % 2, l - 1

        def second(c):
            for i in range(2):
                core_copy(k + 1, c, i).wait_recv()
            value = update(k + 1, c)

            @pl.when(l + 1 < layers)
            def _():
                sent(k, 1 - parity, c)
                acts[k + 1, m, chunk(c), :] = value
                send(k + 2, 1 - parity, c)

        with scope("s_feedwait"):
            feed_ready(f)
        for spot, c in enumerate(order):
            at = chunk(c)
            with scope("s_fin%d" % spot):
                finish(k, parity, c)

            @pl.when(l > 1)
            def _():
                core_sent(k - 1, c)

            acts[k, m, at, :] = product(k, at, weight.at[k]).astype(bf16)
            core_copy(k + 1, c, 0).start()
            with scope("s_rel%d" % spot):
                if spot + 1 < len(order):
                    relay(k, parity, order[spot + 1])
            acts[k, across_y, at, :] = product(k, at, opposite.at[f]).astype(bf16)
            core_copy(k + 1, c, 1).start()
            if spot >= 1:
                with scope("s_second%d" % spot):
                    second(order[spot - 1])
            if spot == 1:
                @pl.when(l == 1)
                def _():
                    with scope("s_corner11"):
                        for later in range(1, feeds):
                            feed_corner(later, 1)

        @pl.when(l + 1 < layers)
        def _():
            with scope("s_relnext"):
                relay(k + 2, 1 - parity, order[0])

        with scope("s_second_last"):
            second(order[-1])
        return 0

    with scope("s_layers"):
        lax.fori_loop(1, layers, layer_step, 0)

    atom_in.wait()
    atom_rows = min(atoms, 256)
    parts, part_lane = table.shape[0], table.shape[2]
    here = pl.ds(pl.multiple_of(g * ATOM_DEV, ATOM_DEV), ATOM_DEV)
    atom_span = pl.ds(0, atoms - ATOM_DEV)
    gathers = [exchange(2, 2 * pieces + p, piece(atoms_to, p, ATOM_DEV), piece(atoms_from, p, ATOM_DEV),
                        atoms_from.at[p, atom_span]) for p in range(parts)]
    spreads = [exchange(3, 2 * pieces + parts + p, lambda peer, p=p: piece(table, p, ATOM_DEV)(g),
                        piece(table, p, ATOM_DEV), table.at[p, atom_span]) for p in range(parts)]

    def columns(p):
        return slice(p * part_lane, (p + 1) * part_lane)

    with scope("s_collect"):
        def collect(i, _):
            at = pl.ds(pl.multiple_of(i * atom_rows, atom_rows), atom_rows)
            ids = one_hot(atom_rows, atom_ref[...] - i * atom_rows)
            high, low = halves(hidden[...])
            total = dot(ids, high) + dot(ids, low)
            for p in range(parts):
                atoms_own[p, at] = total[:, columns(p)]
                atoms_to[p, at] = total[:, columns(p)].astype(bf16)
            return 0

        lax.fori_loop(0, atoms // atom_rows, collect, 0)
        for p in range(parts):
            gathers[p][0]()
    for p in range(parts):
        atoms_from[p, here] = jnp.zeros((ATOM_DEV, part_lane), bf16)
    for c in order:
        sent(1, (layers - 1) % 2, c)
        if layers > 1:
            sent(1, layers % 2, c)
            core_sent(1, c)
    feed_sent()
    for p in range(parts):
        with scope("s_atomwait%d" % p):
            gathers[p][1]()

        def add(i, total):
            return total + atoms_from[p, pl.ds(pl.multiple_of(i * ATOM_DEV, ATOM_DEV), ATOM_DEV)].astype(f32)

        total = lax.fori_loop(0, graph, add, atoms_own[p, here])
        mine_out = silu(atom_scale * total).astype(bf16)
        table[p, here] = mine_out
        spreads[p][0]()
        atom_out_ref[:, columns(p)] = mine_out
    arrived(atoms_from.at[:, atom_span], 2, 0).wait_send()
    for p in range(parts):
        with scope("s_spreadwait%d" % p):
            spreads[p][1]()

        def spread(i, total):
            at = pl.ds(pl.multiple_of(i * atom_rows, atom_rows), atom_rows)
            return total + dot(one_hot(atom_rows, atom_ref[...] - i * atom_rows), table[p, at], 0, 0)

        total = lax.fori_loop(0, atoms // atom_rows, spread, hidden[:, columns(p)])
        edge_out_ref[:, columns(p)] = total.astype(bf16)
    arrived(table.at[:, atom_span], 3, 0).wait_send()


def hand_on(edge_ref, atom_ref, edge_out_ref, atom_out_ref, sem):
    edge = pltpu.make_async_copy(edge_ref, edge_out_ref, sem.at[0])
    atom = pltpu.make_async_copy(atom_ref, atom_out_ref, sem.at[1])
    edge.start()
    atom.start()
    edge.wait()
    atom.wait()


def local(graph, mp, edge_state, down_weight, basis, basis_weight, up_weight, dense_weight,
          send_rows, trip_in, trip_out, trip_live, edge_atom):
    rows, width = edge_state.shape
    trip = down_weight.shape[1]
    slot_total = graph * send_rows.shape[2]
    triplets = trip_in.shape[0]
    maps = dense_weight.shape[0] * dense_weight.shape[1]
    tile = 2048 if slot_total <= 512 else 128
    atoms = graph * ATOM_DEV
    feeds = max(dense_weight.shape[0] - 1, 1)
    chunks = 2 * len(chunks_of(rows // 2)[1])
    stages = mp.bit_length()
    extra = max(stages - 2, 1)
    half = rows // 2
    vmem = pltpu.VMEM
    pieces = trip // 128 if trip % 128 == 0 else 1
    lane = trip // pieces
    pad = -(-basis.shape[0] // 16) * 16
    hot_bytes = 2 * 2 * slot_total * triplets
    hots = [vmem((slot_total, triplets), bf16)] * 2 if hot_bytes <= 2 ** 24 else [None, None]
    reduce_bufs = [
        vmem((pieces, rows, lane), bf16), vmem((pieces, half, lane), bf16), vmem((pieces, extra, half, lane), bf16),
        vmem((pieces, extra, half, lane), bf16), vmem((pieces, rows, lane), bf16),
    ]
    dma = pltpu.SemaphoreType.DMA
    spec = pl.BlockSpec(memory_space=pltpu.VMEM)
    operands = [
        edge_state, down_weight, basis, basis_weight, up_weight,
        dense_weight.reshape((maps,) + dense_weight.shape[2:]),
        send_rows, trip_in.reshape(1, triplets), trip_out.reshape(1, triplets),
        trip_live.reshape(1, triplets), edge_atom.reshape(1, rows),
    ]
    inputs = [vmem(a.shape, a.dtype) for i, a in enumerate(operands) if i not in (0, 4, 5)]
    parts = width // 128 if width % 128 == 0 else 1
    atom_buf = (parts, atoms, width // parts)
    body = functools.partial(kernel, graph, mp, tile)
    before = [
        *inputs, dma((len(inputs) + 2,)),
        vmem((mp, rows, width), bf16), vmem((mp, trip, width), bf16), dma((2,)), dma((2, mp - 1)), dma(()), dma((2,)),
        vmem((maps,) + dense_weight.shape[2:], bf16), dma(()),
        vmem((feeds,) + dense_weight.shape[2:], bf16), dma((feeds,)), dma((feeds, 2)), dma((feeds,)), dma((feeds, 2, 3)),
        dma((chunks,)), dma((chunks, 2)),
        *reduce_bufs, *reduce_bufs,
        dma((2, stages)), dma((2, pieces, stages)),
        *[vmem((pieces, slot_total, lane), bf16)] * 4,
        dma((4,)), dma((2 * pieces + 2 * parts,)),
        vmem((rows, slot_total), bf16), vmem((3 * pad, triplets), bf16), vmem((3 * pad, trip), bf16),
        vmem((trip, triplets), f32), vmem((slot_total, lane), f32),
    ]
    if hots[0] is None:
        hots, kept_body, at = [], body, len(operands) + 2 + len(before)
        body = lambda *refs: kept_body(*refs[:at], None, None, *refs[at:])
    outs = pl.pallas_call(
        body,
        out_shape=(
            pltpu.VMEM((rows, width), bf16),
            pltpu.VMEM((ATOM_DEV, width), bf16),
        ),
        in_specs=[pl.BlockSpec(memory_space=pl.ANY)] * len(operands),
        out_specs=(spec, spec),
        scratch_shapes=[
            *before, *hots,
            vmem((maps - 1, mp, rows, width), bf16), vmem((mp, rows, width), f32), vmem((rows, width), f32),
            dma((2, chunks)), dma((2, chunks, mp - 1)),
            vmem(atom_buf, f32), vmem(atom_buf, bf16), vmem(atom_buf, bf16), vmem(atom_buf, bf16),
        ],
        compiler_params=pltpu.CompilerParams(
            collective_id=0, has_side_effects=True, vmem_limit_bytes=64000 * 1024
        ),
        name="edge_block",
    )(*operands)
    outs = [pltpu.with_memory_space_constraint(o, pltpu.VMEM) for o in outs]
    return pl.pallas_call(
        hand_on,
        out_shape=tuple(jax.ShapeDtypeStruct(o.shape, o.dtype) for o in outs),
        in_specs=[spec] * 2,
        out_specs=[pl.BlockSpec(memory_space=pl.ANY)] * 2,
        scratch_shapes=[dma((2,))],
        name="hand_on",
    )(*outs)


def solution(mesh):
    in_specs = (
        P("graph", "mp"),
        P("mp", None),
        P(None, ("graph", "mp")),
        P(),
        P(None, "mp"),
        P(None, None, None, "mp"),
        P("graph", "mp", None),
        P(("graph", "mp")),
        P(("graph", "mp")),
        P(("graph", "mp")),
        P("graph"),
    )
    out_specs = (P("graph", "mp"), P("graph", "mp"))
    body = functools.partial(local, mesh.shape["graph"], mesh.shape["mp"])
    return jax.shard_map(body, mesh=mesh, in_specs=in_specs, out_specs=out_specs, check_vma=False)
```

```python
import functools

import jax
import jax.numpy as jnp
from jax import lax
from jax.experimental import pallas as pl
from jax.experimental.pallas import tpu as pltpu
from jax.sharding import PartitionSpec as P

ATOM_DEV = 32

inv_root_two = 0.7071067811865476
atom_scale = 0.2

MESH = pl.DeviceIdType.MESH
bf16 = jnp.bfloat16
f32 = jnp.float32


def scope(name):
    return jax.named_scope(name)


def silu(v):
    return v / (1.0 + jnp.exp(-v))


def flip(index, bit):
    return index + bit - 2 * bit * ((index // bit) % 2)


def one_hot(rows, ids):
    shape = (rows, ids.shape[1])
    return jnp.where(lax.broadcasted_iota(jnp.int32, shape, 0) == ids, 1.0, 0.0).astype(bf16)


def dot(a, b, ca=1, cb=0):
    return lax.dot_general(a, b, (((ca,), (cb,)), ((), ())), preferred_element_type=f32)


def halves(v):
    high = v.astype(bf16)
    return high, (v - high.astype(f32)).astype(bf16)


def chunks_of(half):
    return (0, half // 2), (half // 2, half // 2)


def gather_plan(mp):
    plan, held, bit = [], [0], mp // 2
    while bit >= 1:
        plan += [(bit, off) for off in held]
        held += [bit ^ off for off in held]
        bit //= 2
    return plan, held


def kernel(
    graph, mp, tile,
    state_hbm, down_hbm, basis_hbm, bw_hbm, up_hbm, dense_hbm, lists_hbm, in_hbm, out_hbm, live_hbm, atom_hbm,
    edge_out_ref, atom_out_ref,
    down_ref, basis_ref, bw_ref, lists_ref, in_ref, out_ref, live_ref, atom_ref, load_sem,
    states, ups, early_send, early_recv, up_send, up_recv,
    weight, joint, weight_sem, feed_send, feed_y, feed_far, near_recv, core_send, core_recv,
    part_a, got_a, sum_a, more_a, full_a,
    part_b, got_b, sum_b, more_b, full_b,
    red_send, red_recv,
    to_a, from_a, to_b, from_b, xc_send, xc_recv,
    list_hot, basis_stack, bw_stack, angle, slots, in_hot, out_hot,
    acts, partial, hidden, act_send, act_recv,
    atoms_own, atoms_to, atoms_from, table,
):
    g = lax.axis_index("graph")
    m = lax.axis_index("mp")
    rows, width = hidden.shape
    trip = down_ref.shape[1]
    layers = weight.shape[0] - 1
    cap = lists_ref.shape[2]
    slot_total = graph * cap
    pieces, lane = to_a.shape[0], to_a.shape[2]
    kept = in_hot is not None
    triplets = in_ref.shape[1]
    atoms = graph * ATOM_DEV
    half = rows // 2
    feeds = layers - 1
    bits = [1 << i for i in range(mp.bit_length() - 1)]
    stages = len(bits)

    barrier = pltpu.get_barrier_semaphore()

    def greet(k, _):
        pl.semaphore_signal(barrier, inc=1, device_id={"graph": (g + k) % graph}, device_id_type=MESH)
        return 0

    lax.fori_loop(1, graph, greet, 0)
    for bit in bits:
        pl.semaphore_signal(barrier, inc=1, device_id={"mp": flip(m, bit)}, device_id_type=MESH)

    hbm = [state_hbm, down_hbm, lists_hbm, in_hbm, out_hbm, live_hbm, basis_hbm, bw_hbm, up_hbm, atom_hbm]
    here_refs = [
        states.at[m], down_ref, lists_ref, in_ref, out_ref, live_ref, basis_ref, bw_ref, ups.at[m], atom_ref]
    loads = [pltpu.make_async_copy(a, b, load_sem.at[i]) for i, (a, b) in enumerate(zip(hbm, here_refs))]
    for load in loads:
        load.start()
    state_in, down_in, lists_in, in_in, out_in, live_in, basis_in, bw_in, up_in, atom_in = loads

    def mp_copy(src, dst, which, j, stage, bit):
        return pltpu.make_async_remote_copy(
            src_ref=src, dst_ref=dst, send_sem=red_send.at[which, stage], recv_sem=red_recv.at[which, j, stage],
            device_id={"mp": flip(m, bit)}, device_id_type=MESH)

    mine = pl.ds(pl.multiple_of((m % 2) * half, half), half)
    other = pl.ds(pl.multiple_of(half - (m % 2) * half, half), half)

    plan, held = gather_plan(mp)

    def other_of(off):
        index = m
        for bit in bits:
            if off & bit:
                index = flip(index, bit)
        return index

    local = [i for i, (bit, off) in enumerate(plan) if off == 0]
    relayed = [i for i, (bit, off) in enumerate(plan) if off != 0]
    brings = {bit ^ off: i for i, (bit, off) in enumerate(plan)}
    relays_from = sorted({brings[plan[i][1]] for i in relayed})

    across_y = flip(m, mp // 2)

    def early(which, i):
        bit, off = plan[i]
        at = (states, ups)[which].at[other_of(off)]
        return pltpu.make_async_remote_copy(
            src_ref=at, dst_ref=at, send_sem=early_send.at[which], recv_sem=early_recv.at[which, i],
            device_id={"mp": flip(m, bit)}, device_id_type=MESH)

    trip_half = trip // 2
    up_rows = pl.ds(pl.multiple_of((g % 2) * trip_half, trip_half), trip_half)

    def up_copy(i):
        at = ups.at[(m, across_y)[i], up_rows]
        return pltpu.make_async_remote_copy(
            src_ref=at, dst_ref=at, send_sem=up_send, recv_sem=up_recv.at[i],
            device_id=({"mp": across_y}, {"graph": flip(g, 1)})[i], device_id_type=MESH)

    def up_beside():
        up_copy(0).wait_recv()
        up_copy(1).start()

    def up_home():
        up_copy(1).wait_recv()
        for i in relayed:
            early(1, i).start()

    def early_sent(which):
        at = (states, ups)[which].at[pl.ds(0, mp - 1 - which)]
        pltpu.make_async_remote_copy(
            src_ref=at, dst_ref=at, send_sem=early_send.at[which], recv_sem=early_recv.at[which, 0],
            device_id={"mp": flip(m, 1)}, device_id_type=MESH).wait_send()

    def early_relay(which):
        for i in relayed:
            first = brings[plan[i][1]]
            if [j for j in relayed if brings[plan[j][1]] == first][0] == i:
                early(which, first).wait_recv()
            early(which, i).start()

    def early_finish(which):
        for i in range(len(plan)):
            if i not in relays_from:
                early(which, i).wait_recv()

    eighth = weight.shape[1] // 8
    mine8 = g % 8

    def xor(a, k):
        for bit in (1, 2, 4):
            if k & bit:
                a = flip(a, bit)
        return a

    def part8(e):
        return pl.ds(pl.multiple_of(e * eighth, eighth), eighth)

    def feed_copy(src, f, e, sem, device):
        return pltpu.make_async_remote_copy(
            src_ref=src, dst_ref=joint.at[f, part8(e), far_cols], send_sem=feed_send.at[f], recv_sem=sem,
            device_id=device, device_id_type=MESH)

    def enter(f, far):
        e = xor(mine8, 4 * far)
        return feed_copy(joint.at[f, part8(e), own_cols], f, e, feed_y.at[f, far], {"mp": across_y})

    def hop(f):
        return feed_copy(joint.at[f, part8(mine8), far_cols], f, mine8, feed_far.at[f], {"graph": xor(g, 4)})

    def near(f, far, k):
        e = xor(mine8, 4 * far)
        return feed_copy(joint.at[f, part8(e), far_cols], f, e, near_recv.at[f, far, k - 1], {"graph": xor(g, k)})

    def corner(f, far):
        came, goes = (2, 1) if far == 0 else (1, 2)
        e = xor(mine8, 4 * far + came)
        return feed_copy(joint.at[f, part8(e), far_cols], f, e, near_recv.at[f, far, 2], {"graph": xor(g, goes)})

    def feed_corner(f, far):
        near(f, far, 2 if far == 0 else 1).wait_recv()
        corner(f, far).start()

    def feed_ready(f):
        for far in range(2):
            near(f, far, 1 if far == 0 else 2).wait_recv()
            corner(f, far).wait_recv()

    def feed_sent():
        for f in range(feeds):
            at = joint.at[f, :, far_cols]
            pltpu.make_async_remote_copy(
                src_ref=at, dst_ref=at, send_sem=feed_send.at[f], recv_sem=near_recv.at[f, 0, 0],
                device_id={"mp": across_y}, device_id_type=MESH).wait_send()

    class Sum:
        def __init__(self, which, part, got, summed, more, full):
            self.which, self.part, self.got = which, part, got
            self.summed, self.more, self.full = summed, more, full

        def first(self, j):
            return mp_copy(self.part.at[j, other], self.got.at[j], self.which, j, 0, 1)

        def step(self, j, b):
            return mp_copy(self.summed.at[j, b], self.more.at[j, b], self.which, j, 1 + b, bits[1 + b])

        def last(self, j):
            at = self.full.at[j, mine]
            return mp_copy(at, at, self.which, j, stages, 1)

        def into(self, j):
            self.first(j).start()

        def across(self, j):
            self.first(j).wait_recv()
            total = self.part[j, mine].astype(f32) + self.got[j].astype(f32)
            if stages > 1:
                self.summed[j, 0] = total.astype(bf16)
                self.step(j, 0).start()
            else:
                self.full[j, mine] = total.astype(bf16)

        def home(self, j):
            for b in range(stages - 1):
                self.step(j, b).wait_recv()
                total = self.summed[j, b].astype(f32) + self.more[j, b].astype(f32)
                if b + 2 < stages:
                    self.summed[j, b + 1] = total.astype(bf16)
                    self.step(j, b + 1).start()
                else:
                    self.full[j, mine] = total.astype(bf16)
            self.last(j).start()

        def done(self, j):
            self.last(j).wait_recv()

        def drain(self):
            for stage in range(stages + 1):
                mp_copy(self.got, self.got, self.which, 0, stage, 1).wait_send()

    sum0 = Sum(0, part_a, got_a, sum_a, more_a, full_a)
    sum1 = Sum(1, part_b, got_b, sum_b, more_b, full_b)

    def peer_of(k):
        if graph & (graph - 1):
            return (g + k) % graph
        return sum(bit * ((g // bit + k // bit) % 2) for bit in (1 << i for i in range(graph.bit_length() - 1)))

    peers = [peer_of(k) for k in range(graph - 1, 0, -1)] if graph <= 8 else None

    def arrived(whole, group, which):
        return pltpu.make_async_remote_copy(
            src_ref=whole, dst_ref=whole, send_sem=xc_send.at[group], recv_sem=xc_recv.at[which],
            device_id={"graph": (g + 1) % graph}, device_id_type=MESH)

    def exchange(group, which, src_at, dst_at, whole):
        def to(peer):
            pltpu.make_async_remote_copy(
                src_ref=src_at(peer), dst_ref=dst_at(g), send_sem=xc_send.at[group], recv_sem=xc_recv.at[which],
                device_id={"graph": peer}, device_id_type=MESH).start()

        def one(i, _):
            to(peer_of(graph - 1 - i))
            return 0

        def start():
            if peers is None:
                lax.fori_loop(0, graph - 1, one, 0)
            else:
                for peer in peers:
                    to(peer)

        return start, arrived(whole, group, which).wait_recv

    def block(ref, size):
        return lambda i: ref.at[pl.ds(pl.multiple_of(i * size, size), size)]

    def piece(ref, j, size):
        return lambda i: ref.at[j, pl.ds(pl.multiple_of(i * size, size), size)]

    def tiles(step):
        def one(i, _):
            step(pl.ds(pl.multiple_of(i * tile, tile), tile))
            return 0

        lax.fori_loop(0, triplets // tile, one, 0)

    def in_part(at):
        return one_hot(slot_total, in_ref[:, at])

    def out_part(at):
        return one_hot(slot_total, jnp.where(live_ref[:, at] > 0, out_ref[:, at], -1))

    state_in.wait()
    down_in.wait()
    with scope("s_proj"):
        projected = dot(states[m], down_ref[...]).astype(bf16)
        for j in range(pieces):
            part_a[j] = projected[:, j * lane:(j + 1) * lane]
    with scope("s_barrier"):
        pl.semaphore_wait(barrier, graph - 1 + len(bits))
    for j in range(pieces):
        sum0.into(j)
    own_cols, far_cols = pl.ds(0, width), pl.ds(width, width)
    places = [(0, weight.at[0])] + [(2 * l + 1, weight.at[1 + l]) for l in range(layers)]
    places += [(2 * f + 2, joint.at[f, :, own_cols]) for f in range(feeds)]
    loads_of_maps = [pltpu.make_async_copy(dense_hbm.at[k], at, weight_sem.at[k]) for k, at in places]
    for load in loads_of_maps:
        load.start()

    lists_in.wait()
    with scope("s_hots"):
        for i in range(graph):
            list_hot[:, i * cap:(i + 1) * cap] = one_hot(rows, lists_ref[0, i:i + 1, :])
        in_in.wait()
        if kept:
            def keep_in(at):
                in_hot[:, at] = in_part(at)

            tiles(keep_in)
    with scope("s_across"):
        for j in range(pieces):
            sum0.across(j)
    up_in.wait()
    early(0, local[0]).start()
    out_in.wait()
    live_in.wait()
    if kept:
        def keep_out(at):
            out_hot[:, at] = out_part(at)

        with scope("s_outhot"):
            tiles(keep_out)

    basis_in.wait()
    bw_in.wait()
    depth = basis_ref.shape[0]
    pad = basis_stack.shape[0] // 3
    with scope("s_angles"):
        bw_high, bw_low = halves(bw_ref[...])
        bw_stack[...] = jnp.zeros_like(bw_stack)
        bw_stack[0:depth] = bw_high
        bw_stack[pad:pad + depth] = bw_high
        bw_stack[2 * pad:2 * pad + depth] = bw_low

        def angles(at):
            high, low = halves(basis_ref[:, at])
            basis_stack[:, at] = jnp.zeros((3 * pad, tile), bf16)
            basis_stack[0:depth, at] = high
            basis_stack[pad:pad + depth, at] = low
            basis_stack[2 * pad:2 * pad + depth, at] = high
            angle[:, at] = dot(bw_stack[...], basis_stack[:, at], 0, 0)

        tiles(angles)

    for load in loads_of_maps:
        load.wait()
    if feeds:
        enter(0, 0).start()
    up_copy(0).start()
    for f in range(1, feeds):
        enter(f, 0).start()
    step_rows = min(slot_total, 512)
    own = pl.ds(pl.multiple_of(g * cap, cap), cap)
    span = pl.ds(0, slot_total - cap)
    going = [exchange(0, j, piece(to_a, j, cap), piece(from_a, j, cap), from_a.at[j, span]) for j in range(pieces)]
    back = [exchange(1, pieces + j, piece(to_b, j, cap), piece(from_b, j, cap), from_b.at[j, span])
            for j in range(pieces)]

    def pick_piece(j):
        def pick(i, _):
            at = pl.ds(pl.multiple_of(i * step_rows, step_rows), step_rows)
            to_a[j, at, :] = dot(list_hot[:, at], full_a[j], 0, 0).astype(bf16)
            return 0

        sum0.done(j)
        lax.fori_loop(0, slot_total // step_rows, pick, 0)
        going[j][0]()
        from_a[j, own] = to_a[j, own]

    with scope("s_home"):
        sum0.home(0)
    with scope("s_home1"):
        for j in range(1, pieces):
            sum0.home(j)
            pick_piece(j - 1)
        pick_piece(pieces - 1)
    for which in range(2):
        for i in local[1:]:
            early(which, i).start()
    sum0.drain()

    for j in range(pieces):
        with scope("s_gowait%d" % j):
            going[j][1]()
        slots[...] = jnp.zeros_like(slots)
        received = from_a[j].astype(f32).T.astype(bf16)

        def trips(at):
            source = in_hot[:, at] if kept else in_part(at)
            value = dot(received, source) * angle[j * lane:(j + 1) * lane, at]
            target = out_hot[:, at] if kept else out_part(at)
            slots[...] += dot(target, value.astype(bf16), 1, 1)

        with scope("s_trips%d" % j):
            tiles(trips)
        to_b[j] = slots[...].astype(bf16)
        back[j][0]()
        from_b[j, own] = to_b[j, own]
    with scope("s_early0"):
        early_relay(0)
    with scope("s_upbeside"):
        up_beside()

    def add_up(j):
        for index in range(mp):
            rest = dot(full_b[j], ups[index, j * lane:(j + 1) * lane, :])
            partial[index] = (states[index].astype(f32) if j == 0 else partial[index]) + rest

    for j in range(pieces):
        with scope("s_backwait%d" % j):
            back[j][1]()
        part_b[j] = dot(list_hot[...], from_b[j]).astype(bf16)
        sum1.into(j)
        if j + 1 < pieces:
            sum1.across(j)
    with scope("s_sum1"):
        sum1.across(pieces - 1)
        with scope("s_early1"):
            up_home()
        with scope("s_feedspread"):
            if feeds:
                enter(0, 0).wait_recv()
                near(0, 0, 2).start()
                near(0, 0, 1).start()
                hop(0).start()
        for j in range(pieces - 2):
            sum1.home(j)
        early_finish(0)
        early_finish(1)
        if pieces > 1:
            sum1.home(pieces - 2)
        for j in range(pieces - 1):
            sum1.done(j)
            add_up(j)
        with scope("s_lasthome"):
            sum1.home(pieces - 1)

    starts, sizes = chunks_of(half)
    order = [(h, t) for t in range(len(sizes)) for h in (0, 1)]

    def chunk(c):
        side, t = c
        start = side * half + starts[t]
        return pl.ds(start if isinstance(side, int) else pl.multiple_of(start, half // 2), sizes[t])

    def chunk_id(c):
        return c[0] * len(sizes) + c[1]

    def act_copy(layer, parity, c, which):
        bit, off = plan[which]
        at = acts.at[layer - 1, other_of(off), chunk(c)]
        return pltpu.make_async_remote_copy(
            src_ref=at, dst_ref=at,
            send_sem=act_send.at[parity, chunk_id(c)], recv_sem=act_recv.at[parity, chunk_id(c), which],
            device_id={"mp": flip(m, bit)}, device_id_type=MESH)

    def send(layer, parity, c):
        for i in local:
            act_copy(layer, parity, c, i).start()

    def relay(layer, parity, c):
        for i in relayed:
            first = brings[plan[i][1]]
            if [j for j in relayed if brings[plan[j][1]] == first][0] == i:
                act_copy(layer, parity, c, first).wait_recv()
            act_copy(layer, parity, c, i).start()

    def finish(layer, parity, c):
        for i in range(len(plan)):
            if i not in relays_from:
                act_copy(layer, parity, c, i).wait_recv()

    def sent(layer, parity, c):
        at = acts.at[layer - 1, pl.ds(0, mp - 1), chunk(c)]
        pltpu.make_async_remote_copy(
            src_ref=at, dst_ref=at, send_sem=act_send.at[parity, chunk_id(c)], recv_sem=act_recv.at[parity, chunk_id(c), 0],
            device_id={"mp": flip(m, 1)}, device_id_type=MESH).wait_send()

    def product(k, at, held_weight):
        rows_in = jnp.concatenate([acts[k - 1, index, at, :] for index in range(mp)], axis=1)
        return silu(dot(rows_in, held_weight[...]))

    def core_copy(layer, c, i):
        at = acts.at[layer - 1, (m, across_y)[i], chunk(c)]
        return pltpu.make_async_remote_copy(
            src_ref=at, dst_ref=at, send_sem=core_send.at[chunk_id(c)], recv_sem=core_recv.at[chunk_id(c), i],
            device_id={"mp": flip(m, 1)}, device_id_type=MESH)

    def core_sent(layer, c):
        at = acts.at[layer - 1, pl.ds(0, 2), chunk(c)]
        pltpu.make_async_remote_copy(
            src_ref=at, dst_ref=at, send_sem=core_send.at[chunk_id(c)], recv_sem=core_recv.at[chunk_id(c), 0],
            device_id={"mp": flip(m, 1)}, device_id_type=MESH).wait_send()

    last_up = (pieces - 1) * lane
    with scope("s_begin"):
        for spot in range(len(order)):
            c = (m % 2 if spot % 2 == 0 else 1 - m % 2), spot // 2
            at = chunk(c)
            if spot == 1:
                sum1.done(pieces - 1)
            if spot == 3 and feeds:
                with scope("s_corner00"):
                    feed_corner(0, 0)
                    for f in range(1, feeds):
                        enter(f, 0).wait_recv()
                        near(f, 0, 2).start()
            firsts = []
            for index in range(mp):
                before = partial[index, at] if pieces > 1 else states[index, at].astype(f32)
                first = before + dot(full_b[pieces - 1, at], ups[index, last_up:last_up + lane, :])
                partial[index, at] = first
                firsts.append(first.astype(bf16))
            total = dot(jnp.concatenate(firsts, axis=1), weight[0])
            hidden[at, :] = partial[m, at]
            acts[0, m, at, :] = silu(total).astype(bf16)
            send(1, 0, c)
        sum1.drain()
        arrived(from_a.at[:, span], 0, 0).wait_send()
        arrived(from_b.at[:, span], 1, 0).wait_send()
        for which in range(2):
            early_sent(which)
        pltpu.make_async_remote_copy(
            src_ref=ups.at[m], dst_ref=ups.at[m], send_sem=up_send, recv_sem=up_recv.at[0],
            device_id={"mp": across_y}, device_id_type=MESH).wait_send()
    def update(l, c):
        at = chunk(c)
        value = (hidden[at, :] + product(2 * l + 1, at, weight.at[1 + l])) * inv_root_two
        hidden[at, :] = value
        return value.astype(bf16)

    with scope("s_layer0"):
        with scope("s_feedrest0"):
            for f in range(1, feeds):
                enter(f, 1).start()
            if feeds:
                hop(0).wait_recv()
                near(0, 1, 1).start()
                near(0, 1, 2).start()
        with scope("s_l0rel"):
            relay(1, 0, order[0])
        for spot, c in enumerate(order):
            with scope("s_l0fin%d" % spot):
                finish(1, 0, c)
            with scope("s_l0rel%d" % spot):
                if spot + 1 < len(order):
                    relay(1, 0, order[spot + 1])
            value = update(0, c)
            if layers > 1:
                acts[1, m, chunk(c), :] = value
                send(2, 1, c)
            with scope("s_l0feed%d" % spot):
                if spot == 1 and feeds:
                    feed_corner(0, 1)
                    for f in range(1, feeds):
                        near(f, 0, 1).start()
                if spot == 2:
                    for f in range(1, feeds):
                        feed_corner(f, 0)
        if layers > 1:
            with scope("s_l1rel"):
                relay(2, 1, order[0])
        with scope("s_feedrest1"):
            for f in range(1, feeds):
                enter(f, 1).wait_recv()
                near(f, 1, 1).start()
                near(f, 1, 2).start()

    def layer_step(l, _):
        k, parity, f = 2 * l, l % 2, l - 1

        def second(c):
            for i in range(2):
                core_copy(k + 1, c, i).wait_recv()
            value = update(l, c)

            @pl.when(l + 1 < layers)
            def _():
                sent(k, 1 - parity, c)
                acts[k + 1, m, chunk(c), :] = value
                send(k + 2, 1 - parity, c)

        with scope("s_feedwait"):
            feed_ready(f)
        for spot, c in enumerate(order):
            at = chunk(c)
            with scope("s_fin%d" % spot):
                finish(k, parity, c)

            @pl.when(l > 1)
            def _():
                core_sent(k - 1, c)

            with scope("s_rel%d" % spot):
                if spot + 1 < len(order):
                    relay(k, parity, order[spot + 1])
            both = product(k, at, joint.at[f]).astype(bf16)
            acts[k, m, at, :] = both[:, :width]
            acts[k, across_y, at, :] = both[:, width:]
            for i in range(2):
                core_copy(k + 1, c, i).start()
            if spot >= 1:
                with scope("s_second%d" % spot):
                    second(order[spot - 1])
            if spot == 1:
                @pl.when(l == 1)
                def _():
                    with scope("s_corner11"):
                        for later in range(1, feeds):
                            feed_corner(later, 1)

        @pl.when(l + 1 < layers)
        def _():
            with scope("s_relnext"):
                relay(k + 2, 1 - parity, order[0])

        with scope("s_second_last"):
            second(order[-1])
        return 0

    with scope("s_layers"):
        lax.fori_loop(1, layers, layer_step, 0)

    atom_in.wait()
    atom_rows = min(atoms, 256)
    parts, part_lane = table.shape[0], table.shape[2]
    here = pl.ds(pl.multiple_of(g * ATOM_DEV, ATOM_DEV), ATOM_DEV)
    atom_span = pl.ds(0, atoms - ATOM_DEV)
    gathers = [exchange(2, 2 * pieces + p, piece(atoms_to, p, ATOM_DEV), piece(atoms_from, p, ATOM_DEV),
                        atoms_from.at[p, atom_span]) for p in range(parts)]
    spreads = [exchange(3, 2 * pieces + parts + p, lambda peer, p=p: piece(table, p, ATOM_DEV)(g),
                        piece(table, p, ATOM_DEV), table.at[p, atom_span]) for p in range(parts)]

    def columns(p):
        return slice(p * part_lane, (p + 1) * part_lane)

    with scope("s_collect"):
        def collect(i, _):
            at = pl.ds(pl.multiple_of(i * atom_rows, atom_rows), atom_rows)
            ids = one_hot(atom_rows, atom_ref[...] - i * atom_rows)
            high, low = halves(hidden[...])
            total = dot(ids, high) + dot(ids, low)
            for p in range(parts):
                atoms_own[p, at] = total[:, columns(p)]
                atoms_to[p, at] = total[:, columns(p)].astype(bf16)
            return 0

        lax.fori_loop(0, atoms // atom_rows, collect, 0)
        for p in range(parts):
            gathers[p][0]()
    for p in range(parts):
        atoms_from[p, here] = jnp.zeros((ATOM_DEV, part_lane), bf16)
    for c in order:
        sent(1, (layers - 1) % 2, c)
        if layers > 1:
            sent(1, layers % 2, c)
            core_sent(1, c)
    feed_sent()
    for p in range(parts):
        with scope("s_atomwait%d" % p):
            gathers[p][1]()

        def add(i, total):
            return total + atoms_from[p, pl.ds(pl.multiple_of(i * ATOM_DEV, ATOM_DEV), ATOM_DEV)].astype(f32)

        total = lax.fori_loop(0, graph, add, atoms_own[p, here])
        mine_out = silu(atom_scale * total).astype(bf16)
        table[p, here] = mine_out
        spreads[p][0]()
        atom_out_ref[:, columns(p)] = mine_out
    arrived(atoms_from.at[:, atom_span], 2, 0).wait_send()
    for p in range(parts):
        with scope("s_spreadwait%d" % p):
            spreads[p][1]()

        def spread(i, total):
            at = pl.ds(pl.multiple_of(i * atom_rows, atom_rows), atom_rows)
            return total + dot(one_hot(atom_rows, atom_ref[...] - i * atom_rows), table[p, at], 0, 0)

        total = lax.fori_loop(0, atoms // atom_rows, spread, hidden[:, columns(p)])
        edge_out_ref[:, columns(p)] = total.astype(bf16)
    arrived(table.at[:, atom_span], 3, 0).wait_send()


def hand_on(edge_ref, atom_ref, edge_out_ref, atom_out_ref, sem):
    edge = pltpu.make_async_copy(edge_ref, edge_out_ref, sem.at[0])
    atom = pltpu.make_async_copy(atom_ref, atom_out_ref, sem.at[1])
    edge.start()
    atom.start()
    edge.wait()
    atom.wait()


def local(graph, mp, edge_state, down_weight, basis, basis_weight, up_weight, dense_weight,
          send_rows, trip_in, trip_out, trip_live, edge_atom):
    rows, width = edge_state.shape
    trip = down_weight.shape[1]
    slot_total = graph * send_rows.shape[2]
    triplets = trip_in.shape[0]
    maps = dense_weight.shape[0] * dense_weight.shape[1]
    tile = 2048 if slot_total <= 512 else 128
    atoms = graph * ATOM_DEV
    feeds = dense_weight.shape[0] - 1
    chunks = 2 * len(chunks_of(rows // 2)[1])
    stages = mp.bit_length()
    extra = max(stages - 2, 1)
    half = rows // 2
    vmem = pltpu.VMEM
    pieces = trip // 128 if trip % 128 == 0 else 1
    lane = trip // pieces
    pad = -(-basis.shape[0] // 16) * 16
    hot_bytes = 2 * 2 * slot_total * triplets
    hots = [vmem((slot_total, triplets), bf16)] * 2 if hot_bytes <= 2 ** 24 else [None, None]
    reduce_bufs = [
        vmem((pieces, rows, lane), bf16), vmem((pieces, half, lane), bf16), vmem((pieces, extra, half, lane), bf16),
        vmem((pieces, extra, half, lane), bf16), vmem((pieces, rows, lane), bf16),
    ]
    dma = pltpu.SemaphoreType.DMA
    spec = pl.BlockSpec(memory_space=pltpu.VMEM)
    operands = [
        edge_state, down_weight, basis, basis_weight, up_weight,
        dense_weight.reshape((maps,) + dense_weight.shape[2:]),
        send_rows, trip_in.reshape(1, triplets), trip_out.reshape(1, triplets),
        trip_live.reshape(1, triplets), edge_atom.reshape(1, rows),
    ]
    inputs = [vmem(a.shape, a.dtype) for i, a in enumerate(operands) if i not in (0, 4, 5)]
    parts = width // 128 if width % 128 == 0 else 1
    atom_buf = (parts, atoms, width // parts)
    body = functools.partial(kernel, graph, mp, tile)
    before = [
        *inputs, dma((len(inputs) + 2,)),
        vmem((mp, rows, width), bf16), vmem((mp, trip, width), bf16), dma((2,)), dma((2, mp - 1)), dma(()), dma((2,)),
        vmem((dense_weight.shape[0] + 1,) + dense_weight.shape[2:], bf16),
        vmem((feeds, dense_weight.shape[2], 2 * width), bf16), dma((maps,)), dma((feeds,)), dma((feeds, 2)), dma((feeds,)), dma((feeds, 2, 3)),
        dma((chunks,)), dma((chunks, 2)),
        *reduce_bufs, *reduce_bufs,
        dma((2, stages)), dma((2, pieces, stages)),
        *[vmem((pieces, slot_total, lane), bf16)] * 4,
        dma((4,)), dma((2 * pieces + 2 * parts,)),
        vmem((rows, slot_total), bf16), vmem((3 * pad, triplets), bf16), vmem((3 * pad, trip), bf16),
        vmem((trip, triplets), f32), vmem((slot_total, lane), f32),
    ]
    if hots[0] is None:
        hots, kept_body, at = [], body, len(operands) + 2 + len(before)
        body = lambda *refs: kept_body(*refs[:at], None, None, *refs[at:])
    outs = pl.pallas_call(
        body,
        out_shape=(
            pltpu.VMEM((rows, width), bf16),
            pltpu.VMEM((ATOM_DEV, width), bf16),
        ),
        in_specs=[pl.BlockSpec(memory_space=pl.ANY)] * len(operands),
        out_specs=(spec, spec),
        scratch_shapes=[
            *before, *hots,
            vmem((maps - 1, mp, rows, width), bf16), vmem((mp, rows, width), f32), vmem((rows, width), f32),
            dma((2, chunks)), dma((2, chunks, mp - 1)),
            vmem(atom_buf, f32), vmem(atom_buf, bf16), vmem(atom_buf, bf16), vmem(atom_buf, bf16),
        ],
        compiler_params=pltpu.CompilerParams(
            collective_id=0, has_side_effects=True, vmem_limit_bytes=64000 * 1024
        ),
        name="edge_block",
    )(*operands)
    outs = [pltpu.with_memory_space_constraint(o, pltpu.VMEM) for o in outs]
    return pl.pallas_call(
        hand_on,
        out_shape=tuple(jax.ShapeDtypeStruct(o.shape, o.dtype) for o in outs),
        in_specs=[spec] * 2,
        out_specs=[pl.BlockSpec(memory_space=pl.ANY)] * 2,
        scratch_shapes=[dma((2,))],
        name="hand_on",
    )(*outs)


def solution(mesh):
    in_specs = (
        P("graph", "mp"),
        P("mp", None),
        P(None, ("graph", "mp")),
        P(),
        P(None, "mp"),
        P(None, None, None, "mp"),
        P("graph", "mp", None),
        P(("graph", "mp")),
        P(("graph", "mp")),
        P(("graph", "mp")),
        P("graph"),
    )
    out_specs = (P("graph", "mp"), P("graph", "mp"))
    body = functools.partial(local, mesh.shape["graph"], mesh.shape["mp"])
    return jax.shard_map(body, mesh=mesh, in_specs=in_specs, out_specs=out_specs, check_vma=False)
```

```python
import functools

import jax
import jax.numpy as jnp
from jax import lax
from jax.experimental import pallas as pl
from jax.experimental.pallas import tpu as pltpu
from jax.sharding import PartitionSpec as P

ATOM_DEV = 32

inv_root_two = 0.7071067811865476
atom_scale = 0.2

MESH = pl.DeviceIdType.MESH
bf16 = jnp.bfloat16
f32 = jnp.float32


def scope(name):
    return jax.named_scope(name)


def silu(v):
    return v / (1.0 + jnp.exp(-v))


def flip(index, bit):
    return index + bit - 2 * bit * ((index // bit) % 2)


def one_hot(rows, ids):
    shape = (rows, ids.shape[1])
    return jnp.where(lax.broadcasted_iota(jnp.int32, shape, 0) == ids, 1.0, 0.0).astype(bf16)


def dot(a, b, ca=1, cb=0):
    return lax.dot_general(a, b, (((ca,), (cb,)), ((), ())), preferred_element_type=f32)


def halves(v):
    high = v.astype(bf16)
    return high, (v - high.astype(f32)).astype(bf16)


def chunks_of(half):
    return (0, half // 2), (half // 2, half // 2)


def gather_plan(mp):
    plan, held, bit = [], [0], mp // 2
    while bit >= 1:
        plan += [(bit, off) for off in held]
        held += [bit ^ off for off in held]
        bit //= 2
    return plan, held


def kernel(
    graph, mp, tile,
    state_hbm, down_hbm, basis_hbm, bw_hbm, up_hbm, dense_hbm, lists_hbm, in_hbm, out_hbm, live_hbm, atom_hbm,
    edge_out_ref, atom_out_ref,
    down_ref, basis_ref, bw_ref, lists_ref, in_ref, out_ref, live_ref, atom_ref, load_sem,
    states, ups, early_send, early_recv, up_send, up_recv,
    weight, joint, weight_sem, feed_send, feed_y, near_recv, core_send, core_recv,
    part_a, got_a, sum_a, more_a, full_a,
    part_b, got_b, sum_b, more_b, full_b,
    red_send, red_recv,
    to_a, from_a, to_b, from_b, xc_send, xc_recv,
    list_hot, basis_stack, bw_stack, angle, slots, in_hot, out_hot,
    acts, partial, hidden, act_send, act_recv,
    atoms_own, atoms_to, atoms_from, table,
):
    g = lax.axis_index("graph")
    m = lax.axis_index("mp")
    rows, width = hidden.shape
    trip = down_ref.shape[1]
    layers = weight.shape[0] - 1
    cap = lists_ref.shape[2]
    slot_total = graph * cap
    pieces, lane = to_a.shape[0], to_a.shape[2]
    kept = in_hot is not None
    triplets = in_ref.shape[1]
    atoms = graph * ATOM_DEV
    half = rows // 2
    feeds = layers - 1
    bits = [1 << i for i in range(mp.bit_length() - 1)]
    stages = len(bits)

    barrier = pltpu.get_barrier_semaphore()

    def greet(k, _):
        pl.semaphore_signal(barrier, inc=1, device_id={"graph": (g + k) % graph}, device_id_type=MESH)
        return 0

    lax.fori_loop(1, graph, greet, 0)
    for bit in bits:
        pl.semaphore_signal(barrier, inc=1, device_id={"mp": flip(m, bit)}, device_id_type=MESH)

    hbm = [state_hbm, down_hbm, lists_hbm, in_hbm, out_hbm, live_hbm, basis_hbm, bw_hbm, up_hbm, atom_hbm]
    here_refs = [
        states.at[m], down_ref, lists_ref, in_ref, out_ref, live_ref, basis_ref, bw_ref, ups.at[m], atom_ref]
    loads = [pltpu.make_async_copy(a, b, load_sem.at[i]) for i, (a, b) in enumerate(zip(hbm, here_refs))]
    for load in loads:
        load.start()
    state_in, down_in, lists_in, in_in, out_in, live_in, basis_in, bw_in, up_in, atom_in = loads

    def mp_copy(src, dst, which, j, stage, bit):
        return pltpu.make_async_remote_copy(
            src_ref=src, dst_ref=dst, send_sem=red_send.at[which, stage], recv_sem=red_recv.at[which, j, stage],
            device_id={"mp": flip(m, bit)}, device_id_type=MESH)

    mine = pl.ds(pl.multiple_of((m % 2) * half, half), half)
    other = pl.ds(pl.multiple_of(half - (m % 2) * half, half), half)

    plan, held = gather_plan(mp)

    def other_of(off):
        index = m
        for bit in bits:
            if off & bit:
                index = flip(index, bit)
        return index

    local = [i for i, (bit, off) in enumerate(plan) if off == 0]
    relayed = [i for i, (bit, off) in enumerate(plan) if off != 0]
    brings = {bit ^ off: i for i, (bit, off) in enumerate(plan)}
    relays_from = sorted({brings[plan[i][1]] for i in relayed})

    across_y = flip(m, mp // 2)

    def early(which, i):
        bit, off = plan[i]
        at = (states, ups)[which].at[other_of(off)]
        return pltpu.make_async_remote_copy(
            src_ref=at, dst_ref=at, send_sem=early_send.at[which], recv_sem=early_recv.at[which, i],
            device_id={"mp": flip(m, bit)}, device_id_type=MESH)

    trip_half = trip // 2
    up_rows = pl.ds(pl.multiple_of((g % 2) * trip_half, trip_half), trip_half)

    def up_copy(i):
        at = ups.at[(m, across_y)[i], up_rows]
        return pltpu.make_async_remote_copy(
            src_ref=at, dst_ref=at, send_sem=up_send, recv_sem=up_recv.at[i],
            device_id=({"mp": across_y}, {"graph": flip(g, 1)})[i], device_id_type=MESH)

    def up_beside():
        up_copy(0).wait_recv()
        up_copy(1).start()

    def up_home():
        up_copy(1).wait_recv()
        for i in relayed:
            early(1, i).start()

    def state_copy(i):
        cut = rows // 8
        at = states.at[m, (pl.ds(0, cut), pl.ds(cut, rows - cut))[i]]
        return pltpu.make_async_remote_copy(
            src_ref=at, dst_ref=at, send_sem=early_send.at[0], recv_sem=early_recv.at[0, local[0]],
            device_id={"mp": across_y}, device_id_type=MESH)

    def early_sent(which):
        at = (states, ups)[which].at[pl.ds(0, mp - 1 - which)]
        pltpu.make_async_remote_copy(
            src_ref=at, dst_ref=at, send_sem=early_send.at[which], recv_sem=early_recv.at[which, 0],
            device_id={"mp": flip(m, 1)}, device_id_type=MESH).wait_send()

    def early_relay(which):
        for i in relayed:
            first = brings[plan[i][1]]
            if [j for j in relayed if brings[plan[j][1]] == first][0] == i:
                early(which, first).wait_recv()
            early(which, i).start()

    def early_finish(which):
        for i in range(len(plan)):
            if i not in relays_from:
                early(which, i).wait_recv()

    eighth = weight.shape[1] // 8
    mine8 = g % 8

    def xor(a, k):
        for bit in (1, 2, 4):
            if k & bit:
                a = flip(a, bit)
        return a

    def part8(e):
        return pl.ds(pl.multiple_of(e * eighth, eighth), eighth)

    def feed_copy(src, f, e, sem, device):
        return pltpu.make_async_remote_copy(
            src_ref=src, dst_ref=joint.at[f, part8(e), far_cols], send_sem=feed_send.at[f], recv_sem=sem,
            device_id=device, device_id_type=MESH)

    def enter(f, far):
        e = xor(mine8, 4 * far)
        return feed_copy(joint.at[f, part8(e), own_cols], f, e, feed_y.at[f, far], {"mp": across_y})

    def near(f, far, k):
        e = xor(mine8, 4 * far)
        return feed_copy(joint.at[f, part8(e), far_cols], f, e, near_recv.at[f, far, k - 1], {"graph": xor(g, k)})

    def corner(f, far):
        came, goes = (2, 1) if far == 0 else (1, 2)
        e = xor(mine8, 4 * far + came)
        return feed_copy(joint.at[f, part8(e), far_cols], f, e, near_recv.at[f, far, 2], {"graph": xor(g, goes)})

    def feed_corner(f, far):
        near(f, far, 2 if far == 0 else 1).wait_recv()
        corner(f, far).start()

    def feed_ready(f):
        for far in range(2):
            near(f, far, 1 if far == 0 else 2).wait_recv()
            corner(f, far).wait_recv()

    def feed_sent():
        for f in range(feeds):
            at = joint.at[f, :, far_cols]
            pltpu.make_async_remote_copy(
                src_ref=at, dst_ref=at, send_sem=feed_send.at[f], recv_sem=near_recv.at[f, 0, 0],
                device_id={"mp": across_y}, device_id_type=MESH).wait_send()

    class Sum:
        def __init__(self, which, part, got, summed, more, full):
            self.which, self.part, self.got = which, part, got
            self.summed, self.more, self.full = summed, more, full

        def first(self, j):
            return mp_copy(self.part.at[j, other], self.got.at[j], self.which, j, 0, 1)

        def step(self, j, b):
            return mp_copy(self.summed.at[j, b], self.more.at[j, b], self.which, j, 1 + b, bits[1 + b])

        def last(self, j):
            at = self.full.at[j, mine]
            return mp_copy(at, at, self.which, j, stages, 1)

        def into(self, j):
            self.first(j).start()

        def across(self, j):
            self.first(j).wait_recv()
            total = self.part[j, mine].astype(f32) + self.got[j].astype(f32)
            if stages > 1:
                self.summed[j, 0] = total.astype(bf16)
                self.step(j, 0).start()
            else:
                self.full[j, mine] = total.astype(bf16)

        def home(self, j):
            for b in range(stages - 1):
                self.step(j, b).wait_recv()
                total = self.summed[j, b].astype(f32) + self.more[j, b].astype(f32)
                if b + 2 < stages:
                    self.summed[j, b + 1] = total.astype(bf16)
                    self.step(j, b + 1).start()
                else:
                    self.full[j, mine] = total.astype(bf16)
            self.last(j).start()

        def done(self, j):
            self.last(j).wait_recv()

        def drain(self):
            for stage in range(stages + 1):
                mp_copy(self.got, self.got, self.which, 0, stage, 1).wait_send()

    sum0 = Sum(0, part_a, got_a, sum_a, more_a, full_a)
    sum1 = Sum(1, part_b, got_b, sum_b, more_b, full_b)

    def peer_of(k):
        if graph & (graph - 1):
            return (g + k) % graph
        return sum(bit * ((g // bit + k // bit) % 2) for bit in (1 << i for i in range(graph.bit_length() - 1)))

    peers = [peer_of(k) for k in range(graph - 1, 0, -1)] if graph <= 8 else None

    def arrived(whole, group, which):
        return pltpu.make_async_remote_copy(
            src_ref=whole, dst_ref=whole, send_sem=xc_send.at[group], recv_sem=xc_recv.at[which],
            device_id={"graph": (g + 1) % graph}, device_id_type=MESH)

    def exchange(group, which, src_at, dst_at, whole):
        def to(peer):
            pltpu.make_async_remote_copy(
                src_ref=src_at(peer), dst_ref=dst_at(g), send_sem=xc_send.at[group], recv_sem=xc_recv.at[which],
                device_id={"graph": peer}, device_id_type=MESH).start()

        def one(i, _):
            to(peer_of(graph - 1 - i))
            return 0

        def start():
            if peers is None:
                lax.fori_loop(0, graph - 1, one, 0)
            else:
                for peer in peers:
                    to(peer)

        return start, arrived(whole, group, which).wait_recv

    def block(ref, size):
        return lambda i: ref.at[pl.ds(pl.multiple_of(i * size, size), size)]

    def piece(ref, j, size):
        return lambda i: ref.at[j, pl.ds(pl.multiple_of(i * size, size), size)]

    def tiles(step):
        def one(i, _):
            step(pl.ds(pl.multiple_of(i * tile, tile), tile))
            return 0

        lax.fori_loop(0, triplets // tile, one, 0)

    def in_part(at):
        return one_hot(slot_total, in_ref[:, at])

    def out_part(at):
        return one_hot(slot_total, jnp.where(live_ref[:, at] > 0, out_ref[:, at], -1))

    state_in.wait()
    down_in.wait()
    with scope("s_proj"):
        projected = dot(states[m], down_ref[...]).astype(bf16)
        for j in range(pieces):
            part_a[j] = projected[:, j * lane:(j + 1) * lane]
    with scope("s_barrier"):
        pl.semaphore_wait(barrier, graph - 1 + len(bits))
    for j in range(pieces):
        sum0.into(j)
    state_copy(0).start()
    own_cols, far_cols = pl.ds(0, width), pl.ds(width, width)
    places = [(0, weight.at[0])] + [(2 * l + 1, weight.at[1 + l]) for l in range(layers)]
    places += [(2 * f + 2, joint.at[f, :, own_cols]) for f in range(feeds)]
    loads_of_maps = [pltpu.make_async_copy(dense_hbm.at[k], at, weight_sem.at[k]) for k, at in places]
    for load in loads_of_maps:
        load.start()

    lists_in.wait()
    with scope("s_hots"):
        for i in range(graph):
            list_hot[:, i * cap:(i + 1) * cap] = one_hot(rows, lists_ref[0, i:i + 1, :])
        in_in.wait()
        if kept:
            def keep_in(at):
                in_hot[:, at] = in_part(at)

            tiles(keep_in)
    with scope("s_across"):
        for j in range(pieces):
            sum0.across(j)
    up_in.wait()
    state_copy(1).start()
    out_in.wait()
    live_in.wait()
    if kept:
        def keep_out(at):
            out_hot[:, at] = out_part(at)

        with scope("s_outhot"):
            tiles(keep_out)

    basis_in.wait()
    bw_in.wait()
    depth = basis_ref.shape[0]
    pad = basis_stack.shape[0] // 3
    with scope("s_angles"):
        bw_high, bw_low = halves(bw_ref[...])
        bw_stack[...] = jnp.zeros_like(bw_stack)
        bw_stack[0:depth] = bw_high
        bw_stack[pad:pad + depth] = bw_high
        bw_stack[2 * pad:2 * pad + depth] = bw_low

        def angles(at):
            high, low = halves(basis_ref[:, at])
            basis_stack[:, at] = jnp.zeros((3 * pad, tile), bf16)
            basis_stack[0:depth, at] = high
            basis_stack[pad:pad + depth, at] = low
            basis_stack[2 * pad:2 * pad + depth, at] = high
            angle[:, at] = dot(bw_stack[...], basis_stack[:, at], 0, 0)

        tiles(angles)

    for load in loads_of_maps:
        load.wait()
    if feeds:
        enter(0, 0).start()
    up_copy(0).start()
    if feeds:
        enter(0, 1).start()
    for f in range(1, feeds):
        enter(f, 0).start()
    step_rows = min(slot_total, 512)
    own = pl.ds(pl.multiple_of(g * cap, cap), cap)
    span = pl.ds(0, slot_total - cap)
    going = [exchange(0, j, piece(to_a, j, cap), piece(from_a, j, cap), from_a.at[j, span]) for j in range(pieces)]
    back = [exchange(1, pieces + j, piece(to_b, j, cap), piece(from_b, j, cap), from_b.at[j, span])
            for j in range(pieces)]

    def pick_piece(j):
        def pick(i, _):
            at = pl.ds(pl.multiple_of(i * step_rows, step_rows), step_rows)
            to_a[j, at, :] = dot(list_hot[:, at], full_a[j], 0, 0).astype(bf16)
            return 0

        sum0.done(j)
        lax.fori_loop(0, slot_total // step_rows, pick, 0)
        going[j][0]()
        from_a[j, own] = to_a[j, own]

    with scope("s_home"):
        sum0.home(0)
    with scope("s_home1"):
        for j in range(1, pieces):
            sum0.home(j)
            pick_piece(j - 1)
        pick_piece(pieces - 1)
    for which in range(2):
        for i in local[1:]:
            early(which, i).start()
    sum0.drain()

    for j in range(pieces):
        with scope("s_gowait%d" % j):
            going[j][1]()
        slots[...] = jnp.zeros_like(slots)
        received = from_a[j].astype(f32).T.astype(bf16)

        def trips(at):
            source = in_hot[:, at] if kept else in_part(at)
            value = dot(received, source) * angle[j * lane:(j + 1) * lane, at]
            target = out_hot[:, at] if kept else out_part(at)
            slots[...] += dot(target, value.astype(bf16), 1, 1)

        with scope("s_trips%d" % j):
            tiles(trips)
        to_b[j] = slots[...].astype(bf16)
        back[j][0]()
        from_b[j, own] = to_b[j, own]
    with scope("s_early0"):
        early_relay(0)

    def add_up(j):
        for index in range(mp):
            rest = dot(full_b[j], ups[index, j * lane:(j + 1) * lane, :])
            partial[index] = (states[index].astype(f32) if j == 0 else partial[index]) + rest

    for j in range(pieces):
        with scope("s_backwait%d" % j):
            back[j][1]()
        part_b[j] = dot(list_hot[...], from_b[j]).astype(bf16)
        sum1.into(j)
        if j == 0:
            with scope("s_upbeside"):
                up_beside()
        if j + 1 < pieces:
            sum1.across(j)
    with scope("s_sum1"):
        sum1.across(pieces - 1)
        with scope("s_early1"):
            up_home()
        with scope("s_feedspread"):
            for f in range(1, feeds):
                enter(f, 1).start()
            if feeds:
                for far in range(2):
                    enter(0, far).wait_recv()
                    near(0, far, 2 - far).start()
                    near(0, far, 1 + far).start()
        for j in range(pieces - 2):
            sum1.home(j)
        early_finish(0)
        early_finish(1)
        if pieces > 1:
            sum1.home(pieces - 2)
        for j in range(pieces - 2):
            sum1.done(j)
            add_up(j)
        with scope("s_lasthome"):
            sum1.home(pieces - 1)

    starts, sizes = chunks_of(half)
    order = [(h, t) for t in range(len(sizes)) for h in (0, 1)]

    def chunk(c):
        side, t = c
        start = side * half + starts[t]
        return pl.ds(start if isinstance(side, int) else pl.multiple_of(start, half // 2), sizes[t])

    def chunk_id(c):
        return c[0] * len(sizes) + c[1]

    def act_copy(layer, parity, c, which):
        bit, off = plan[which]
        at = acts.at[layer - 1, other_of(off), chunk(c)]
        return pltpu.make_async_remote_copy(
            src_ref=at, dst_ref=at,
            send_sem=act_send.at[parity, chunk_id(c)], recv_sem=act_recv.at[parity, chunk_id(c), which],
            device_id={"mp": flip(m, bit)}, device_id_type=MESH)

    def send(layer, parity, c):
        for i in local:
            act_copy(layer, parity, c, i).start()

    def relay(layer, parity, c):
        for i in relayed:
            first = brings[plan[i][1]]
            if [j for j in relayed if brings[plan[j][1]] == first][0] == i:
                act_copy(layer, parity, c, first).wait_recv()
            act_copy(layer, parity, c, i).start()

    def finish(layer, parity, c):
        for i in range(len(plan)):
            if i not in relays_from:
                act_copy(layer, parity, c, i).wait_recv()

    def sent(layer, parity, c):
        at = acts.at[layer - 1, pl.ds(0, mp - 1), chunk(c)]
        pltpu.make_async_remote_copy(
            src_ref=at, dst_ref=at, send_sem=act_send.at[parity, chunk_id(c)], recv_sem=act_recv.at[parity, chunk_id(c), 0],
            device_id={"mp": flip(m, 1)}, device_id_type=MESH).wait_send()

    def product(k, at, held_weight):
        rows_in = jnp.concatenate([acts[k - 1, index, at, :] for index in range(mp)], axis=1)
        return silu(dot(rows_in, held_weight[...]))

    def core_copy(layer, c, i):
        at = acts.at[layer - 1, (m, across_y)[i], chunk(c)]
        return pltpu.make_async_remote_copy(
            src_ref=at, dst_ref=at, send_sem=core_send.at[chunk_id(c)], recv_sem=core_recv.at[chunk_id(c), i],
            device_id={"mp": flip(m, 1)}, device_id_type=MESH)

    def core_sent(layer, c):
        at = acts.at[layer - 1, pl.ds(0, 2), chunk(c)]
        pltpu.make_async_remote_copy(
            src_ref=at, dst_ref=at, send_sem=core_send.at[chunk_id(c)], recv_sem=core_recv.at[chunk_id(c), 0],
            device_id={"mp": flip(m, 1)}, device_id_type=MESH).wait_send()

    late = range(max(pieces - 2, 0), pieces)
    late_up = pl.ds(late[0] * lane, len(late) * lane)
    with scope("s_begin"):
        for spot in range(len(order)):
            c = (m % 2 if spot % 2 == 0 else 1 - m % 2), spot // 2
            at = chunk(c)
            if spot == 1:
                for j in late:
                    sum1.done(j)
            update_rows = jnp.concatenate([full_b[j, at] for j in late], axis=1)
            firsts = []
            for index in range(mp):
                before = partial[index, at] if pieces > 2 else states[index, at].astype(f32)
                first = before + dot(update_rows, ups[index, late_up, :])
                partial[index, at] = first
                firsts.append(first.astype(bf16))
            total = dot(jnp.concatenate(firsts, axis=1), weight[0])
            hidden[at, :] = partial[m, at]
            acts[0, m, at, :] = silu(total).astype(bf16)
            send(1, 0, c)
        if feeds:
            with scope("s_corner0"):
                for far in range(2):
                    feed_corner(0, far)
        sum1.drain()
        arrived(from_a.at[:, span], 0, 0).wait_send()
        arrived(from_b.at[:, span], 1, 0).wait_send()
        for which in range(2):
            early_sent(which)
        pltpu.make_async_remote_copy(
            src_ref=ups.at[m], dst_ref=ups.at[m], send_sem=up_send, recv_sem=up_recv.at[0],
            device_id={"mp": across_y}, device_id_type=MESH).wait_send()
    def update(l, c):
        at = chunk(c)
        value = (hidden[at, :] + product(2 * l + 1, at, weight.at[1 + l])) * inv_root_two
        hidden[at, :] = value
        return value.astype(bf16)

    with scope("s_layer0"):
        with scope("s_feedrest0"):
            for f in range(1, feeds):
                for far in range(2):
                    enter(f, far).wait_recv()
                    near(f, far, 2 - far).start()
                    near(f, far, 1 + far).start()
        with scope("s_l0rel"):
            relay(1, 0, order[0])
        for spot, c in enumerate(order):
            with scope("s_l0fin%d" % spot):
                finish(1, 0, c)
            with scope("s_l0rel%d" % spot):
                if spot + 1 < len(order):
                    relay(1, 0, order[spot + 1])
            value = update(0, c)
            if layers > 1:
                acts[1, m, chunk(c), :] = value
                send(2, 1, c)
            with scope("s_l0feed%d" % spot):
                if spot == 2:
                    for f in range(1, feeds):
                        feed_corner(f, 0)
        if layers > 1:
            with scope("s_l1rel"):
                relay(2, 1, order[0])
    def layer_step(l, _):
        k, parity, f = 2 * l, l % 2, l - 1

        def second(c):
            for i in range(2):
                core_copy(k + 1, c, i).wait_recv()
            value = update(l, c)

            @pl.when(l + 1 < layers)
            def _():
                sent(k, 1 - parity, c)
                acts[k + 1, m, chunk(c), :] = value
                send(k + 2, 1 - parity, c)

        with scope("s_feedwait"):
            feed_ready(f)
        for spot, c in enumerate(order):
            at = chunk(c)
            with scope("s_fin%d" % spot):
                finish(k, parity, c)

            @pl.when(l > 1)
            def _():
                core_sent(k - 1, c)

            both = product(k, at, joint.at[f]).astype(bf16)
            acts[k, m, at, :] = both[:, :width]
            acts[k, across_y, at, :] = both[:, width:]
            for i in range(2):
                core_copy(k + 1, c, i).start()
            last = spot + 1 == len(order)
            with scope("s_rel%d" % spot):
                if not last:
                    relay(k, parity, order[spot + 1])
            with scope("s_second%d" % spot):
                if spot == 0:
                    second(c)

                    @pl.when(l == 1)
                    def _():
                        for later in range(1, feeds):
                            feed_corner(later, 1)
                elif spot > 1:
                    second(order[spot - 1])
            if last:
                with scope("s_relnext"):
                    @pl.when(l + 1 < layers)
                    def _():
                        relay(k + 2, 1 - parity, order[0])
                with scope("s_last"):
                    second(c)
        return 0

    with scope("s_layers"):
        lax.fori_loop(1, layers, layer_step, 0)

    atom_in.wait()
    atom_rows = min(atoms, 256)
    parts, part_lane = table.shape[0], table.shape[2]
    here = pl.ds(pl.multiple_of(g * ATOM_DEV, ATOM_DEV), ATOM_DEV)
    atom_span = pl.ds(0, atoms - ATOM_DEV)
    gathers = [exchange(2, 2 * pieces + p, piece(atoms_to, p, ATOM_DEV), piece(atoms_from, p, ATOM_DEV),
                        atoms_from.at[p, atom_span]) for p in range(parts)]
    spreads = [exchange(3, 2 * pieces + parts + p, lambda peer, p=p: piece(table, p, ATOM_DEV)(g),
                        piece(table, p, ATOM_DEV), table.at[p, atom_span]) for p in range(parts)]

    def columns(p):
        return slice(p * part_lane, (p + 1) * part_lane)

    with scope("s_collect"):
        def collect(i, _):
            at = pl.ds(pl.multiple_of(i * atom_rows, atom_rows), atom_rows)
            ids = one_hot(atom_rows, atom_ref[...] - i * atom_rows)
            high, low = halves(hidden[...])
            total = dot(ids, high) + dot(ids, low)
            for p in range(parts):
                atoms_own[p, at] = total[:, columns(p)]
                atoms_to[p, at] = total[:, columns(p)].astype(bf16)
            return 0

        lax.fori_loop(0, atoms // atom_rows, collect, 0)
        for p in range(parts):
            gathers[p][0]()
    for p in range(parts):
        atoms_from[p, here] = jnp.zeros((ATOM_DEV, part_lane), bf16)
    for c in order:
        sent(1, (layers - 1) % 2, c)
        if layers > 1:
            sent(1, layers % 2, c)
            core_sent(1, c)
    feed_sent()
    for p in range(parts):
        with scope("s_atomwait%d" % p):
            gathers[p][1]()

        def add(i, total):
            return total + atoms_from[p, pl.ds(pl.multiple_of(i * ATOM_DEV, ATOM_DEV), ATOM_DEV)].astype(f32)

        total = lax.fori_loop(0, graph, add, atoms_own[p, here])
        mine_out = silu(atom_scale * total).astype(bf16)
        table[p, here] = mine_out
        spreads[p][0]()
        atom_out_ref[:, columns(p)] = mine_out
    arrived(atoms_from.at[:, atom_span], 2, 0).wait_send()
    for p in range(parts):
        with scope("s_spreadwait%d" % p):
            spreads[p][1]()

        def spread(i, total):
            at = pl.ds(pl.multiple_of(i * atom_rows, atom_rows), atom_rows)
            return total + dot(one_hot(atom_rows, atom_ref[...] - i * atom_rows), table[p, at], 0, 0)

        total = lax.fori_loop(0, atoms // atom_rows, spread, hidden[:, columns(p)])
        edge_out_ref[:, columns(p)] = total.astype(bf16)
    arrived(table.at[:, atom_span], 3, 0).wait_send()


def hand_on(edge_ref, atom_ref, edge_out_ref, atom_out_ref, sem):
    edge = pltpu.make_async_copy(edge_ref, edge_out_ref, sem.at[0])
    atom = pltpu.make_async_copy(atom_ref, atom_out_ref, sem.at[1])
    edge.start()
    atom.start()
    edge.wait()
    atom.wait()


def local(graph, mp, edge_state, down_weight, basis, basis_weight, up_weight, dense_weight,
          send_rows, trip_in, trip_out, trip_live, edge_atom):
    rows, width = edge_state.shape
    trip = down_weight.shape[1]
    slot_total = graph * send_rows.shape[2]
    triplets = trip_in.shape[0]
    maps = dense_weight.shape[0] * dense_weight.shape[1]
    tile = 2048 if slot_total <= 512 else 128
    atoms = graph * ATOM_DEV
    feeds = dense_weight.shape[0] - 1
    chunks = 2 * len(chunks_of(rows // 2)[1])
    stages = mp.bit_length()
    extra = max(stages - 2, 1)
    half = rows // 2
    vmem = pltpu.VMEM
    pieces = trip // 128 if trip % 128 == 0 else 1
    lane = trip // pieces
    pad = -(-basis.shape[0] // 16) * 16
    hot_bytes = 2 * 2 * slot_total * triplets
    hots = [vmem((slot_total, triplets), bf16)] * 2 if hot_bytes <= 2 ** 24 else [None, None]
    reduce_bufs = [
        vmem((pieces, rows, lane), bf16), vmem((pieces, half, lane), bf16), vmem((pieces, extra, half, lane), bf16),
        vmem((pieces, extra, half, lane), bf16), vmem((pieces, rows, lane), bf16),
    ]
    dma = pltpu.SemaphoreType.DMA
    spec = pl.BlockSpec(memory_space=pltpu.VMEM)
    operands = [
        edge_state, down_weight, basis, basis_weight, up_weight,
        dense_weight.reshape((maps,) + dense_weight.shape[2:]),
        send_rows, trip_in.reshape(1, triplets), trip_out.reshape(1, triplets),
        trip_live.reshape(1, triplets), edge_atom.reshape(1, rows),
    ]
    inputs = [vmem(a.shape, a.dtype) for i, a in enumerate(operands) if i not in (0, 4, 5)]
    parts = width // 128 if width % 128 == 0 else 1
    atom_buf = (parts, atoms, width // parts)
    body = functools.partial(kernel, graph, mp, tile)
    before = [
        *inputs, dma((len(inputs) + 2,)),
        vmem((mp, rows, width), bf16), vmem((mp, trip, width), bf16), dma((2,)), dma((2, mp - 1)), dma(()), dma((2,)),
        vmem((dense_weight.shape[0] + 1,) + dense_weight.shape[2:], bf16),
        vmem((feeds, dense_weight.shape[2], 2 * width), bf16), dma((maps,)), dma((feeds,)), dma((feeds, 2)), dma((feeds, 2, 3)),
        dma((chunks,)), dma((chunks, 2)),
        *reduce_bufs, *reduce_bufs,
        dma((2, stages)), dma((2, pieces, stages)),
        *[vmem((pieces, slot_total, lane), bf16)] * 4,
        dma((4,)), dma((2 * pieces + 2 * parts,)),
        vmem((rows, slot_total), bf16), vmem((3 * pad, triplets), bf16), vmem((3 * pad, trip), bf16),
        vmem((trip, triplets), f32), vmem((slot_total, lane), f32),
    ]
    if hots[0] is None:
        hots, kept_body, at = [], body, len(operands) + 2 + len(before)
        body = lambda *refs: kept_body(*refs[:at], None, None, *refs[at:])
    outs = pl.pallas_call(
        body,
        out_shape=(
            pltpu.VMEM((rows, width), bf16),
            pltpu.VMEM((ATOM_DEV, width), bf16),
        ),
        in_specs=[pl.BlockSpec(memory_space=pl.ANY)] * len(operands),
        out_specs=(spec, spec),
        scratch_shapes=[
            *before, *hots,
            vmem((maps - 1, mp, rows, width), bf16), vmem((mp, rows, width), f32), vmem((rows, width), f32),
            dma((2, chunks)), dma((2, chunks, mp - 1)),
            vmem(atom_buf, f32), vmem(atom_buf, bf16), vmem(atom_buf, bf16), vmem(atom_buf, bf16),
        ],
        compiler_params=pltpu.CompilerParams(
            collective_id=0, has_side_effects=True, vmem_limit_bytes=64000 * 1024
        ),
        name="edge_block",
    )(*operands)
    outs = [pltpu.with_memory_space_constraint(o, pltpu.VMEM) for o in outs]
    return pl.pallas_call(
        hand_on,
        out_shape=tuple(jax.ShapeDtypeStruct(o.shape, o.dtype) for o in outs),
        in_specs=[spec] * 2,
        out_specs=[pl.BlockSpec(memory_space=pl.ANY)] * 2,
        scratch_shapes=[dma((2,))],
        name="hand_on",
    )(*outs)


def solution(mesh):
    in_specs = (
        P("graph", "mp"),
        P("mp", None),
        P(None, ("graph", "mp")),
        P(),
        P(None, "mp"),
        P(None, None, None, "mp"),
        P("graph", "mp", None),
        P(("graph", "mp")),
        P(("graph", "mp")),
        P(("graph", "mp")),
        P("graph"),
    )
    out_specs = (P("graph", "mp"), P("graph", "mp"))
    body = functools.partial(local, mesh.shape["graph"], mesh.shape["mp"])
    return jax.shard_map(body, mesh=mesh, in_specs=in_specs, out_specs=out_specs, check_vma=False)
```

```python
import functools

import jax
import jax.numpy as jnp
from jax import lax
from jax.experimental import pallas as pl
from jax.experimental.pallas import tpu as pltpu
from jax.sharding import PartitionSpec as P

ATOM_DEV = 32

inv_root_two = 0.7071067811865476
atom_scale = 0.2

MESH = pl.DeviceIdType.MESH
bf16 = jnp.bfloat16
f32 = jnp.float32


def scope(name):
    return jax.named_scope(name)


def silu(v):
    return v / (1.0 + jnp.exp(-v))


def flip(index, bit):
    return index + bit - 2 * bit * ((index // bit) % 2)


def one_hot(rows, ids):
    shape = (rows, ids.shape[1])
    return jnp.where(lax.broadcasted_iota(jnp.int32, shape, 0) == ids, 1.0, 0.0).astype(bf16)


def dot(a, b, ca=1, cb=0):
    return lax.dot_general(a, b, (((ca,), (cb,)), ((), ())), preferred_element_type=f32)


def halves(v):
    high = v.astype(bf16)
    return high, (v - high.astype(f32)).astype(bf16)


def chunks_of(half):
    return (0, half // 2), (half // 2, half // 2)


def gather_plan(mp):
    plan, held, bit = [], [0], mp // 2
    while bit >= 1:
        plan += [(bit, off) for off in held]
        held += [bit ^ off for off in held]
        bit //= 2
    return plan, held


def kernel(
    graph, mp, tile,
    state_hbm, down_hbm, basis_hbm, bw_hbm, up_hbm, dense_hbm, lists_hbm, in_hbm, out_hbm, live_hbm, atom_hbm,
    edge_out_ref, atom_out_ref,
    down_ref, basis_ref, bw_ref, lists_ref, in_ref, out_ref, live_ref, atom_ref, load_sem,
    states, ups, early_send, early_recv, up_send, up_recv,
    weight, joint, weight_sem, feed_send, feed_y, near_recv, core_send, core_recv,
    part_a, got_a, sum_a, more_a, full_a,
    part_b, got_b, sum_b, more_b, full_b,
    red_send, red_recv,
    to_a, from_a, to_b, from_b, xc_send, xc_recv,
    list_hot, basis_stack, bw_stack, angle, slots, in_hot, out_hot,
    acts, partial, hidden, act_send, act_recv,
    atoms_own, atoms_to, atoms_from, table,
):
    g = lax.axis_index("graph")
    m = lax.axis_index("mp")
    rows, width = hidden.shape
    trip = down_ref.shape[1]
    layers = weight.shape[0] - 1
    cap = lists_ref.shape[2]
    slot_total = graph * cap
    pieces, lane = to_a.shape[0], to_a.shape[2]
    kept = in_hot is not None
    triplets = in_ref.shape[1]
    atoms = graph * ATOM_DEV
    half = rows // 2
    feeds = layers - 1
    bits = [1 << i for i in range(mp.bit_length() - 1)]
    stages = len(bits)

    barrier = pltpu.get_barrier_semaphore()

    def greet(k, _):
        pl.semaphore_signal(barrier, inc=1, device_id={"graph": (g + k) % graph}, device_id_type=MESH)
        return 0

    lax.fori_loop(1, graph, greet, 0)
    for bit in bits:
        pl.semaphore_signal(barrier, inc=1, device_id={"mp": flip(m, bit)}, device_id_type=MESH)

    hbm = [state_hbm, down_hbm, lists_hbm, in_hbm, out_hbm, live_hbm, basis_hbm, bw_hbm, up_hbm, atom_hbm]
    here_refs = [
        states.at[m], down_ref, lists_ref, in_ref, out_ref, live_ref, basis_ref, bw_ref, ups.at[m], atom_ref]
    loads = [pltpu.make_async_copy(a, b, load_sem.at[i]) for i, (a, b) in enumerate(zip(hbm, here_refs))]
    for load in loads:
        load.start()
    state_in, down_in, lists_in, in_in, out_in, live_in, basis_in, bw_in, up_in, atom_in = loads

    def mp_copy(src, dst, which, j, stage, bit):
        return pltpu.make_async_remote_copy(
            src_ref=src, dst_ref=dst, send_sem=red_send.at[which, stage], recv_sem=red_recv.at[which, j, stage],
            device_id={"mp": flip(m, bit)}, device_id_type=MESH)

    mine = pl.ds(pl.multiple_of((m % 2) * half, half), half)
    other = pl.ds(pl.multiple_of(half - (m % 2) * half, half), half)

    plan, held = gather_plan(mp)

    def other_of(off):
        index = m
        for bit in bits:
            if off & bit:
                index = flip(index, bit)
        return index

    local = [i for i, (bit, off) in enumerate(plan) if off == 0]
    relayed = [i for i, (bit, off) in enumerate(plan) if off != 0]
    brings = {bit ^ off: i for i, (bit, off) in enumerate(plan)}
    relays_from = sorted({brings[plan[i][1]] for i in relayed})

    across_y = flip(m, mp // 2)

    def early(which, i):
        bit, off = plan[i]
        at = (states, ups)[which].at[other_of(off)]
        return pltpu.make_async_remote_copy(
            src_ref=at, dst_ref=at, send_sem=early_send.at[which], recv_sem=early_recv.at[which, 0 if i in relays_from else 1],
            device_id={"mp": flip(m, bit)}, device_id_type=MESH)

    trip_half = trip // 2
    up_rows = pl.ds(pl.multiple_of((g % 2) * trip_half, trip_half), trip_half)

    def up_copy(i):
        at = ups.at[(m, across_y)[i], up_rows]
        return pltpu.make_async_remote_copy(
            src_ref=at, dst_ref=at, send_sem=up_send, recv_sem=up_recv.at[i],
            device_id=({"mp": across_y}, {"graph": flip(g, 1)})[i], device_id_type=MESH)

    def up_beside():
        up_copy(0).wait_recv()
        up_copy(1).start()

    def up_home():
        up_copy(1).wait_recv()
        for i in relayed:
            early(1, i).start()

    def state_copy(i):
        cut = rows // 8
        at = states.at[m, (pl.ds(0, cut), pl.ds(cut, rows - cut))[i]]
        return pltpu.make_async_remote_copy(
            src_ref=at, dst_ref=at, send_sem=early_send.at[0], recv_sem=early_recv.at[0, 0],
            device_id={"mp": across_y}, device_id_type=MESH)

    def early_sent(which):
        at = (states, ups)[which].at[pl.ds(0, mp - 1 - which)]
        pltpu.make_async_remote_copy(
            src_ref=at, dst_ref=at, send_sem=early_send.at[which], recv_sem=early_recv.at[which, 0],
            device_id={"mp": flip(m, 1)}, device_id_type=MESH).wait_send()

    def early_relay(which):
        for i in relayed:
            first = brings[plan[i][1]]
            if [j for j in relayed if brings[plan[j][1]] == first][0] == i:
                early(which, first).wait_recv()
            early(which, i).start()

    def early_finish(which):
        at = (states, ups)[which].at[pl.ds(0, len(plan) - len(relays_from))]
        pltpu.make_async_remote_copy(
            src_ref=at, dst_ref=at, send_sem=early_send.at[which], recv_sem=early_recv.at[which, 1],
            device_id={"mp": flip(m, 1)}, device_id_type=MESH).wait_recv()

    eighth = weight.shape[1] // 8
    mine8 = g % 8

    def xor(a, k):
        for bit in (1, 2, 4):
            if k & bit:
                a = flip(a, bit)
        return a

    def part8(e):
        return pl.ds(pl.multiple_of(e * eighth, eighth), eighth)

    def feed_copy(src, f, e, sem, device):
        return pltpu.make_async_remote_copy(
            src_ref=src, dst_ref=joint.at[f, part8(e), far_cols], send_sem=feed_send.at[f], recv_sem=sem,
            device_id=device, device_id_type=MESH)

    def enter(f, far):
        e = xor(mine8, 4 * far)
        return feed_copy(joint.at[f, part8(e), own_cols], f, e, feed_y.at[f, far], {"mp": across_y})

    def near(f, far, k):
        e = xor(mine8, 4 * far)
        return feed_copy(joint.at[f, part8(e), far_cols], f, e, near_recv.at[f, far, 0 if k == 2 - far else 1], {"graph": xor(g, k)})

    def corner(f, far):
        came, goes = (2, 1) if far == 0 else (1, 2)
        e = xor(mine8, 4 * far + came)
        return feed_copy(joint.at[f, part8(e), far_cols], f, e, near_recv.at[f, far, 1], {"graph": xor(g, goes)})

    def feed_corner(f, far):
        near(f, far, 2 if far == 0 else 1).wait_recv()
        corner(f, far).start()

    def feed_ready(f):
        at = joint.at[f, pl.ds(0, 2 * eighth), far_cols]
        for far in range(2):
            pltpu.make_async_remote_copy(
                src_ref=at, dst_ref=at, send_sem=feed_send.at[f], recv_sem=near_recv.at[f, far, 1],
                device_id={"mp": across_y}, device_id_type=MESH).wait_recv()

    def feed_sent():
        for f in range(feeds):
            at = joint.at[f, :, far_cols]
            pltpu.make_async_remote_copy(
                src_ref=at, dst_ref=at, send_sem=feed_send.at[f], recv_sem=near_recv.at[f, 0, 0],
                device_id={"mp": across_y}, device_id_type=MESH).wait_send()

    class Sum:
        def __init__(self, which, part, got, summed, more, full):
            self.which, self.part, self.got = which, part, got
            self.summed, self.more, self.full = summed, more, full

        def first(self, j):
            return mp_copy(self.part.at[j, other], self.got.at[j], self.which, j, 0, 1)

        def step(self, j, b):
            return mp_copy(self.summed.at[j, b], self.more.at[j, b], self.which, j, 1 + b, bits[1 + b])

        def last(self, j):
            at = self.full.at[j, mine]
            return mp_copy(at, at, self.which, j, stages, 1)

        def into(self, j):
            self.first(j).start()

        def across(self, j):
            self.first(j).wait_recv()
            total = self.part[j, mine].astype(f32) + self.got[j].astype(f32)
            if stages > 1:
                self.summed[j, 0] = total.astype(bf16)
                self.step(j, 0).start()
            else:
                self.full[j, mine] = total.astype(bf16)

        def home(self, j):
            for b in range(stages - 1):
                self.step(j, b).wait_recv()
                total = self.summed[j, b].astype(f32) + self.more[j, b].astype(f32)
                if b + 2 < stages:
                    self.summed[j, b + 1] = total.astype(bf16)
                    self.step(j, b + 1).start()
                else:
                    self.full[j, mine] = total.astype(bf16)
            self.last(j).start()

        def done(self, j):
            self.last(j).wait_recv()

        def drain(self):
            for stage in range(stages + 1):
                mp_copy(self.got, self.got, self.which, 0, stage, 1).wait_send()

    sum0 = Sum(0, part_a, got_a, sum_a, more_a, full_a)
    sum1 = Sum(1, part_b, got_b, sum_b, more_b, full_b)

    def peer_of(k):
        if graph & (graph - 1):
            return (g + k) % graph
        return sum(bit * ((g // bit + k // bit) % 2) for bit in (1 << i for i in range(graph.bit_length() - 1)))

    peers = [peer_of(k) for k in range(graph - 1, 0, -1)] if graph <= 8 else None

    def arrived(whole, group, which):
        return pltpu.make_async_remote_copy(
            src_ref=whole, dst_ref=whole, send_sem=xc_send.at[group], recv_sem=xc_recv.at[which],
            device_id={"graph": (g + 1) % graph}, device_id_type=MESH)

    def exchange(group, which, src_at, dst_at, whole):
        def to(peer):
            pltpu.make_async_remote_copy(
                src_ref=src_at(peer), dst_ref=dst_at(g), send_sem=xc_send.at[group], recv_sem=xc_recv.at[which],
                device_id={"graph": peer}, device_id_type=MESH).start()

        def one(i, _):
            to(peer_of(graph - 1 - i))
            return 0

        def start():
            if peers is None:
                lax.fori_loop(0, graph - 1, one, 0)
            else:
                for peer in peers:
                    to(peer)

        return start, arrived(whole, group, which).wait_recv

    def block(ref, size):
        return lambda i: ref.at[pl.ds(pl.multiple_of(i * size, size), size)]

    def piece(ref, j, size):
        return lambda i: ref.at[j, pl.ds(pl.multiple_of(i * size, size), size)]

    def tiles(step):
        def one(i, _):
            step(pl.ds(pl.multiple_of(i * tile, tile), tile))
            return 0

        lax.fori_loop(0, triplets // tile, one, 0)

    def in_part(at):
        return one_hot(slot_total, in_ref[:, at])

    def out_part(at):
        return one_hot(slot_total, jnp.where(live_ref[:, at] > 0, out_ref[:, at], -1))

    state_in.wait()
    down_in.wait()
    with scope("s_proj"):
        projected = dot(states[m], down_ref[...]).astype(bf16)
        for j in range(pieces):
            part_a[j] = projected[:, j * lane:(j + 1) * lane]
    with scope("s_barrier"):
        pl.semaphore_wait(barrier, graph - 1 + len(bits))
    for j in range(pieces):
        sum0.into(j)
    state_copy(0).start()
    own_cols, far_cols = pl.ds(0, width), pl.ds(width, width)
    places = [(0, weight.at[0])] + [(2 * l + 1, weight.at[1 + l]) for l in range(layers)]
    places += [(2 * f + 2, joint.at[f, :, own_cols]) for f in range(feeds)]
    for k, at in places:
        pltpu.make_async_copy(dense_hbm.at[k], at, weight_sem.at[1 if k and k % 2 == 0 else 0]).start()

    lists_in.wait()
    with scope("s_hots"):
        for i in range(graph):
            list_hot[:, i * cap:(i + 1) * cap] = one_hot(rows, lists_ref[0, i:i + 1, :])
        in_in.wait()
        if kept:
            def keep_in(at):
                in_hot[:, at] = in_part(at)

            tiles(keep_in)
    with scope("s_across"):
        for j in range(pieces):
            sum0.across(j)
    up_in.wait()
    state_copy(1).start()
    out_in.wait()
    live_in.wait()
    if kept:
        def keep_out(at):
            out_hot[:, at] = out_part(at)

        with scope("s_outhot"):
            tiles(keep_out)

    basis_in.wait()
    bw_in.wait()
    depth = basis_ref.shape[0]
    pad = basis_stack.shape[0] // 3
    with scope("s_angles"):
        bw_high, bw_low = halves(bw_ref[...])
        bw_stack[...] = jnp.zeros_like(bw_stack)
        bw_stack[0:depth] = bw_high
        bw_stack[pad:pad + depth] = bw_high
        bw_stack[2 * pad:2 * pad + depth] = bw_low

        def angles(at):
            high, low = halves(basis_ref[:, at])
            basis_stack[:, at] = jnp.zeros((3 * pad, tile), bf16)
            basis_stack[0:depth, at] = high
            basis_stack[pad:pad + depth, at] = low
            basis_stack[2 * pad:2 * pad + depth, at] = high
            angle[:, at] = dot(bw_stack[...], basis_stack[:, at], 0, 0)

        tiles(angles)

    pltpu.make_async_copy(weight, weight, weight_sem.at[0]).wait()
    if feeds:
        pltpu.make_async_copy(joint.at[:, :, own_cols], joint.at[:, :, own_cols], weight_sem.at[1]).wait()
    if feeds:
        enter(0, 0).start()
    up_copy(0).start()
    if feeds:
        enter(0, 1).start()
    for f in range(1, feeds):
        enter(f, 0).start()
    step_rows = min(slot_total, 512)
    own = pl.ds(pl.multiple_of(g * cap, cap), cap)
    span = pl.ds(0, slot_total - cap)
    going = [exchange(0, j, piece(to_a, j, cap), piece(from_a, j, cap), from_a.at[j, span]) for j in range(pieces)]
    back = [exchange(1, pieces + j, piece(to_b, j, cap), piece(from_b, j, cap), from_b.at[j, span])
            for j in range(pieces)]

    def pick_piece(j):
        def pick(i, _):
            at = pl.ds(pl.multiple_of(i * step_rows, step_rows), step_rows)
            to_a[j, at, :] = dot(list_hot[:, at], full_a[j], 0, 0).astype(bf16)
            return 0

        sum0.done(j)
        lax.fori_loop(0, slot_total // step_rows, pick, 0)
        going[j][0]()
        from_a[j, own] = to_a[j, own]

    with scope("s_home"):
        sum0.home(0)
    with scope("s_home1"):
        for j in range(1, pieces):
            sum0.home(j)
            pick_piece(j - 1)
        pick_piece(pieces - 1)
    for which in range(2):
        for i in local[1:]:
            early(which, i).start()
    sum0.drain()

    for j in range(pieces):
        with scope("s_gowait%d" % j):
            going[j][1]()
        slots[...] = jnp.zeros_like(slots)
        received = from_a[j].astype(f32).T.astype(bf16)

        def trips(at):
            source = in_hot[:, at] if kept else in_part(at)
            value = dot(received, source) * angle[j * lane:(j + 1) * lane, at]
            target = out_hot[:, at] if kept else out_part(at)
            slots[...] += dot(target, value.astype(bf16), 1, 1)

        with scope("s_trips%d" % j):
            tiles(trips)
        to_b[j] = slots[...].astype(bf16)
        back[j][0]()
        from_b[j, own] = to_b[j, own]
    with scope("s_early0"):
        early_relay(0)

    def add_up(j):
        for index in range(mp):
            rest = dot(full_b[j], ups[index, j * lane:(j + 1) * lane, :])
            partial[index] = (states[index].astype(f32) if j == 0 else partial[index]) + rest

    for j in range(pieces):
        with scope("s_backwait%d" % j):
            back[j][1]()
        part_b[j] = dot(list_hot[...], from_b[j]).astype(bf16)
        sum1.into(j)
        if j == 0:
            with scope("s_upbeside"):
                up_beside()
        if j + 1 < pieces:
            sum1.across(j)
    with scope("s_sum1"):
        sum1.across(pieces - 1)
        with scope("s_early1"):
            up_home()
        with scope("s_feedspread"):
            for f in range(1, feeds):
                enter(f, 1).start()
            if feeds:
                for far in range(2):
                    enter(0, far).wait_recv()
                    near(0, far, 2 - far).start()
                    near(0, far, 1 + far).start()
        for j in range(pieces - 2):
            sum1.home(j)
        early_finish(0)
        early_finish(1)
        if pieces > 1:
            sum1.home(pieces - 2)
        for j in range(pieces - 2):
            sum1.done(j)
            add_up(j)
        with scope("s_lasthome"):
            sum1.home(pieces - 1)

    starts, sizes = chunks_of(half)
    order = [(h, t) for t in range(len(sizes)) for h in (0, 1)]

    def chunk(c):
        side, t = c
        start = side * half + starts[t]
        return pl.ds(start if isinstance(side, int) else pl.multiple_of(start, half // 2), sizes[t])

    def chunk_id(c):
        return c[0] * len(sizes) + c[1]

    def act_copy(layer, parity, c, which):
        bit, off = plan[which]
        at = acts.at[layer - 1, other_of(off), chunk(c)]
        return pltpu.make_async_remote_copy(
            src_ref=at, dst_ref=at,
            send_sem=act_send.at[parity, chunk_id(c)], recv_sem=act_recv.at[parity, chunk_id(c), 0 if which in relays_from else 1],
            device_id={"mp": flip(m, bit)}, device_id_type=MESH)

    def send(layer, parity, c):
        for i in local:
            act_copy(layer, parity, c, i).start()

    def relay(layer, parity, c):
        for i in relayed:
            first = brings[plan[i][1]]
            if [j for j in relayed if brings[plan[j][1]] == first][0] == i:
                act_copy(layer, parity, c, first).wait_recv()
            act_copy(layer, parity, c, i).start()

    def finish(layer, parity, c):
        at = acts.at[layer - 1, pl.ds(0, len(plan) - len(relays_from)), chunk(c)]
        pltpu.make_async_remote_copy(
            src_ref=at, dst_ref=at, send_sem=act_send.at[parity, chunk_id(c)],
            recv_sem=act_recv.at[parity, chunk_id(c), 1],
            device_id={"mp": flip(m, 1)}, device_id_type=MESH).wait_recv()

    def sent(layer, parity, c):
        at = acts.at[layer - 1, pl.ds(0, mp - 1), chunk(c)]
        pltpu.make_async_remote_copy(
            src_ref=at, dst_ref=at, send_sem=act_send.at[parity, chunk_id(c)], recv_sem=act_recv.at[parity, chunk_id(c), 0],
            device_id={"mp": flip(m, 1)}, device_id_type=MESH).wait_send()

    def product(k, at, held_weight):
        rows_in = jnp.concatenate([acts[k - 1, index, at, :] for index in range(mp)], axis=1)
        return silu(dot(rows_in, held_weight[...]))

    def core_copy(layer, c, i):
        at = acts.at[layer - 1, (m, across_y)[i], chunk(c)]
        return pltpu.make_async_remote_copy(
            src_ref=at, dst_ref=at, send_sem=core_send.at[chunk_id(c)], recv_sem=core_recv.at[chunk_id(c)],
            device_id={"mp": flip(m, 1)}, device_id_type=MESH)

    def core_both(layer, c):
        at = acts.at[layer - 1, pl.ds(0, 2), chunk(c)]
        return pltpu.make_async_remote_copy(
            src_ref=at, dst_ref=at, send_sem=core_send.at[chunk_id(c)], recv_sem=core_recv.at[chunk_id(c)],
            device_id={"mp": flip(m, 1)}, device_id_type=MESH)

    def core_sent(layer, c):
        core_both(layer, c).wait_send()

    late = range(max(pieces - 2, 0), pieces)
    late_up = pl.ds(late[0] * lane, len(late) * lane)
    with scope("s_begin"):
        for spot in range(len(order)):
            c = (m % 2 if spot % 2 == 0 else 1 - m % 2), spot // 2
            at = chunk(c)
            if spot == 1:
                for j in late:
                    sum1.done(j)
            update_rows = jnp.concatenate([full_b[j, at] for j in late], axis=1)
            firsts = []
            for index in range(mp):
                before = partial[index, at] if pieces > 2 else states[index, at].astype(f32)
                first = before + dot(update_rows, ups[index, late_up, :])
                partial[index, at] = first
                firsts.append(first.astype(bf16))
            total = dot(jnp.concatenate(firsts, axis=1), weight[0])
            hidden[at, :] = partial[m, at]
            acts[0, m, at, :] = silu(total).astype(bf16)
            send(1, 0, c)
        if feeds:
            with scope("s_corner0"):
                for far in range(2):
                    feed_corner(0, far)
        sum1.drain()
        arrived(from_a.at[:, span], 0, 0).wait_send()
        arrived(from_b.at[:, span], 1, 0).wait_send()
        for which in range(2):
            early_sent(which)
        pltpu.make_async_remote_copy(
            src_ref=ups.at[m], dst_ref=ups.at[m], send_sem=up_send, recv_sem=up_recv.at[0],
            device_id={"mp": across_y}, device_id_type=MESH).wait_send()
    atom_in.wait()
    atom_rows = min(atoms, 256)
    parts, part_lane = table.shape[0], table.shape[2]

    def columns(p):
        return slice(p * part_lane, (p + 1) * part_lane)

    def collect(c):
        at = chunk(c)
        stacked = jnp.concatenate(halves(hidden[at, :]), axis=0)

        def one(i, _):
            here_rows = pl.ds(pl.multiple_of(i * atom_rows, atom_rows), atom_rows)
            ids = one_hot(atom_rows, atom_ref[:, at] - i * atom_rows)
            total = dot(jnp.concatenate([ids, ids], axis=1), stacked)
            for p in range(parts):
                sums = total[:, columns(p)]
                if c != order[0]:
                    sums += atoms_own[p, here_rows]
                atoms_own[p, here_rows] = sums
                if c == order[-1]:
                    atoms_to[p, here_rows] = sums.astype(bf16)
            return 0

        lax.fori_loop(0, atoms // atom_rows, one, 0)

    def update(l, c):
        at = chunk(c)
        value = (hidden[at, :] + product(2 * l + 1, at, weight.at[1 + l])) * inv_root_two
        hidden[at, :] = value
        return value.astype(bf16)

    with scope("s_layer0"):
        with scope("s_feedrest0"):
            for f in range(1, feeds):
                for far in range(2):
                    enter(f, far).wait_recv()
                    near(f, far, 2 - far).start()
                    near(f, far, 1 + far).start()
        with scope("s_l0rel"):
            relay(1, 0, order[0])
        for spot, c in enumerate(order):
            with scope("s_l0fin%d" % spot):
                finish(1, 0, c)
            with scope("s_l0rel%d" % spot):
                if spot + 1 < len(order):
                    relay(1, 0, order[spot + 1])
            value = update(0, c)
            if layers > 1:
                acts[1, m, chunk(c), :] = value
                send(2, 1, c)
            with scope("s_l0feed%d" % spot):
                if spot == 2:
                    for f in range(1, feeds):
                        feed_corner(f, 0)
        if layers > 1:
            with scope("s_l1rel"):
                relay(2, 1, order[0])
    def layer_step(l, _):
        k, parity, f = 2 * l, l % 2, l - 1

        def second(c):
            core_both(k + 1, c).wait_recv()
            value = update(l, c)

            @pl.when(l + 1 < layers)
            def _():
                sent(k, 1 - parity, c)
                acts[k + 1, m, chunk(c), :] = value
                send(k + 2, 1 - parity, c)

            @pl.when(l + 1 == layers)
            def _():
                collect(c)

        with scope("s_feedwait"):
            feed_ready(f)
        def opening(c):
            at = chunk(c)

            @pl.when(l > 1)
            def _():
                core_sent(k - 1, c)

            both = product(k, at, joint.at[f]).astype(bf16)
            acts[k, m, at, :] = both[:, :width]
            acts[k, across_y, at, :] = both[:, width:]
            for i in range(2):
                core_copy(k + 1, c, i).start()

        for spot in range(0, len(order), 2):
            one, two = order[spot:spot + 2]
            with scope("s_finA%d" % spot):
                finish(k, parity, one)
            with scope("s_relA%d" % spot):
                relay(k, parity, two)
            opening(one)
            with scope("s_finB%d" % spot):
                finish(k, parity, two)
            opening(two)
            with scope("s_secA%d" % spot):
                second(one)
            with scope("s_relB%d" % spot):
                if spot + 2 < len(order):
                    relay(k, parity, order[spot + 2])

                    @pl.when(l == 1)
                    def _():
                        for later in range(1, feeds):
                            feed_corner(later, 1)
                else:
                    @pl.when(l + 1 < layers)
                    def _():
                        relay(k + 2, 1 - parity, order[0])
            with scope("s_secB%d" % spot):
                second(two)
        return 0

    with scope("s_layers"):
        lax.fori_loop(1, layers, layer_step, 0)

    here = pl.ds(pl.multiple_of(g * ATOM_DEV, ATOM_DEV), ATOM_DEV)
    atom_span = pl.ds(0, atoms - ATOM_DEV)
    gathers = [exchange(2, 2 * pieces + p, piece(atoms_to, p, ATOM_DEV), piece(atoms_from, p, ATOM_DEV),
                        atoms_from.at[p, atom_span]) for p in range(parts)]
    spreads = [exchange(3, 2 * pieces + parts + p, lambda peer, p=p: piece(table, p, ATOM_DEV)(g),
                        piece(table, p, ATOM_DEV), table.at[p, atom_span]) for p in range(parts)]

    if layers == 1:
        for c in order:
            collect(c)
    for p in range(parts):
        gathers[p][0]()
    for p in range(parts):
        atoms_from[p, here] = jnp.zeros((ATOM_DEV, part_lane), bf16)
    for c in order:
        sent(1, (layers - 1) % 2, c)
        if layers > 1:
            sent(1, layers % 2, c)
            core_sent(1, c)
    feed_sent()
    for p in range(parts):
        with scope("s_atomwait%d" % p):
            gathers[p][1]()

        def add(i, total):
            return total + atoms_from[p, pl.ds(pl.multiple_of(i * ATOM_DEV, ATOM_DEV), ATOM_DEV)].astype(f32)

        total = lax.fori_loop(0, graph, add, atoms_own[p, here])
        mine_out = silu(atom_scale * total).astype(bf16)
        table[p, here] = mine_out
        spreads[p][0]()
        atom_out_ref[:, columns(p)] = mine_out
    arrived(atoms_from.at[:, atom_span], 2, 0).wait_send()
    for p in range(parts):
        with scope("s_spreadwait%d" % p):
            spreads[p][1]()

        def spread(i, total):
            at = pl.ds(pl.multiple_of(i * atom_rows, atom_rows), atom_rows)
            return total + dot(one_hot(atom_rows, atom_ref[...] - i * atom_rows), table[p, at], 0, 0)

        total = lax.fori_loop(0, atoms // atom_rows, spread, hidden[:, columns(p)])
        edge_out_ref[:, columns(p)] = total.astype(bf16)
    arrived(table.at[:, atom_span], 3, 0).wait_send()


def hand_on(edge_ref, atom_ref, edge_out_ref, atom_out_ref, sem):
    edge = pltpu.make_async_copy(edge_ref, edge_out_ref, sem.at[0])
    atom = pltpu.make_async_copy(atom_ref, atom_out_ref, sem.at[1])
    edge.start()
    atom.start()
    edge.wait()
    atom.wait()


def local(graph, mp, edge_state, down_weight, basis, basis_weight, up_weight, dense_weight,
          send_rows, trip_in, trip_out, trip_live, edge_atom):
    rows, width = edge_state.shape
    trip = down_weight.shape[1]
    slot_total = graph * send_rows.shape[2]
    triplets = trip_in.shape[0]
    maps = dense_weight.shape[0] * dense_weight.shape[1]
    tile = 2048 if slot_total <= 512 else 128
    atoms = graph * ATOM_DEV
    feeds = dense_weight.shape[0] - 1
    chunks = 2 * len(chunks_of(rows // 2)[1])
    stages = mp.bit_length()
    extra = max(stages - 2, 1)
    half = rows // 2
    vmem = pltpu.VMEM
    pieces = trip // 128 if trip % 128 == 0 else 1
    lane = trip // pieces
    pad = -(-basis.shape[0] // 16) * 16
    hot_bytes = 2 * 2 * slot_total * triplets
    hots = [vmem((slot_total, triplets), bf16)] * 2 if hot_bytes <= 2 ** 24 else [None, None]
    reduce_bufs = [
        vmem((pieces, rows, lane), bf16), vmem((pieces, half, lane), bf16), vmem((pieces, extra, half, lane), bf16),
        vmem((pieces, extra, half, lane), bf16), vmem((pieces, rows, lane), bf16),
    ]
    dma = pltpu.SemaphoreType.DMA
    spec = pl.BlockSpec(memory_space=pltpu.VMEM)
    operands = [
        edge_state, down_weight, basis, basis_weight, up_weight,
        dense_weight.reshape((maps,) + dense_weight.shape[2:]),
        send_rows, trip_in.reshape(1, triplets), trip_out.reshape(1, triplets),
        trip_live.reshape(1, triplets), edge_atom.reshape(1, rows),
    ]
    inputs = [vmem(a.shape, a.dtype) for i, a in enumerate(operands) if i not in (0, 4, 5)]
    parts = width // 128 if width % 128 == 0 else 1
    atom_buf = (parts, atoms, width // parts)
    body = functools.partial(kernel, graph, mp, tile)
    before = [
        *inputs, dma((len(inputs) + 2,)),
        vmem((mp, rows, width), bf16), vmem((mp, trip, width), bf16), dma((2,)), dma((2, 2)), dma(()), dma((2,)),
        vmem((dense_weight.shape[0] + 1,) + dense_weight.shape[2:], bf16),
        vmem((feeds, dense_weight.shape[2], 2 * width), bf16), dma((2,)), dma((feeds,)), dma((feeds, 2)), dma((feeds, 2, 2)),
        dma((chunks,)), dma((chunks,)),
        *reduce_bufs, *reduce_bufs,
        dma((2, stages)), dma((2, pieces, stages)),
        *[vmem((pieces, slot_total, lane), bf16)] * 4,
        dma((4,)), dma((2 * pieces + 2 * parts,)),
        vmem((rows, slot_total), bf16), vmem((3 * pad, triplets), bf16), vmem((3 * pad, trip), bf16),
        vmem((trip, triplets), f32), vmem((slot_total, lane), f32),
    ]
    if hots[0] is None:
        hots, kept_body, at = [], body, len(operands) + 2 + len(before)
        body = lambda *refs: kept_body(*refs[:at], None, None, *refs[at:])
    outs = pl.pallas_call(
        body,
        out_shape=(
            pltpu.VMEM((rows, width), bf16),
            pltpu.VMEM((ATOM_DEV, width), bf16),
        ),
        in_specs=[pl.BlockSpec(memory_space=pl.ANY)] * len(operands),
        out_specs=(spec, spec),
        scratch_shapes=[
            *before, *hots,
            vmem((maps - 1, mp, rows, width), bf16), vmem((mp, rows, width), f32), vmem((rows, width), f32),
            dma((2, chunks)), dma((2, chunks, 2)),
            vmem(atom_buf, f32), vmem(atom_buf, bf16), vmem(atom_buf, bf16), vmem(atom_buf, bf16),
        ],
        compiler_params=pltpu.CompilerParams(
            collective_id=0, has_side_effects=True, vmem_limit_bytes=64000 * 1024
        ),
        name="edge_block",
    )(*operands)
    outs = [pltpu.with_memory_space_constraint(o, pltpu.VMEM) for o in outs]
    return pl.pallas_call(
        hand_on,
        out_shape=tuple(jax.ShapeDtypeStruct(o.shape, o.dtype) for o in outs),
        in_specs=[spec] * 2,
        out_specs=[pl.BlockSpec(memory_space=pl.ANY)] * 2,
        scratch_shapes=[dma((2,))],
        name="hand_on",
    )(*outs)


def solution(mesh):
    in_specs = (
        P("graph", "mp"),
        P("mp", None),
        P(None, ("graph", "mp")),
        P(),
        P(None, "mp"),
        P(None, None, None, "mp"),
        P("graph", "mp", None),
        P(("graph", "mp")),
        P(("graph", "mp")),
        P(("graph", "mp")),
        P("graph"),
    )
    out_specs = (P("graph", "mp"), P("graph", "mp"))
    body = functools.partial(local, mesh.shape["graph"], mesh.shape["mp"])
    return jax.shard_map(body, mesh=mesh, in_specs=in_specs, out_specs=out_specs, check_vma=False)
```

```python
import functools

import jax
import jax.numpy as jnp
from jax import lax
from jax.experimental import pallas as pl
from jax.experimental.pallas import tpu as pltpu
from jax.sharding import PartitionSpec as P

ATOM_DEV = 32

inv_root_two = 0.7071067811865476
atom_scale = 0.2

MESH = pl.DeviceIdType.MESH
bf16 = jnp.bfloat16
f32 = jnp.float32


def scope(name):
    return jax.named_scope(name)


def silu(v):
    return v / (1.0 + jnp.exp(-v))


def flip(index, bit):
    return index + bit - 2 * bit * ((index // bit) % 2)


def one_hot(rows, ids):
    shape = (rows, ids.shape[1])
    return jnp.where(lax.broadcasted_iota(jnp.int32, shape, 0) == ids, 1.0, 0.0).astype(bf16)


def dot(a, b, ca=1, cb=0):
    return lax.dot_general(a, b, (((ca,), (cb,)), ((), ())), preferred_element_type=f32)


def halves(v):
    high = v.astype(bf16)
    return high, (v - high.astype(f32)).astype(bf16)


def chunks_of(half):
    return (0, half // 2), (half // 2, half // 2)


def gather_plan(mp):
    plan, held, bit = [], [0], mp // 2
    while bit >= 1:
        plan += [(bit, off) for off in held]
        held += [bit ^ off for off in held]
        bit //= 2
    return plan, held


def kernel(
    graph, mp, tile,
    state_hbm, down_hbm, basis_hbm, bw_hbm, up_hbm, dense_hbm, lists_hbm, in_hbm, out_hbm, live_hbm, atom_hbm,
    edge_out_ref, atom_out_ref,
    down_ref, basis_ref, bw_ref, lists_ref, in_ref, out_ref, live_ref, atom_ref, load_sem,
    states, ups, early_send, early_recv, up_send, up_recv,
    weight, joint, weight_sem, feed_send, feed_y, near_recv, core_send, core_recv,
    part_a, got_a, sum_a, more_a, full_a,
    part_b, got_b, sum_b, more_b, full_b,
    red_send, red_recv,
    to_a, from_a, to_b, from_b, xc_send, xc_recv,
    list_hot, basis_stack, bw_stack, angle, slots, in_hot, out_hot,
    acts, partial, hidden, act_send, act_recv,
    atoms_own, atoms_to, atoms_from, table,
):
    g = lax.axis_index("graph")
    m = lax.axis_index("mp")
    rows, width = hidden.shape
    trip = down_ref.shape[1]
    layers = weight.shape[0] - 1
    cap = lists_ref.shape[2]
    slot_total = graph * cap
    pieces, lane = to_a.shape[0], to_a.shape[2]
    kept = in_hot is not None
    triplets = in_ref.shape[1]
    atoms = graph * ATOM_DEV
    half = rows // 2
    feeds = layers - 1
    bits = [1 << i for i in range(mp.bit_length() - 1)]
    stages = len(bits)

    barrier = pltpu.get_barrier_semaphore()

    def greet(k, _):
        pl.semaphore_signal(barrier, inc=1, device_id={"graph": (g + k) % graph}, device_id_type=MESH)
        return 0

    lax.fori_loop(1, graph, greet, 0)
    for bit in bits:
        pl.semaphore_signal(barrier, inc=1, device_id={"mp": flip(m, bit)}, device_id_type=MESH)

    hbm = [state_hbm, down_hbm, lists_hbm, in_hbm, out_hbm, live_hbm, basis_hbm, bw_hbm, up_hbm, atom_hbm]
    here_refs = [
        states.at[m], down_ref, lists_ref, in_ref, out_ref, live_ref, basis_ref, bw_ref, ups.at[m], atom_ref]
    loads = [pltpu.make_async_copy(a, b, load_sem.at[i]) for i, (a, b) in enumerate(zip(hbm, here_refs))]
    for load in loads:
        load.start()
    state_in, down_in, lists_in, in_in, out_in, live_in, basis_in, bw_in, up_in, atom_in = loads

    def mp_copy(src, dst, which, j, stage, bit):
        return pltpu.make_async_remote_copy(
            src_ref=src, dst_ref=dst, send_sem=red_send.at[which, stage], recv_sem=red_recv.at[which, j, stage],
            device_id={"mp": flip(m, bit)}, device_id_type=MESH)

    mine = pl.ds(pl.multiple_of((m % 2) * half, half), half)
    other = pl.ds(pl.multiple_of(half - (m % 2) * half, half), half)

    plan, held = gather_plan(mp)

    def other_of(off):
        index = m
        for bit in bits:
            if off & bit:
                index = flip(index, bit)
        return index

    local = [i for i, (bit, off) in enumerate(plan) if off == 0]
    relayed = [i for i, (bit, off) in enumerate(plan) if off != 0]
    brings = {bit ^ off: i for i, (bit, off) in enumerate(plan)}
    relays_from = sorted({brings[plan[i][1]] for i in relayed})

    across_y = flip(m, mp // 2)

    def early(which, i):
        bit, off = plan[i]
        at = (states, ups)[which].at[other_of(off)]
        return pltpu.make_async_remote_copy(
            src_ref=at, dst_ref=at, send_sem=early_send.at[which], recv_sem=early_recv.at[which, 0 if i in relays_from else 1],
            device_id={"mp": flip(m, bit)}, device_id_type=MESH)

    trip_half = trip // 2
    up_rows = pl.ds(pl.multiple_of((g % 2) * trip_half, trip_half), trip_half)

    def up_copy(i):
        at = ups.at[(m, across_y)[i], up_rows]
        return pltpu.make_async_remote_copy(
            src_ref=at, dst_ref=at, send_sem=up_send, recv_sem=up_recv.at[i],
            device_id=({"mp": across_y}, {"graph": flip(g, 1)})[i], device_id_type=MESH)

    def up_beside():
        up_copy(0).wait_recv()
        up_copy(1).start()

    def up_home():
        up_copy(1).wait_recv()
        for i in relayed:
            early(1, i).start()

    def state_copy(i):
        cut = rows // 8
        at = states.at[m, (pl.ds(0, cut), pl.ds(cut, rows - cut))[i]]
        return pltpu.make_async_remote_copy(
            src_ref=at, dst_ref=at, send_sem=early_send.at[0], recv_sem=early_recv.at[0, 0],
            device_id={"mp": across_y}, device_id_type=MESH)

    def early_sent(which):
        at = (states, ups)[which].at[pl.ds(0, mp - 1 - which)]
        pltpu.make_async_remote_copy(
            src_ref=at, dst_ref=at, send_sem=early_send.at[which], recv_sem=early_recv.at[which, 0],
            device_id={"mp": flip(m, 1)}, device_id_type=MESH).wait_send()

    def early_relay(which):
        for i in relayed:
            first = brings[plan[i][1]]
            if [j for j in relayed if brings[plan[j][1]] == first][0] == i:
                early(which, first).wait_recv()
            early(which, i).start()

    def early_finish(which):
        at = (states, ups)[which].at[pl.ds(0, len(plan) - len(relays_from))]
        pltpu.make_async_remote_copy(
            src_ref=at, dst_ref=at, send_sem=early_send.at[which], recv_sem=early_recv.at[which, 1],
            device_id={"mp": flip(m, 1)}, device_id_type=MESH).wait_recv()

    eighth = weight.shape[1] // 8
    mine8 = g % 8

    def xor(a, k):
        for bit in (1, 2, 4):
            if k & bit:
                a = flip(a, bit)
        return a

    def part8(e):
        return pl.ds(pl.multiple_of(e * eighth, eighth), eighth)

    def feed_copy(src, f, e, sem, device):
        return pltpu.make_async_remote_copy(
            src_ref=src, dst_ref=joint.at[f, part8(e), far_cols], send_sem=feed_send.at[f], recv_sem=sem,
            device_id=device, device_id_type=MESH)

    def enter(f, far):
        e = xor(mine8, 4 * far)
        return feed_copy(joint.at[f, part8(e), own_cols], f, e, feed_y.at[f, far], {"mp": across_y})

    def near(f, far, k):
        e = xor(mine8, 4 * far)
        return feed_copy(joint.at[f, part8(e), far_cols], f, e, near_recv.at[f, far, 0 if k == 2 - far else 1], {"graph": xor(g, k)})

    def corner(f, far):
        came, goes = (2, 1) if far == 0 else (1, 2)
        e = xor(mine8, 4 * far + came)
        return feed_copy(joint.at[f, part8(e), far_cols], f, e, near_recv.at[f, far, 1], {"graph": xor(g, goes)})

    def feed_corner(f, far):
        near(f, far, 2 if far == 0 else 1).wait_recv()
        corner(f, far).start()

    def feed_ready(f):
        at = joint.at[f, pl.ds(0, 2 * eighth), far_cols]
        for far in range(2):
            pltpu.make_async_remote_copy(
                src_ref=at, dst_ref=at, send_sem=feed_send.at[f], recv_sem=near_recv.at[f, far, 1],
                device_id={"mp": across_y}, device_id_type=MESH).wait_recv()

    def feed_sent():
        for f in range(feeds):
            at = joint.at[f, :, far_cols]
            pltpu.make_async_remote_copy(
                src_ref=at, dst_ref=at, send_sem=feed_send.at[f], recv_sem=near_recv.at[f, 0, 0],
                device_id={"mp": across_y}, device_id_type=MESH).wait_send()

    class Sum:
        def __init__(self, which, part, got, summed, more, full):
            self.which, self.part, self.got = which, part, got
            self.summed, self.more, self.full = summed, more, full

        def first(self, j):
            return mp_copy(self.part.at[j, other], self.got.at[j], self.which, j, 0, 1)

        def step(self, j, b):
            return mp_copy(self.summed.at[j, b], self.more.at[j, b], self.which, j, 1 + b, bits[1 + b])

        def last(self, j):
            at = self.full.at[j, mine]
            return mp_copy(at, at, self.which, j, stages, 1)

        def into(self, j):
            self.first(j).start()

        def across(self, j):
            self.first(j).wait_recv()
            total = self.part[j, mine].astype(f32) + self.got[j].astype(f32)
            if stages > 1:
                self.summed[j, 0] = total.astype(bf16)
                self.step(j, 0).start()
            else:
                self.full[j, mine] = total.astype(bf16)

        def home(self, j):
            for b in range(stages - 1):
                self.step(j, b).wait_recv()
                total = self.summed[j, b].astype(f32) + self.more[j, b].astype(f32)
                if b + 2 < stages:
                    self.summed[j, b + 1] = total.astype(bf16)
                    self.step(j, b + 1).start()
                else:
                    self.full[j, mine] = total.astype(bf16)
            self.last(j).start()

        def done(self, j):
            self.last(j).wait_recv()

        def drain(self):
            for stage in range(stages + 1):
                mp_copy(self.got, self.got, self.which, 0, stage, 1).wait_send()

    sum0 = Sum(0, part_a, got_a, sum_a, more_a, full_a)
    sum1 = Sum(1, part_b, got_b, sum_b, more_b, full_b)

    def peer_of(k):
        if graph & (graph - 1):
            return (g + k) % graph
        return sum(bit * ((g // bit + k // bit) % 2) for bit in (1 << i for i in range(graph.bit_length() - 1)))

    peers = [peer_of(k) for k in range(graph - 1, 0, -1)] if graph <= 8 else None

    def arrived(whole, group, which):
        return pltpu.make_async_remote_copy(
            src_ref=whole, dst_ref=whole, send_sem=xc_send.at[group], recv_sem=xc_recv.at[which],
            device_id={"graph": (g + 1) % graph}, device_id_type=MESH)

    def exchange(group, which, src_at, dst_at, whole):
        def to(peer):
            pltpu.make_async_remote_copy(
                src_ref=src_at(peer), dst_ref=dst_at(g), send_sem=xc_send.at[group], recv_sem=xc_recv.at[which],
                device_id={"graph": peer}, device_id_type=MESH).start()

        def one(i, _):
            to(peer_of(graph - 1 - i))
            return 0

        def start():
            if peers is None:
                lax.fori_loop(0, graph - 1, one, 0)
            else:
                for peer in peers:
                    to(peer)

        return start, arrived(whole, group, which).wait_recv

    def block(ref, size):
        return lambda i: ref.at[pl.ds(pl.multiple_of(i * size, size), size)]

    def piece(ref, j, size):
        return lambda i: ref.at[j, pl.ds(pl.multiple_of(i * size, size), size)]

    def tiles(step):
        def one(i, _):
            step(pl.ds(pl.multiple_of(i * tile, tile), tile))
            return 0

        lax.fori_loop(0, triplets // tile, one, 0)

    def in_part(at):
        return one_hot(slot_total, in_ref[:, at])

    def out_part(at):
        return one_hot(slot_total, jnp.where(live_ref[:, at] > 0, out_ref[:, at], -1))

    state_in.wait()
    down_in.wait()
    with scope("s_proj"):
        projected = dot(states[m], down_ref[...]).astype(bf16)
        for j in range(pieces):
            part_a[j] = projected[:, j * lane:(j + 1) * lane]
    with scope("s_barrier"):
        pl.semaphore_wait(barrier, graph - 1 + len(bits))
    for j in range(pieces):
        sum0.into(j)
    state_copy(0).start()
    own_cols, far_cols = pl.ds(0, width), pl.ds(width, width)
    places = [(0, weight.at[0])] + [(2 * l + 1, weight.at[1 + l]) for l in range(layers)]
    places += [(2 * f + 2, joint.at[f, :, own_cols]) for f in range(feeds)]
    for k, at in places:
        pltpu.make_async_copy(dense_hbm.at[k], at, weight_sem.at[1 if k and k % 2 == 0 else 0]).start()

    lists_in.wait()
    with scope("s_hots"):
        for i in range(graph):
            list_hot[:, i * cap:(i + 1) * cap] = one_hot(rows, lists_ref[0, i:i + 1, :])
        in_in.wait()
        if kept:
            def keep_in(at):
                in_hot[:, at] = in_part(at)

            tiles(keep_in)
    with scope("s_across"):
        for j in range(pieces):
            sum0.across(j)
    up_in.wait()
    state_copy(1).start()
    out_in.wait()
    live_in.wait()
    if kept:
        def keep_out(at):
            out_hot[:, at] = out_part(at)

        with scope("s_outhot"):
            tiles(keep_out)

    basis_in.wait()
    bw_in.wait()
    depth = basis_ref.shape[0]
    pad = basis_stack.shape[0] // 3
    with scope("s_angles"):
        bw_high, bw_low = halves(bw_ref[...])
        bw_stack[...] = jnp.zeros_like(bw_stack)
        bw_stack[0:depth] = bw_high
        bw_stack[pad:pad + depth] = bw_high
        bw_stack[2 * pad:2 * pad + depth] = bw_low

        def angles(at):
            high, low = halves(basis_ref[:, at])
            basis_stack[:, at] = jnp.zeros((3 * pad, tile), bf16)
            basis_stack[0:depth, at] = high
            basis_stack[pad:pad + depth, at] = low
            basis_stack[2 * pad:2 * pad + depth, at] = high
            angle[:, at] = dot(bw_stack[...], basis_stack[:, at], 0, 0)

        tiles(angles)

    pltpu.make_async_copy(weight, weight, weight_sem.at[0]).wait()
    if feeds:
        pltpu.make_async_copy(joint.at[:, :, own_cols], joint.at[:, :, own_cols], weight_sem.at[1]).wait()
    if feeds:
        enter(0, 0).start()
    up_copy(0).start()
    if feeds:
        enter(0, 1).start()
    for f in range(1, feeds):
        enter(f, 0).start()
    step_rows = min(slot_total, 512)
    own = pl.ds(pl.multiple_of(g * cap, cap), cap)
    span = pl.ds(0, slot_total - cap)
    most = xc_recv.shape[0] // 2
    going = [exchange(0, j, piece(to_a, j, cap), piece(from_a, j, cap), from_a.at[j, span]) for j in range(pieces)]
    back = [exchange(1, most + j, piece(to_b, j, cap), piece(from_b, j, cap), from_b.at[j, span])
            for j in range(pieces)]

    def pick_piece(j):
        def pick(i, _):
            at = pl.ds(pl.multiple_of(i * step_rows, step_rows), step_rows)
            to_a[j, at, :] = dot(list_hot[:, at], full_a[j], 0, 0).astype(bf16)
            return 0

        sum0.done(j)
        lax.fori_loop(0, slot_total // step_rows, pick, 0)
        going[j][0]()
        from_a[j, own] = to_a[j, own]

    with scope("s_home"):
        for j in range(pieces):
            sum0.home(j)
            pick_piece(j)
    for which in range(2):
        for i in local[1:]:
            early(which, i).start()
    sum0.drain()

    for j in range(pieces):
        with scope("s_gowait%d" % j):
            going[j][1]()
        slots[...] = jnp.zeros_like(slots)
        received = from_a[j].astype(f32).T.astype(bf16)

        def trips(at):
            source = in_hot[:, at] if kept else in_part(at)
            value = dot(received, source) * angle[j * lane:(j + 1) * lane, at]
            target = out_hot[:, at] if kept else out_part(at)
            slots[...] += dot(target, value.astype(bf16), 1, 1)

        with scope("s_trips%d" % j):
            tiles(trips)
        to_b[j] = slots[...].astype(bf16)
        back[j][0]()
        from_b[j, own] = to_b[j, own]
    with scope("s_early0"):
        early_relay(0)

    def add_up(j):
        for index in range(mp):
            rest = dot(full_b[j], ups[index, j * lane:(j + 1) * lane, :])
            partial[index] = (states[index].astype(f32) if j == 0 else partial[index]) + rest

    for j in range(pieces):
        with scope("s_backwait%d" % j):
            back[j][1]()
        part_b[j] = dot(list_hot[...], from_b[j]).astype(bf16)
        sum1.into(j)
        if j == 0:
            with scope("s_upbeside"):
                up_beside()
        if j + 1 < pieces:
            sum1.across(j)
    with scope("s_sum1"):
        sum1.across(pieces - 1)
        with scope("s_early1"):
            up_home()
        with scope("s_feedspread"):
            for f in range(1, feeds):
                enter(f, 1).start()
            if feeds:
                for far in range(2):
                    enter(0, far).wait_recv()
                    near(0, far, 2 - far).start()
                    near(0, far, 1 + far).start()
        for j in range(pieces - 2):
            sum1.home(j)
        early_finish(0)
        early_finish(1)
        if pieces > 1:
            sum1.home(pieces - 2)
        for j in range(pieces - 2):
            sum1.done(j)
            add_up(j)
        with scope("s_lasthome"):
            sum1.home(pieces - 1)

    starts, sizes = chunks_of(half)
    order = [(h, t) for t in range(len(sizes)) for h in (0, 1)]

    def chunk(c):
        side, t = c
        start = side * half + starts[t]
        return pl.ds(start if isinstance(side, int) else pl.multiple_of(start, half // 2), sizes[t])

    def chunk_id(c):
        return c[0] * len(sizes) + c[1]

    def act_copy(layer, parity, c, which):
        bit, off = plan[which]
        at = acts.at[layer - 1, other_of(off), chunk(c)]
        return pltpu.make_async_remote_copy(
            src_ref=at, dst_ref=at,
            send_sem=act_send.at[parity, chunk_id(c)], recv_sem=act_recv.at[parity, chunk_id(c), 0 if which in relays_from else 1],
            device_id={"mp": flip(m, bit)}, device_id_type=MESH)

    def send(layer, parity, c):
        for i in local:
            act_copy(layer, parity, c, i).start()

    def relay(layer, parity, c):
        for i in relayed:
            first = brings[plan[i][1]]
            if [j for j in relayed if brings[plan[j][1]] == first][0] == i:
                act_copy(layer, parity, c, first).wait_recv()
            act_copy(layer, parity, c, i).start()

    def finish(layer, parity, c):
        at = acts.at[layer - 1, pl.ds(0, len(plan) - len(relays_from)), chunk(c)]
        pltpu.make_async_remote_copy(
            src_ref=at, dst_ref=at, send_sem=act_send.at[parity, chunk_id(c)],
            recv_sem=act_recv.at[parity, chunk_id(c), 1],
            device_id={"mp": flip(m, 1)}, device_id_type=MESH).wait_recv()

    def sent(layer, parity, c):
        at = acts.at[layer - 1, pl.ds(0, mp - 1), chunk(c)]
        pltpu.make_async_remote_copy(
            src_ref=at, dst_ref=at, send_sem=act_send.at[parity, chunk_id(c)], recv_sem=act_recv.at[parity, chunk_id(c), 0],
            device_id={"mp": flip(m, 1)}, device_id_type=MESH).wait_send()

    def product(k, at, held_weight):
        rows_in = jnp.concatenate([acts[k - 1, index, at, :] for index in range(mp)], axis=1)
        return silu(dot(rows_in, held_weight[...]))

    def core_copy(layer, c, i):
        at = acts.at[layer - 1, (m, across_y)[i], chunk(c)]
        return pltpu.make_async_remote_copy(
            src_ref=at, dst_ref=at, send_sem=core_send.at[chunk_id(c)], recv_sem=core_recv.at[chunk_id(c)],
            device_id={"mp": flip(m, 1)}, device_id_type=MESH)

    def core_both(layer, c):
        at = acts.at[layer - 1, pl.ds(0, 2), chunk(c)]
        return pltpu.make_async_remote_copy(
            src_ref=at, dst_ref=at, send_sem=core_send.at[chunk_id(c)], recv_sem=core_recv.at[chunk_id(c)],
            device_id={"mp": flip(m, 1)}, device_id_type=MESH)

    def core_sent(layer, c):
        core_both(layer, c).wait_send()

    late = range(max(pieces - 2, 0), pieces)
    late_up = pl.ds(late[0] * lane, len(late) * lane)
    with scope("s_begin"):
        for spot in range(len(order)):
            c = (m % 2 if spot % 2 == 0 else 1 - m % 2), spot // 2
            at = chunk(c)
            if spot == 1:
                for j in late:
                    sum1.done(j)
            update_rows = jnp.concatenate([full_b[j, at] for j in late], axis=1)
            firsts = []
            for index in range(mp):
                before = partial[index, at] if pieces > 2 else states[index, at].astype(f32)
                first = before + dot(update_rows, ups[index, late_up, :])
                partial[index, at] = first
                firsts.append(first.astype(bf16))
            total = dot(jnp.concatenate(firsts, axis=1), weight[0])
            hidden[at, :] = partial[m, at]
            acts[0, m, at, :] = silu(total).astype(bf16)
            send(1, 0, c)
        if feeds:
            with scope("s_corner0"):
                for far in range(2):
                    feed_corner(0, far)
        sum1.drain()
        arrived(from_a.at[:, span], 0, 0).wait_send()
        arrived(from_b.at[:, span], 1, 0).wait_send()
        for which in range(2):
            early_sent(which)
        pltpu.make_async_remote_copy(
            src_ref=ups.at[m], dst_ref=ups.at[m], send_sem=up_send, recv_sem=up_recv.at[0],
            device_id={"mp": across_y}, device_id_type=MESH).wait_send()
    atom_in.wait()
    atom_rows = min(atoms, 256)
    parts, part_lane = table.shape[0], table.shape[2]

    def columns(p):
        return slice(p * part_lane, (p + 1) * part_lane)

    def collect(c):
        at = chunk(c)
        stacked = jnp.concatenate(halves(hidden[at, :]), axis=0)

        def one(i, _):
            here_rows = pl.ds(pl.multiple_of(i * atom_rows, atom_rows), atom_rows)
            ids = one_hot(atom_rows, atom_ref[:, at] - i * atom_rows)
            total = dot(jnp.concatenate([ids, ids], axis=1), stacked)
            for p in range(parts):
                sums = total[:, columns(p)]
                if c != order[0]:
                    sums += atoms_own[p, here_rows]
                atoms_own[p, here_rows] = sums
                if c == order[-1]:
                    atoms_to[p, here_rows] = sums.astype(bf16)
            return 0

        lax.fori_loop(0, atoms // atom_rows, one, 0)

    def update(l, c):
        at = chunk(c)
        value = (hidden[at, :] + product(2 * l + 1, at, weight.at[1 + l])) * inv_root_two
        hidden[at, :] = value
        return value.astype(bf16)

    with scope("s_layer0"):
        with scope("s_feedrest0"):
            for f in range(1, feeds):
                for far in range(2):
                    enter(f, far).wait_recv()
                    near(f, far, 2 - far).start()
                    near(f, far, 1 + far).start()
        with scope("s_l0rel"):
            relay(1, 0, order[0])
        for spot, c in enumerate(order):
            with scope("s_l0fin%d" % spot):
                finish(1, 0, c)
            with scope("s_l0rel%d" % spot):
                if spot + 1 < len(order):
                    relay(1, 0, order[spot + 1])
            if spot + 1 == len(order) and layers > 1:
                with scope("s_l1rel"):
                    relay(2, 1, order[0])
            value = update(0, c)
            if layers > 1:
                acts[1, m, chunk(c), :] = value
                send(2, 1, c)
            with scope("s_l0feed%d" % spot):
                if spot == 2:
                    for f in range(1, feeds):
                        feed_corner(f, 0)

    def layer_step(l, _):
        k, parity, f = 2 * l, l % 2, l - 1

        def second(c):
            core_both(k + 1, c).wait_recv()
            value = update(l, c)

            @pl.when(l + 1 < layers)
            def _():
                sent(k, 1 - parity, c)
                acts[k + 1, m, chunk(c), :] = value
                send(k + 2, 1 - parity, c)

            @pl.when(l + 1 == layers)
            def _():
                collect(c)

        with scope("s_feedwait"):
            feed_ready(f)
        def opening(c):
            at = chunk(c)

            @pl.when(l > 1)
            def _():
                core_sent(k - 1, c)

            both = product(k, at, joint.at[f]).astype(bf16)
            acts[k, m, at, :] = both[:, :width]
            acts[k, across_y, at, :] = both[:, width:]
            for i in range(2):
                core_copy(k + 1, c, i).start()

        for spot in range(0, len(order), 2):
            one, two = order[spot:spot + 2]
            with scope("s_finA%d" % spot):
                finish(k, parity, one)
            with scope("s_relA%d" % spot):
                relay(k, parity, two)
            opening(one)
            with scope("s_finB%d" % spot):
                finish(k, parity, two)
            opening(two)
            with scope("s_secA%d" % spot):
                second(one)
            with scope("s_relB%d" % spot):
                if spot + 2 < len(order):
                    relay(k, parity, order[spot + 2])

                    @pl.when(l == 1)
                    def _():
                        for later in range(1, feeds):
                            feed_corner(later, 1)
                else:
                    @pl.when(l + 1 < layers)
                    def _():
                        relay(k + 2, 1 - parity, order[0])
            with scope("s_secB%d" % spot):
                second(two)
        return 0

    with scope("s_layers"):
        lax.fori_loop(1, layers, layer_step, 0)

    here = pl.ds(pl.multiple_of(g * ATOM_DEV, ATOM_DEV), ATOM_DEV)
    atom_span = pl.ds(0, atoms - ATOM_DEV)
    gathers = [exchange(0, p, piece(atoms_to, p, ATOM_DEV), piece(atoms_from, p, ATOM_DEV),
                        atoms_from.at[p, atom_span]) for p in range(parts)]
    spreads = [exchange(1, most + p, lambda peer, p=p: piece(table, p, ATOM_DEV)(g),
                        piece(table, p, ATOM_DEV), table.at[p, atom_span]) for p in range(parts)]

    if layers == 1:
        for c in order:
            collect(c)
    for p in range(parts):
        gathers[p][0]()
    for p in range(parts):
        atoms_from[p, here] = jnp.zeros((ATOM_DEV, part_lane), bf16)
    for c in order:
        sent(1, (layers - 1) % 2, c)
        if layers > 1:
            sent(1, layers % 2, c)
            core_sent(1, c)
    feed_sent()
    for p in range(parts):
        with scope("s_atomwait%d" % p):
            gathers[p][1]()

        def add(i, total):
            return total + atoms_from[p, pl.ds(pl.multiple_of(i * ATOM_DEV, ATOM_DEV), ATOM_DEV)].astype(f32)

        total = lax.fori_loop(0, graph, add, atoms_own[p, here])
        mine_out = silu(atom_scale * total).astype(bf16)
        table[p, here] = mine_out
        spreads[p][0]()
        atom_out_ref[:, columns(p)] = mine_out
    arrived(atoms_from.at[:, atom_span], 0, 0).wait_send()
    for p in range(parts):
        with scope("s_spreadwait%d" % p):
            spreads[p][1]()

        def spread(i, total):
            at = pl.ds(pl.multiple_of(i * atom_rows, atom_rows), atom_rows)
            return total + dot(one_hot(atom_rows, atom_ref[...] - i * atom_rows), table[p, at], 0, 0)

        total = lax.fori_loop(0, atoms // atom_rows, spread, hidden[:, columns(p)])
        edge_out_ref[:, columns(p)] = total.astype(bf16)
    arrived(table.at[:, atom_span], 1, 0).wait_send()


def hand_on(edge_ref, atom_ref, edge_out_ref, atom_out_ref, sem):
    edge = pltpu.make_async_copy(edge_ref, edge_out_ref, sem.at[0])
    atom = pltpu.make_async_copy(atom_ref, atom_out_ref, sem.at[1])
    edge.start()
    atom.start()
    edge.wait()
    atom.wait()


def local(graph, mp, edge_state, down_weight, basis, basis_weight, up_weight, dense_weight,
          send_rows, trip_in, trip_out, trip_live, edge_atom):
    rows, width = edge_state.shape
    trip = down_weight.shape[1]
    slot_total = graph * send_rows.shape[2]
    triplets = trip_in.shape[0]
    maps = dense_weight.shape[0] * dense_weight.shape[1]
    tile = 2048 if slot_total <= 512 else 128
    atoms = graph * ATOM_DEV
    feeds = dense_weight.shape[0] - 1
    chunks = 2 * len(chunks_of(rows // 2)[1])
    stages = mp.bit_length()
    extra = max(stages - 2, 1)
    half = rows // 2
    vmem = pltpu.VMEM
    pieces = trip // 128 if trip % 128 == 0 else 1
    lane = trip // pieces
    pad = -(-basis.shape[0] // 16) * 16
    hot_bytes = 2 * 2 * slot_total * triplets
    hots = [vmem((slot_total, triplets), bf16)] * 2 if hot_bytes <= 2 ** 24 else [None, None]
    reduce_bufs = [
        vmem((pieces, rows, lane), bf16), vmem((pieces, half, lane), bf16), vmem((pieces, extra, half, lane), bf16),
        vmem((pieces, extra, half, lane), bf16), vmem((pieces, rows, lane), bf16),
    ]
    dma = pltpu.SemaphoreType.DMA
    spec = pl.BlockSpec(memory_space=pltpu.VMEM)
    operands = [
        edge_state, down_weight, basis, basis_weight, up_weight,
        dense_weight.reshape((maps,) + dense_weight.shape[2:]),
        send_rows, trip_in.reshape(1, triplets), trip_out.reshape(1, triplets),
        trip_live.reshape(1, triplets), edge_atom.reshape(1, rows),
    ]
    inputs = [vmem(a.shape, a.dtype) for i, a in enumerate(operands) if i not in (0, 4, 5)]
    parts = width // 128 if width % 128 == 0 else 1
    atom_buf = (parts, atoms, width // parts)
    body = functools.partial(kernel, graph, mp, tile)
    before = [
        *inputs, dma((len(inputs) + 2,)),
        vmem((mp, rows, width), bf16), vmem((mp, trip, width), bf16), dma((2,)), dma((2, 2)), dma(()), dma((2,)),
        vmem((dense_weight.shape[0] + 1,) + dense_weight.shape[2:], bf16),
        vmem((feeds, dense_weight.shape[2], 2 * width), bf16), dma((2,)), dma((feeds,)), dma((feeds, 2)), dma((feeds, 2, 2)),
        dma((chunks,)), dma((chunks,)),
        *reduce_bufs, *reduce_bufs,
        dma((2, stages)), dma((2, pieces, stages)),
        *[vmem((pieces, slot_total, lane), bf16)] * 4,
        dma((2,)), dma((2 * max(pieces, parts),)),
        vmem((rows, slot_total), bf16), vmem((3 * pad, triplets), bf16), vmem((3 * pad, trip), bf16),
        vmem((trip, triplets), f32), vmem((slot_total, lane), f32),
    ]
    if hots[0] is None:
        hots, kept_body, at = [], body, len(operands) + 2 + len(before)
        body = lambda *refs: kept_body(*refs[:at], None, None, *refs[at:])
    outs = pl.pallas_call(
        body,
        out_shape=(
            pltpu.VMEM((rows, width), bf16),
            pltpu.VMEM((ATOM_DEV, width), bf16),
        ),
        in_specs=[pl.BlockSpec(memory_space=pl.ANY)] * len(operands),
        out_specs=(spec, spec),
        scratch_shapes=[
            *before, *hots,
            vmem((maps - 1, mp, rows, width), bf16), vmem((mp, rows, width), f32), vmem((rows, width), f32),
            dma((2, chunks)), dma((2, chunks, 2)),
            vmem(atom_buf, f32), vmem(atom_buf, bf16), vmem(atom_buf, bf16), vmem(atom_buf, bf16),
        ],
        compiler_params=pltpu.CompilerParams(
            collective_id=0, has_side_effects=True, vmem_limit_bytes=64000 * 1024
        ),
        name="edge_block",
    )(*operands)
    outs = [pltpu.with_memory_space_constraint(o, pltpu.VMEM) for o in outs]
    return pl.pallas_call(
        hand_on,
        out_shape=tuple(jax.ShapeDtypeStruct(o.shape, o.dtype) for o in outs),
        in_specs=[spec] * 2,
        out_specs=[pl.BlockSpec(memory_space=pl.ANY)] * 2,
        scratch_shapes=[dma((2,))],
        name="hand_on",
    )(*outs)


def solution(mesh):
    in_specs = (
        P("graph", "mp"),
        P("mp", None),
        P(None, ("graph", "mp")),
        P(),
        P(None, "mp"),
        P(None, None, None, "mp"),
        P("graph", "mp", None),
        P(("graph", "mp")),
        P(("graph", "mp")),
        P(("graph", "mp")),
        P("graph"),
    )
    out_specs = (P("graph", "mp"), P("graph", "mp"))
    body = functools.partial(local, mesh.shape["graph"], mesh.shape["mp"])
    return jax.shard_map(body, mesh=mesh, in_specs=in_specs, out_specs=out_specs, check_vma=False)
```

```python
import functools

import jax
import jax.numpy as jnp
from jax import lax
from jax.experimental import pallas as pl
from jax.experimental.pallas import tpu as pltpu
from jax.sharding import PartitionSpec as P

ATOM_DEV = 32

inv_root_two = 0.7071067811865476
atom_scale = 0.2

MESH = pl.DeviceIdType.MESH
bf16 = jnp.bfloat16
f32 = jnp.float32


def scope(name):
    return jax.named_scope(name)


def silu(v):
    return v / (1.0 + jnp.exp(-v))


def flip(index, bit):
    return index + bit - 2 * bit * ((index // bit) % 2)


def one_hot(rows, ids):
    shape = (rows, ids.shape[1])
    return jnp.where(lax.broadcasted_iota(jnp.int32, shape, 0) == ids, 1.0, 0.0).astype(bf16)


def dot(a, b, ca=1, cb=0):
    return lax.dot_general(a, b, (((ca,), (cb,)), ((), ())), preferred_element_type=f32)


def halves(v):
    high = v.astype(bf16)
    return high, (v - high.astype(f32)).astype(bf16)


def chunks_of(half):
    return (0, half // 2), (half // 2, half // 2)


def gather_plan(mp):
    plan, held, bit = [], [0], mp // 2
    while bit >= 1:
        plan += [(bit, off) for off in held]
        held += [bit ^ off for off in held]
        bit //= 2
    return plan, held


def kernel(
    graph, mp, tile,
    state_hbm, down_hbm, basis_hbm, bw_hbm, up_hbm, dense_hbm, lists_hbm, in_hbm, out_hbm, live_hbm, atom_hbm,
    edge_out_ref, atom_out_ref,
    down_ref, basis_ref, bw_ref, lists_ref, in_ref, out_ref, live_ref, atom_ref, load_sem,
    states, ups, early_send, early_recv, up_send, up_recv,
    weight, joint, weight_sem, feed_send, feed_y, near_recv, core_send, core_recv,
    part_a, got_a, sum_a, more_a, full_a,
    part_b, got_b, sum_b, more_b, full_b,
    red_send, red_recv,
    to_a, from_a, to_b, from_b, xc_send, xc_recv,
    list_hot, basis_stack, bw_stack, angle, slots, in_hot, out_hot,
    acts, partial, hidden, act_send, act_recv,
    atoms_own, atoms_to, atoms_from, table,
):
    g = lax.axis_index("graph")
    m = lax.axis_index("mp")
    rows, width = hidden.shape
    trip = down_ref.shape[1]
    layers = weight.shape[0] - 1
    cap = lists_ref.shape[2]
    slot_total = graph * cap
    pieces, lane = to_a.shape[0], to_a.shape[2]
    kept = in_hot is not None
    triplets = in_ref.shape[1]
    atoms = graph * ATOM_DEV
    half = rows // 2
    feeds = layers - 1
    bits = [1 << i for i in range(mp.bit_length() - 1)]
    stages = len(bits)

    barrier = pltpu.get_barrier_semaphore()

    def greet(k, _):
        pl.semaphore_signal(barrier, inc=1, device_id={"graph": (g + k) % graph}, device_id_type=MESH)
        return 0

    lax.fori_loop(1, graph, greet, 0)
    for bit in bits:
        pl.semaphore_signal(barrier, inc=1, device_id={"mp": flip(m, bit)}, device_id_type=MESH)

    hbm = [state_hbm, down_hbm, lists_hbm, in_hbm, out_hbm, live_hbm, basis_hbm, bw_hbm, up_hbm, atom_hbm]
    here_refs = [
        states.at[m], down_ref, lists_ref, in_ref, out_ref, live_ref, basis_ref, bw_ref, ups.at[m], atom_ref]
    loads = [pltpu.make_async_copy(a, b, load_sem.at[i]) for i, (a, b) in enumerate(zip(hbm, here_refs))]
    for load in loads:
        load.start()
    state_in, down_in, lists_in, in_in, out_in, live_in, basis_in, bw_in, up_in, atom_in = loads

    def mp_copy(src, dst, which, j, stage, bit):
        return pltpu.make_async_remote_copy(
            src_ref=src, dst_ref=dst, send_sem=red_send.at[which, stage], recv_sem=red_recv.at[which, j, stage],
            device_id={"mp": flip(m, bit)}, device_id_type=MESH)

    mine = pl.ds(pl.multiple_of((m % 2) * half, half), half)
    other = pl.ds(pl.multiple_of(half - (m % 2) * half, half), half)

    plan, held = gather_plan(mp)

    def other_of(off):
        index = m
        for bit in bits:
            if off & bit:
                index = flip(index, bit)
        return index

    local = [i for i, (bit, off) in enumerate(plan) if off == 0]
    relayed = [i for i, (bit, off) in enumerate(plan) if off != 0]
    brings = {bit ^ off: i for i, (bit, off) in enumerate(plan)}
    relays_from = sorted({brings[plan[i][1]] for i in relayed})

    across_y = flip(m, mp // 2)

    def early(which, i):
        bit, off = plan[i]
        at = (states, ups)[which].at[other_of(off)]
        return pltpu.make_async_remote_copy(
            src_ref=at, dst_ref=at, send_sem=early_send.at[which], recv_sem=early_recv.at[which, 0 if i in relays_from else 1],
            device_id={"mp": flip(m, bit)}, device_id_type=MESH)

    trip_half = trip // 2
    up_rows = pl.ds(pl.multiple_of((g % 2) * trip_half, trip_half), trip_half)

    def up_copy(i):
        at = ups.at[(m, across_y)[i], up_rows]
        return pltpu.make_async_remote_copy(
            src_ref=at, dst_ref=at, send_sem=up_send, recv_sem=up_recv.at[i],
            device_id=({"mp": across_y}, {"graph": flip(g, 1)})[i], device_id_type=MESH)

    def up_beside():
        up_copy(0).wait_recv()
        up_copy(1).start()

    def up_home():
        up_copy(1).wait_recv()
        for i in relayed:
            early(1, i).start()

    def state_copy(i):
        cut = rows // 8
        at = states.at[m, (pl.ds(0, cut), pl.ds(cut, rows - cut))[i]]
        return pltpu.make_async_remote_copy(
            src_ref=at, dst_ref=at, send_sem=early_send.at[0], recv_sem=early_recv.at[0, 0],
            device_id={"mp": across_y}, device_id_type=MESH)

    def early_sent(which):
        at = (states, ups)[which].at[pl.ds(0, mp - 1 - which)]
        pltpu.make_async_remote_copy(
            src_ref=at, dst_ref=at, send_sem=early_send.at[which], recv_sem=early_recv.at[which, 0],
            device_id={"mp": flip(m, 1)}, device_id_type=MESH).wait_send()

    def early_relay(which):
        for i in relayed:
            first = brings[plan[i][1]]
            if [j for j in relayed if brings[plan[j][1]] == first][0] == i:
                early(which, first).wait_recv()
            early(which, i).start()

    def early_finish(which):
        at = (states, ups)[which].at[pl.ds(0, len(plan) - len(relays_from))]
        pltpu.make_async_remote_copy(
            src_ref=at, dst_ref=at, send_sem=early_send.at[which], recv_sem=early_recv.at[which, 1],
            device_id={"mp": flip(m, 1)}, device_id_type=MESH).wait_recv()

    eighth = weight.shape[1] // 8
    mine8 = g % 8

    def xor(a, k):
        for bit in (1, 2, 4):
            if k & bit:
                a = flip(a, bit)
        return a

    def part8(e):
        return pl.ds(pl.multiple_of(e * eighth, eighth), eighth)

    def feed_copy(src, f, e, sem, device):
        return pltpu.make_async_remote_copy(
            src_ref=src, dst_ref=joint.at[f, part8(e), far_cols], send_sem=feed_send.at[f], recv_sem=sem,
            device_id=device, device_id_type=MESH)

    def enter(f, far):
        e = xor(mine8, 4 * far)
        return feed_copy(joint.at[f, part8(e), own_cols], f, e, feed_y.at[f, far], {"mp": across_y})

    def hop(f):
        return feed_copy(joint.at[f, part8(mine8), far_cols], f, mine8, feed_y.at[f, 1], {"graph": xor(g, 4)})

    def near(f, far, k):
        e = xor(mine8, 4 * far)
        return feed_copy(joint.at[f, part8(e), far_cols], f, e, near_recv.at[f, far, 0 if k == 2 - far else 1], {"graph": xor(g, k)})

    def corner(f, far):
        came, goes = (2, 1) if far == 0 else (1, 2)
        e = xor(mine8, 4 * far + came)
        return feed_copy(joint.at[f, part8(e), far_cols], f, e, near_recv.at[f, far, 1], {"graph": xor(g, goes)})

    def feed_corner(f, far):
        near(f, far, 2 if far == 0 else 1).wait_recv()
        corner(f, far).start()

    def feed_ready(f):
        at = joint.at[f, pl.ds(0, 2 * eighth), far_cols]
        for far in range(2):
            pltpu.make_async_remote_copy(
                src_ref=at, dst_ref=at, send_sem=feed_send.at[f], recv_sem=near_recv.at[f, far, 1],
                device_id={"mp": across_y}, device_id_type=MESH).wait_recv()

    def feed_sent():
        for f in range(feeds):
            at = joint.at[f, :, far_cols]
            pltpu.make_async_remote_copy(
                src_ref=at, dst_ref=at, send_sem=feed_send.at[f], recv_sem=near_recv.at[f, 0, 0],
                device_id={"mp": across_y}, device_id_type=MESH).wait_send()

    class Sum:
        def __init__(self, which, part, got, summed, more, full):
            self.which, self.part, self.got = which, part, got
            self.summed, self.more, self.full = summed, more, full

        def first(self, j):
            return mp_copy(self.part.at[j, other], self.got.at[j], self.which, j, 0, 1)

        def step(self, j, b):
            return mp_copy(self.summed.at[j, b], self.more.at[j, b], self.which, j, 1 + b, bits[1 + b])

        def last(self, j):
            at = self.full.at[j, mine]
            return mp_copy(at, at, self.which, j, stages, 1)

        def into(self, j):
            self.first(j).start()

        def across(self, j):
            self.first(j).wait_recv()
            total = self.part[j, mine].astype(f32) + self.got[j].astype(f32)
            if stages > 1:
                self.summed[j, 0] = total.astype(bf16)
                self.step(j, 0).start()
            else:
                self.full[j, mine] = total.astype(bf16)

        def home(self, j):
            for b in range(stages - 1):
                self.step(j, b).wait_recv()
                total = self.summed[j, b].astype(f32) + self.more[j, b].astype(f32)
                if b + 2 < stages:
                    self.summed[j, b + 1] = total.astype(bf16)
                    self.step(j, b + 1).start()
                else:
                    self.full[j, mine] = total.astype(bf16)
            self.last(j).start()

        def done(self, j):
            self.last(j).wait_recv()

        def drain(self):
            for stage in range(stages + 1):
                mp_copy(self.got, self.got, self.which, 0, stage, 1).wait_send()

    sum0 = Sum(0, part_a, got_a, sum_a, more_a, full_a)
    sum1 = Sum(1, part_b, got_b, sum_b, more_b, full_b)

    def peer_of(k):
        if graph & (graph - 1):
            return (g + k) % graph
        return sum(bit * ((g // bit + k // bit) % 2) for bit in (1 << i for i in range(graph.bit_length() - 1)))

    peers = [peer_of(k) for k in range(graph - 1, 0, -1)] if graph <= 8 else None

    def arrived(whole, group, which):
        return pltpu.make_async_remote_copy(
            src_ref=whole, dst_ref=whole, send_sem=xc_send.at[group], recv_sem=xc_recv.at[which],
            device_id={"graph": (g + 1) % graph}, device_id_type=MESH)

    def exchange(group, which, src_at, dst_at, whole):
        def to(peer):
            pltpu.make_async_remote_copy(
                src_ref=src_at(peer), dst_ref=dst_at(g), send_sem=xc_send.at[group], recv_sem=xc_recv.at[which],
                device_id={"graph": peer}, device_id_type=MESH).start()

        def one(i, _):
            to(peer_of(graph - 1 - i))
            return 0

        def start():
            if peers is None:
                lax.fori_loop(0, graph - 1, one, 0)
            else:
                for peer in peers:
                    to(peer)

        return start, arrived(whole, group, which).wait_recv

    def block(ref, size):
        return lambda i: ref.at[pl.ds(pl.multiple_of(i * size, size), size)]

    def piece(ref, j, size):
        return lambda i: ref.at[j, pl.ds(pl.multiple_of(i * size, size), size)]

    def tiles(step):
        def one(i, _):
            step(pl.ds(pl.multiple_of(i * tile, tile), tile))
            return 0

        lax.fori_loop(0, triplets // tile, one, 0)

    def in_part(at):
        return one_hot(slot_total, in_ref[:, at])

    def out_part(at):
        return one_hot(slot_total, jnp.where(live_ref[:, at] > 0, out_ref[:, at], -1))

    state_in.wait()
    down_in.wait()
    with scope("s_proj"):
        projected = dot(states[m], down_ref[...]).astype(bf16)
        for j in range(pieces):
            part_a[j] = projected[:, j * lane:(j + 1) * lane]
    with scope("s_barrier"):
        pl.semaphore_wait(barrier, graph - 1 + len(bits))
    for j in range(pieces):
        sum0.into(j)
    state_copy(0).start()
    own_cols, far_cols = pl.ds(0, width), pl.ds(width, width)
    places = [(0, weight.at[0])] + [(2 * l + 1, weight.at[1 + l]) for l in range(layers)]
    places += [(2 * f + 2, joint.at[f, :, own_cols]) for f in range(feeds)]
    for k, at in places:
        pltpu.make_async_copy(dense_hbm.at[k], at, weight_sem.at[1 if k and k % 2 == 0 else 0]).start()

    lists_in.wait()
    with scope("s_hots"):
        for i in range(graph):
            list_hot[:, i * cap:(i + 1) * cap] = one_hot(rows, lists_ref[0, i:i + 1, :])
        in_in.wait()
        if kept:
            def keep_in(at):
                in_hot[:, at] = in_part(at)

            tiles(keep_in)
    with scope("s_across"):
        for j in range(pieces):
            sum0.across(j)
    up_in.wait()
    state_copy(1).start()
    out_in.wait()
    live_in.wait()
    if kept:
        def keep_out(at):
            out_hot[:, at] = out_part(at)

        with scope("s_outhot"):
            tiles(keep_out)

    basis_in.wait()
    bw_in.wait()
    depth = basis_ref.shape[0]
    pad = basis_stack.shape[0] // 3
    with scope("s_angles"):
        bw_high, bw_low = halves(bw_ref[...])
        bw_stack[...] = jnp.zeros_like(bw_stack)
        bw_stack[0:depth] = bw_high
        bw_stack[pad:pad + depth] = bw_high
        bw_stack[2 * pad:2 * pad + depth] = bw_low

        def angles(at):
            high, low = halves(basis_ref[:, at])
            basis_stack[:, at] = jnp.zeros((3 * pad, tile), bf16)
            basis_stack[0:depth, at] = high
            basis_stack[pad:pad + depth, at] = low
            basis_stack[2 * pad:2 * pad + depth, at] = high
            angle[:, at] = dot(bw_stack[...], basis_stack[:, at], 0, 0)

        tiles(angles)

    pltpu.make_async_copy(weight, weight, weight_sem.at[0]).wait()
    if feeds:
        pltpu.make_async_copy(joint.at[:, :, own_cols], joint.at[:, :, own_cols], weight_sem.at[1]).wait()
    if feeds:
        enter(0, 0).start()
    up_copy(0).start()
    if feeds:
        enter(0, 1).start()
    step_rows = min(slot_total, 512)
    own = pl.ds(pl.multiple_of(g * cap, cap), cap)
    span = pl.ds(0, slot_total - cap)
    most = xc_recv.shape[0] // 2
    going = [exchange(0, j, piece(to_a, j, cap), piece(from_a, j, cap), from_a.at[j, span]) for j in range(pieces)]
    back = [exchange(1, most + j, piece(to_b, j, cap), piece(from_b, j, cap), from_b.at[j, span])
            for j in range(pieces)]

    def pick_piece(j):
        def pick(i, _):
            at = pl.ds(pl.multiple_of(i * step_rows, step_rows), step_rows)
            to_a[j, at, :] = dot(list_hot[:, at], full_a[j], 0, 0).astype(bf16)
            return 0

        sum0.done(j)
        lax.fori_loop(0, slot_total // step_rows, pick, 0)
        going[j][0]()
        from_a[j, own] = to_a[j, own]

    with scope("s_home"):
        for j in range(pieces):
            sum0.home(j)
            pick_piece(j)
    for which in range(2):
        for i in local[1:]:
            early(which, i).start()
    sum0.drain()

    for j in range(pieces):
        with scope("s_gowait%d" % j):
            going[j][1]()
        slots[...] = jnp.zeros_like(slots)
        received = from_a[j].astype(f32).T.astype(bf16)

        def trips(at):
            source = in_hot[:, at] if kept else in_part(at)
            value = dot(received, source) * angle[j * lane:(j + 1) * lane, at]
            target = out_hot[:, at] if kept else out_part(at)
            slots[...] += dot(target, value.astype(bf16), 1, 1)

        with scope("s_trips%d" % j):
            tiles(trips)
        to_b[j] = slots[...].astype(bf16)
        back[j][0]()
        from_b[j, own] = to_b[j, own]
    with scope("s_early0"):
        early_relay(0)

    def add_up(j):
        for index in range(mp):
            rest = dot(full_b[j], ups[index, j * lane:(j + 1) * lane, :])
            partial[index] = (states[index].astype(f32) if j == 0 else partial[index]) + rest

    for j in range(pieces):
        with scope("s_backwait%d" % j):
            back[j][1]()
        part_b[j] = dot(list_hot[...], from_b[j]).astype(bf16)
        sum1.into(j)
        if j == 0:
            with scope("s_upbeside"):
                up_beside()
        if j + 1 < pieces:
            sum1.across(j)
    with scope("s_sum1"):
        sum1.across(pieces - 1)
        with scope("s_early1"):
            up_home()
        with scope("s_feedspread"):
            for f in range(1, feeds):
                enter(f, 0).start()
            if feeds:
                for far in range(2):
                    enter(0, far).wait_recv()
                    near(0, far, 2 - far).start()
                    near(0, far, 1 + far).start()
        for j in range(pieces - 2):
            sum1.home(j)
        early_finish(0)
        early_finish(1)
        if pieces > 1:
            sum1.home(pieces - 2)
        for j in range(pieces - 2):
            sum1.done(j)
            add_up(j)
        with scope("s_lasthome"):
            sum1.home(pieces - 1)

    starts, sizes = chunks_of(half)
    order = [(h, t) for t in range(len(sizes)) for h in (0, 1)]

    def chunk(c):
        side, t = c
        start = side * half + starts[t]
        return pl.ds(start if isinstance(side, int) else pl.multiple_of(start, half // 2), sizes[t])

    def chunk_id(c):
        return c[0] * len(sizes) + c[1]

    def act_copy(layer, parity, c, which):
        bit, off = plan[which]
        at = acts.at[layer - 1, other_of(off), chunk(c)]
        return pltpu.make_async_remote_copy(
            src_ref=at, dst_ref=at,
            send_sem=act_send.at[parity, chunk_id(c)], recv_sem=act_recv.at[parity, chunk_id(c), 0 if which in relays_from else 1],
            device_id={"mp": flip(m, bit)}, device_id_type=MESH)

    def send(layer, parity, c):
        for i in local:
            act_copy(layer, parity, c, i).start()

    def relay(layer, parity, c):
        for i in relayed:
            first = brings[plan[i][1]]
            if [j for j in relayed if brings[plan[j][1]] == first][0] == i:
                act_copy(layer, parity, c, first).wait_recv()
            act_copy(layer, parity, c, i).start()

    def finish(layer, parity, c):
        at = acts.at[layer - 1, pl.ds(0, len(plan) - len(relays_from)), chunk(c)]
        pltpu.make_async_remote_copy(
            src_ref=at, dst_ref=at, send_sem=act_send.at[parity, chunk_id(c)],
            recv_sem=act_recv.at[parity, chunk_id(c), 1],
            device_id={"mp": flip(m, 1)}, device_id_type=MESH).wait_recv()

    def sent(layer, parity, c):
        at = acts.at[layer - 1, pl.ds(0, mp - 1), chunk(c)]
        pltpu.make_async_remote_copy(
            src_ref=at, dst_ref=at, send_sem=act_send.at[parity, chunk_id(c)], recv_sem=act_recv.at[parity, chunk_id(c), 0],
            device_id={"mp": flip(m, 1)}, device_id_type=MESH).wait_send()

    def product(k, at, held_weight):
        rows_in = jnp.concatenate([acts[k - 1, index, at, :] for index in range(mp)], axis=1)
        return silu(dot(rows_in, held_weight[...]))

    def core_copy(layer, c, i):
        at = acts.at[layer - 1, (m, across_y)[i], chunk(c)]
        return pltpu.make_async_remote_copy(
            src_ref=at, dst_ref=at, send_sem=core_send.at[chunk_id(c)], recv_sem=core_recv.at[chunk_id(c)],
            device_id={"mp": flip(m, 1)}, device_id_type=MESH)

    def core_both(layer, c):
        at = acts.at[layer - 1, pl.ds(0, 2), chunk(c)]
        return pltpu.make_async_remote_copy(
            src_ref=at, dst_ref=at, send_sem=core_send.at[chunk_id(c)], recv_sem=core_recv.at[chunk_id(c)],
            device_id={"mp": flip(m, 1)}, device_id_type=MESH)

    def core_sent(layer, c):
        core_both(layer, c).wait_send()

    late = range(max(pieces - 2, 0), pieces)
    late_up = pl.ds(late[0] * lane, len(late) * lane)
    with scope("s_begin"):
        for spot in range(len(order)):
            c = (m % 2 if spot % 2 == 0 else 1 - m % 2), spot // 2
            at = chunk(c)
            if spot == 1:
                for j in late:
                    sum1.done(j)
            update_rows = jnp.concatenate([full_b[j, at] for j in late], axis=1)
            firsts = []
            for index in range(mp):
                before = partial[index, at] if pieces > 2 else states[index, at].astype(f32)
                first = before + dot(update_rows, ups[index, late_up, :])
                partial[index, at] = first
                firsts.append(first.astype(bf16))
            total = dot(jnp.concatenate(firsts, axis=1), weight[0])
            hidden[at, :] = partial[m, at]
            acts[0, m, at, :] = silu(total).astype(bf16)
            send(1, 0, c)
        if feeds:
            with scope("s_corner0"):
                for f in range(1, feeds):
                    enter(f, 0).wait_recv()
                    hop(f).start()
                for far in range(2):
                    feed_corner(0, far)
        sum1.drain()
        arrived(from_a.at[:, span], 0, 0).wait_send()
        arrived(from_b.at[:, span], 1, 0).wait_send()
        for which in range(2):
            early_sent(which)
        pltpu.make_async_remote_copy(
            src_ref=ups.at[m], dst_ref=ups.at[m], send_sem=up_send, recv_sem=up_recv.at[0],
            device_id={"mp": across_y}, device_id_type=MESH).wait_send()
    atom_in.wait()
    atom_rows = min(atoms, 256)
    parts, part_lane = table.shape[0], table.shape[2]

    def columns(p):
        return slice(p * part_lane, (p + 1) * part_lane)

    def collect(c):
        at = chunk(c)
        stacked = jnp.concatenate(halves(hidden[at, :]), axis=0)

        def one(i, _):
            here_rows = pl.ds(pl.multiple_of(i * atom_rows, atom_rows), atom_rows)
            ids = one_hot(atom_rows, atom_ref[:, at] - i * atom_rows)
            total = dot(jnp.concatenate([ids, ids], axis=1), stacked)
            for p in range(parts):
                sums = total[:, columns(p)]
                if c != order[0]:
                    sums += atoms_own[p, here_rows]
                atoms_own[p, here_rows] = sums
                if c == order[-1]:
                    atoms_to[p, here_rows] = sums.astype(bf16)
            return 0

        lax.fori_loop(0, atoms // atom_rows, one, 0)

    def update(l, c):
        at = chunk(c)
        value = (hidden[at, :] + product(2 * l + 1, at, weight.at[1 + l])) * inv_root_two
        hidden[at, :] = value
        return value.astype(bf16)

    with scope("s_layer0"):
        with scope("s_feedrest0"):
            for f in range(1, feeds):
                near(f, 0, 2).start()
                near(f, 0, 1).start()
        with scope("s_l0rel"):
            relay(1, 0, order[0])
        for spot, c in enumerate(order):
            with scope("s_l0fin%d" % spot):
                finish(1, 0, c)
            with scope("s_l0rel%d" % spot):
                if spot + 1 < len(order):
                    relay(1, 0, order[spot + 1])
            if spot + 1 == len(order) and layers > 1:
                with scope("s_l1rel"):
                    relay(2, 1, order[0])
            value = update(0, c)
            if layers > 1:
                acts[1, m, chunk(c), :] = value
                send(2, 1, c)
            with scope("s_l0feed%d" % spot):
                if spot + 1 == len(order):
                    for f in range(1, feeds):
                        hop(f).wait_recv()
                        near(f, 1, 1).start()
                        near(f, 1, 2).start()
                        feed_corner(f, 0)

    def layer_step(l, _):
        k, parity, f = 2 * l, l % 2, l - 1

        def second(c):
            core_both(k + 1, c).wait_recv()
            value = update(l, c)

            @pl.when(l + 1 < layers)
            def _():
                sent(k, 1 - parity, c)
                acts[k + 1, m, chunk(c), :] = value
                send(k + 2, 1 - parity, c)

            @pl.when(l + 1 == layers)
            def _():
                collect(c)

        with scope("s_feedwait"):
            feed_ready(f)
        def opening(c):
            at = chunk(c)

            @pl.when(l > 1)
            def _():
                core_sent(k - 1, c)

            both = product(k, at, joint.at[f]).astype(bf16)
            acts[k, m, at, :] = both[:, :width]
            acts[k, across_y, at, :] = both[:, width:]
            for i in range(2):
                core_copy(k + 1, c, i).start()

        for spot in range(0, len(order), 2):
            one, two = order[spot:spot + 2]
            with scope("s_finA%d" % spot):
                finish(k, parity, one)
            with scope("s_relA%d" % spot):
                relay(k, parity, two)
            opening(one)
            with scope("s_finB%d" % spot):
                finish(k, parity, two)
            opening(two)
            with scope("s_secA%d" % spot):
                second(one)
            with scope("s_relB%d" % spot):
                if spot + 2 < len(order):
                    relay(k, parity, order[spot + 2])

                    @pl.when(l == 1)
                    def _():
                        for later in range(1, feeds):
                            feed_corner(later, 1)
                else:
                    @pl.when(l + 1 < layers)
                    def _():
                        relay(k + 2, 1 - parity, order[0])
            with scope("s_secB%d" % spot):
                second(two)
        return 0

    with scope("s_layers"):
        lax.fori_loop(1, layers, layer_step, 0)

    here = pl.ds(pl.multiple_of(g * ATOM_DEV, ATOM_DEV), ATOM_DEV)
    atom_span = pl.ds(0, atoms - ATOM_DEV)
    gathers = [exchange(0, p, piece(atoms_to, p, ATOM_DEV), piece(atoms_from, p, ATOM_DEV),
                        atoms_from.at[p, atom_span]) for p in range(parts)]
    spreads = [exchange(1, most + p, lambda peer, p=p: piece(table, p, ATOM_DEV)(g),
                        piece(table, p, ATOM_DEV), table.at[p, atom_span]) for p in range(parts)]

    if layers == 1:
        for c in order:
            collect(c)
    for p in range(parts):
        gathers[p][0]()
    for p in range(parts):
        atoms_from[p, here] = jnp.zeros((ATOM_DEV, part_lane), bf16)
    for c in order:
        sent(1, (layers - 1) % 2, c)
        if layers > 1:
            sent(1, layers % 2, c)
            core_sent(1, c)
    feed_sent()
    for p in range(parts):
        with scope("s_atomwait%d" % p):
            gathers[p][1]()

        def add(i, total):
            return total + atoms_from[p, pl.ds(pl.multiple_of(i * ATOM_DEV, ATOM_DEV), ATOM_DEV)].astype(f32)

        total = lax.fori_loop(0, graph, add, atoms_own[p, here])
        mine_out = silu(atom_scale * total).astype(bf16)
        table[p, here] = mine_out
        spreads[p][0]()
        atom_out_ref[:, columns(p)] = mine_out
    arrived(atoms_from.at[:, atom_span], 0, 0).wait_send()
    for p in range(parts):
        with scope("s_spreadwait%d" % p):
            spreads[p][1]()

        def spread(i, total):
            at = pl.ds(pl.multiple_of(i * atom_rows, atom_rows), atom_rows)
            return total + dot(one_hot(atom_rows, atom_ref[...] - i * atom_rows), table[p, at], 0, 0)

        total = lax.fori_loop(0, atoms // atom_rows, spread, hidden[:, columns(p)])
        edge_out_ref[:, columns(p)] = total.astype(bf16)
    arrived(table.at[:, atom_span], 1, 0).wait_send()


def hand_on(edge_ref, atom_ref, edge_out_ref, atom_out_ref, sem):
    edge = pltpu.make_async_copy(edge_ref, edge_out_ref, sem.at[0])
    atom = pltpu.make_async_copy(atom_ref, atom_out_ref, sem.at[1])
    edge.start()
    atom.start()
    edge.wait()
    atom.wait()


def local(graph, mp, edge_state, down_weight, basis, basis_weight, up_weight, dense_weight,
          send_rows, trip_in, trip_out, trip_live, edge_atom):
    rows, width = edge_state.shape
    trip = down_weight.shape[1]
    slot_total = graph * send_rows.shape[2]
    triplets = trip_in.shape[0]
    maps = dense_weight.shape[0] * dense_weight.shape[1]
    tile = 2048 if slot_total <= 512 else 128
    atoms = graph * ATOM_DEV
    feeds = dense_weight.shape[0] - 1
    chunks = 2 * len(chunks_of(rows // 2)[1])
    stages = mp.bit_length()
    extra = max(stages - 2, 1)
    half = rows // 2
    vmem = pltpu.VMEM
    pieces = trip // 128 if trip % 128 == 0 else 1
    lane = trip // pieces
    pad = -(-basis.shape[0] // 16) * 16
    hot_bytes = 2 * 2 * slot_total * triplets
    hots = [vmem((slot_total, triplets), bf16)] * 2 if hot_bytes <= 2 ** 24 else [None, None]
    reduce_bufs = [
        vmem((pieces, rows, lane), bf16), vmem((pieces, half, lane), bf16), vmem((pieces, extra, half, lane), bf16),
        vmem((pieces, extra, half, lane), bf16), vmem((pieces, rows, lane), bf16),
    ]
    dma = pltpu.SemaphoreType.DMA
    spec = pl.BlockSpec(memory_space=pltpu.VMEM)
    operands = [
        edge_state, down_weight, basis, basis_weight, up_weight,
        dense_weight.reshape((maps,) + dense_weight.shape[2:]),
        send_rows, trip_in.reshape(1, triplets), trip_out.reshape(1, triplets),
        trip_live.reshape(1, triplets), edge_atom.reshape(1, rows),
    ]
    inputs = [vmem(a.shape, a.dtype) for i, a in enumerate(operands) if i not in (0, 4, 5)]
    parts = width // 128 if width % 128 == 0 else 1
    atom_buf = (parts, atoms, width // parts)
    body = functools.partial(kernel, graph, mp, tile)
    before = [
        *inputs, dma((len(inputs) + 2,)),
        vmem((mp, rows, width), bf16), vmem((mp, trip, width), bf16), dma((2,)), dma((2, 2)), dma(()), dma((2,)),
        vmem((dense_weight.shape[0] + 1,) + dense_weight.shape[2:], bf16),
        vmem((feeds, dense_weight.shape[2], 2 * width), bf16), dma((2,)), dma((feeds,)), dma((feeds, 2)), dma((feeds, 2, 2)),
        dma((chunks,)), dma((chunks,)),
        *reduce_bufs, *reduce_bufs,
        dma((2, stages)), dma((2, pieces, stages)),
        *[vmem((pieces, slot_total, lane), bf16)] * 4,
        dma((2,)), dma((2 * max(pieces, parts),)),
        vmem((rows, slot_total), bf16), vmem((3 * pad, triplets), bf16), vmem((3 * pad, trip), bf16),
        vmem((trip, triplets), f32), vmem((slot_total, lane), f32),
    ]
    if hots[0] is None:
        hots, kept_body, at = [], body, len(operands) + 2 + len(before)
        body = lambda *refs: kept_body(*refs[:at], None, None, *refs[at:])
    outs = pl.pallas_call(
        body,
        out_shape=(
            pltpu.VMEM((rows, width), bf16),
            pltpu.VMEM((ATOM_DEV, width), bf16),
        ),
        in_specs=[pl.BlockSpec(memory_space=pl.ANY)] * len(operands),
        out_specs=(spec, spec),
        scratch_shapes=[
            *before, *hots,
            vmem((maps - 1, mp, rows, width), bf16), vmem((mp, rows, width), f32), vmem((rows, width), f32),
            dma((2, chunks)), dma((2, chunks, 2)),
            vmem(atom_buf, f32), vmem(atom_buf, bf16), vmem(atom_buf, bf16), vmem(atom_buf, bf16),
        ],
        compiler_params=pltpu.CompilerParams(
            collective_id=0, has_side_effects=True, vmem_limit_bytes=64000 * 1024
        ),
        name="edge_block",
    )(*operands)
    outs = [pltpu.with_memory_space_constraint(o, pltpu.VMEM) for o in outs]
    return pl.pallas_call(
        hand_on,
        out_shape=tuple(jax.ShapeDtypeStruct(o.shape, o.dtype) for o in outs),
        in_specs=[spec] * 2,
        out_specs=[pl.BlockSpec(memory_space=pl.ANY)] * 2,
        scratch_shapes=[dma((2,))],
        name="hand_on",
    )(*outs)


def solution(mesh):
    in_specs = (
        P("graph", "mp"),
        P("mp", None),
        P(None, ("graph", "mp")),
        P(),
        P(None, "mp"),
        P(None, None, None, "mp"),
        P("graph", "mp", None),
        P(("graph", "mp")),
        P(("graph", "mp")),
        P(("graph", "mp")),
        P("graph"),
    )
    out_specs = (P("graph", "mp"), P("graph", "mp"))
    body = functools.partial(local, mesh.shape["graph"], mesh.shape["mp"])
    return jax.shard_map(body, mesh=mesh, in_specs=in_specs, out_specs=out_specs, check_vma=False)
```

```python
import functools

import jax
import jax.numpy as jnp
from jax import lax
from jax.experimental import pallas as pl
from jax.experimental.pallas import tpu as pltpu
from jax.sharding import PartitionSpec as P

ATOM_DEV = 32

inv_root_two = 0.7071067811865476
atom_scale = 0.2

MESH = pl.DeviceIdType.MESH
bf16 = jnp.bfloat16
f32 = jnp.float32


def scope(name):
    return jax.named_scope(name)


def silu(v):
    return v / (1.0 + jnp.exp(-v))


def flip(index, bit):
    return index + bit - 2 * bit * ((index // bit) % 2)


def one_hot(rows, ids):
    shape = (rows, ids.shape[1])
    return jnp.where(lax.broadcasted_iota(jnp.int32, shape, 0) == ids, 1.0, 0.0).astype(bf16)


def dot(a, b, ca=1, cb=0):
    return lax.dot_general(a, b, (((ca,), (cb,)), ((), ())), preferred_element_type=f32)


def halves(v):
    high = v.astype(bf16)
    return high, (v - high.astype(f32)).astype(bf16)


def chunks_of(half):
    return (0, half // 2), (half // 2, half // 2)


def gather_plan(mp):
    plan, held, bit = [], [0], mp // 2
    while bit >= 1:
        plan += [(bit, off) for off in held]
        held += [bit ^ off for off in held]
        bit //= 2
    return plan, held


def kernel(
    graph, mp, tile,
    state_hbm, down_hbm, basis_hbm, bw_hbm, up_hbm, dense_hbm, lists_hbm, in_hbm, out_hbm, live_hbm, atom_hbm,
    edge_out_ref, atom_out_ref,
    down_ref, basis_ref, bw_ref, lists_ref, in_ref, out_ref, live_ref, atom_ref, load_sem,
    states, ups, early_send, early_recv, up_send, up_recv,
    weight, joint, weight_sem, feed_send, feed_y, near_recv, core_send, core_recv,
    part_a, got_a, sum_a, more_a, full_a,
    part_b, got_b, sum_b, more_b, full_b,
    red_send, red_recv,
    to_a, from_a, to_b, from_b, xc_send, xc_recv,
    list_hot, basis_stack, bw_stack, angle, slots, in_hot, out_hot,
    acts, partial, hidden, act_send, act_recv,
    atoms_own, atoms_to, atoms_from, table,
):
    g = lax.axis_index("graph")
    m = lax.axis_index("mp")
    rows, width = hidden.shape
    trip = down_ref.shape[1]
    layers = weight.shape[0] - 1
    cap = lists_ref.shape[2]
    slot_total = graph * cap
    pieces, lane = to_a.shape[0], to_a.shape[2]
    kept = in_hot is not None
    triplets = in_ref.shape[1]
    atoms = graph * ATOM_DEV
    half = rows // 2
    feeds = layers - 1
    bits = [1 << i for i in range(mp.bit_length() - 1)]
    stages = len(bits)

    barrier = pltpu.get_barrier_semaphore()

    def greet(k, _):
        pl.semaphore_signal(barrier, inc=1, device_id={"graph": (g + k) % graph}, device_id_type=MESH)
        return 0

    lax.fori_loop(1, graph, greet, 0)
    for bit in bits:
        pl.semaphore_signal(barrier, inc=1, device_id={"mp": flip(m, bit)}, device_id_type=MESH)

    hbm = [state_hbm, down_hbm, lists_hbm, in_hbm, out_hbm, live_hbm, basis_hbm, bw_hbm, up_hbm, atom_hbm]
    here_refs = [
        states.at[m], down_ref, lists_ref, in_ref, out_ref, live_ref, basis_ref, bw_ref, ups.at[m], atom_ref]
    loads = [pltpu.make_async_copy(a, b, load_sem.at[i]) for i, (a, b) in enumerate(zip(hbm, here_refs))]
    for load in loads:
        load.start()
    state_in, down_in, lists_in, in_in, out_in, live_in, basis_in, bw_in, up_in, atom_in = loads

    def mp_copy(src, dst, which, j, stage, bit):
        return pltpu.make_async_remote_copy(
            src_ref=src, dst_ref=dst, send_sem=red_send.at[which, stage], recv_sem=red_recv.at[which, j, stage],
            device_id={"mp": flip(m, bit)}, device_id_type=MESH)

    mine = pl.ds(pl.multiple_of((m % 2) * half, half), half)
    other = pl.ds(pl.multiple_of(half - (m % 2) * half, half), half)

    plan, held = gather_plan(mp)

    def other_of(off):
        index = m
        for bit in bits:
            if off & bit:
                index = flip(index, bit)
        return index

    local = [i for i, (bit, off) in enumerate(plan) if off == 0]
    relayed = [i for i, (bit, off) in enumerate(plan) if off != 0]
    brings = {bit ^ off: i for i, (bit, off) in enumerate(plan)}
    relays_from = sorted({brings[plan[i][1]] for i in relayed})

    across_y = flip(m, mp // 2)

    def early(which, i):
        bit, off = plan[i]
        at = (states, ups)[which].at[other_of(off)]
        return pltpu.make_async_remote_copy(
            src_ref=at, dst_ref=at, send_sem=early_send.at[which], recv_sem=early_recv.at[which, 0 if i in relays_from else 1],
            device_id={"mp": flip(m, bit)}, device_id_type=MESH)

    trip_half = trip // 2
    up_rows = pl.ds(pl.multiple_of((g % 2) * trip_half, trip_half), trip_half)

    def up_copy(i):
        at = ups.at[(m, across_y)[i], up_rows]
        return pltpu.make_async_remote_copy(
            src_ref=at, dst_ref=at, send_sem=up_send, recv_sem=up_recv.at[i],
            device_id=({"mp": across_y}, {"graph": flip(g, 1)})[i], device_id_type=MESH)

    def up_beside():
        up_copy(0).wait_recv()
        up_copy(1).start()

    def up_home():
        up_copy(1).wait_recv()
        for i in relayed:
            early(1, i).start()

    def state_copy(i):
        cut = rows // 8
        at = states.at[m, (pl.ds(0, cut), pl.ds(cut, rows - cut))[i]]
        return pltpu.make_async_remote_copy(
            src_ref=at, dst_ref=at, send_sem=early_send.at[0], recv_sem=early_recv.at[0, 0],
            device_id={"mp": across_y}, device_id_type=MESH)

    def early_sent(which):
        at = (states, ups)[which].at[pl.ds(0, mp - 1 - which)]
        pltpu.make_async_remote_copy(
            src_ref=at, dst_ref=at, send_sem=early_send.at[which], recv_sem=early_recv.at[which, 0],
            device_id={"mp": flip(m, 1)}, device_id_type=MESH).wait_send()

    def early_relay(which):
        for i in relayed:
            first = brings[plan[i][1]]
            if [j for j in relayed if brings[plan[j][1]] == first][0] == i:
                early(which, first).wait_recv()
            early(which, i).start()

    def early_finish(which):
        at = (states, ups)[which].at[pl.ds(0, len(plan) - len(relays_from))]
        pltpu.make_async_remote_copy(
            src_ref=at, dst_ref=at, send_sem=early_send.at[which], recv_sem=early_recv.at[which, 1],
            device_id={"mp": flip(m, 1)}, device_id_type=MESH).wait_recv()

    eighth = weight.shape[1] // 8
    mine8 = g % 8

    def xor(a, k):
        for bit in (1, 2, 4):
            if k & bit:
                a = flip(a, bit)
        return a

    def part8(e):
        return pl.ds(pl.multiple_of(e * eighth, eighth), eighth)

    def feed_copy(src, f, e, sem, device):
        return pltpu.make_async_remote_copy(
            src_ref=src, dst_ref=joint.at[f, part8(e), far_cols], send_sem=feed_send.at[f], recv_sem=sem,
            device_id=device, device_id_type=MESH)

    def enter(f, far):
        e = xor(mine8, 4 * far)
        return feed_copy(joint.at[f, part8(e), own_cols], f, e, feed_y.at[f, far], {"mp": across_y})

    def hop(f):
        return feed_copy(joint.at[f, part8(mine8), far_cols], f, mine8, feed_y.at[f, 1], {"graph": xor(g, 4)})

    def near(f, far, k):
        e = xor(mine8, 4 * far)
        return feed_copy(joint.at[f, part8(e), far_cols], f, e, near_recv.at[f, far, 0 if k == 2 - far else 1], {"graph": xor(g, k)})

    def corner(f, far):
        came, goes = (2, 1) if far == 0 else (1, 2)
        e = xor(mine8, 4 * far + came)
        return feed_copy(joint.at[f, part8(e), far_cols], f, e, near_recv.at[f, far, 1], {"graph": xor(g, goes)})

    def feed_corner(f, far):
        near(f, far, 2 if far == 0 else 1).wait_recv()
        corner(f, far).start()

    def feed_ready(f):
        at = joint.at[f, pl.ds(0, 2 * eighth), far_cols]
        for far in range(2):
            pltpu.make_async_remote_copy(
                src_ref=at, dst_ref=at, send_sem=feed_send.at[f], recv_sem=near_recv.at[f, far, 1],
                device_id={"mp": across_y}, device_id_type=MESH).wait_recv()

    def feed_sent():
        for f in range(feeds):
            at = joint.at[f, :, far_cols]
            pltpu.make_async_remote_copy(
                src_ref=at, dst_ref=at, send_sem=feed_send.at[f], recv_sem=near_recv.at[f, 0, 0],
                device_id={"mp": across_y}, device_id_type=MESH).wait_send()

    class Sum:
        def __init__(self, which, part, got, summed, more, full):
            self.which, self.part, self.got = which, part, got
            self.summed, self.more, self.full = summed, more, full

        def first(self, j):
            return mp_copy(self.part.at[j, other], self.got.at[j], self.which, j, 0, 1)

        def step(self, j, b):
            return mp_copy(self.summed.at[j, b], self.more.at[j, b], self.which, j, 1 + b, bits[1 + b])

        def last(self, j):
            at = self.full.at[j, mine]
            return mp_copy(at, at, self.which, j, stages, 1)

        def into(self, j):
            self.first(j).start()

        def across(self, j):
            self.first(j).wait_recv()
            total = self.part[j, mine].astype(f32) + self.got[j].astype(f32)
            if stages > 1:
                self.summed[j, 0] = total.astype(bf16)
                self.step(j, 0).start()
            else:
                self.full[j, mine] = total.astype(bf16)

        def home(self, j):
            for b in range(stages - 1):
                self.step(j, b).wait_recv()
                total = self.summed[j, b].astype(f32) + self.more[j, b].astype(f32)
                if b + 2 < stages:
                    self.summed[j, b + 1] = total.astype(bf16)
                    self.step(j, b + 1).start()
                else:
                    self.full[j, mine] = total.astype(bf16)
            self.last(j).start()

        def done(self, j):
            self.last(j).wait_recv()

        def drain(self):
            for stage in range(stages + 1):
                mp_copy(self.got, self.got, self.which, 0, stage, 1).wait_send()

    sum0 = Sum(0, part_a, got_a, sum_a, more_a, full_a)
    sum1 = Sum(1, part_b, got_b, sum_b, more_b, full_b)

    def peer_of(k):
        if graph & (graph - 1):
            return (g + k) % graph
        return sum(bit * ((g // bit + k // bit) % 2) for bit in (1 << i for i in range(graph.bit_length() - 1)))

    peers = [peer_of(k) for k in range(graph - 1, 0, -1)] if graph <= 8 else None

    def arrived(whole, group, which):
        return pltpu.make_async_remote_copy(
            src_ref=whole, dst_ref=whole, send_sem=xc_send.at[group], recv_sem=xc_recv.at[which],
            device_id={"graph": (g + 1) % graph}, device_id_type=MESH)

    def exchange(group, which, src_at, dst_at, whole):
        def to(peer):
            pltpu.make_async_remote_copy(
                src_ref=src_at(peer), dst_ref=dst_at(g), send_sem=xc_send.at[group], recv_sem=xc_recv.at[which],
                device_id={"graph": peer}, device_id_type=MESH).start()

        def one(i, _):
            to(peer_of(graph - 1 - i))
            return 0

        def start():
            if peers is None:
                lax.fori_loop(0, graph - 1, one, 0)
            else:
                for peer in peers:
                    to(peer)

        return start, arrived(whole, group, which).wait_recv

    def block(ref, size):
        return lambda i: ref.at[pl.ds(pl.multiple_of(i * size, size), size)]

    def piece(ref, j, size):
        return lambda i: ref.at[j, pl.ds(pl.multiple_of(i * size, size), size)]

    def tiles(step):
        def one(i, _):
            step(pl.ds(pl.multiple_of(i * tile, tile), tile))
            return 0

        lax.fori_loop(0, triplets // tile, one, 0)

    def in_part(at):
        return one_hot(slot_total, in_ref[:, at])

    def out_part(at):
        return one_hot(slot_total, jnp.where(live_ref[:, at] > 0, out_ref[:, at], -1))

    state_in.wait()
    down_in.wait()
    with scope("s_proj"):
        projected = dot(states[m], down_ref[...]).astype(bf16)
        for j in range(pieces):
            part_a[j] = projected[:, j * lane:(j + 1) * lane]
    with scope("s_barrier"):
        pl.semaphore_wait(barrier, graph - 1 + len(bits))
    for j in range(pieces):
        sum0.into(j)
    state_copy(0).start()
    own_cols, far_cols = pl.ds(0, width), pl.ds(width, width)
    places = [(0, weight.at[0])] + [(2 * l + 1, weight.at[1 + l]) for l in range(layers)]
    places += [(2 * f + 2, joint.at[f, :, own_cols]) for f in range(feeds)]
    for k, at in places:
        pltpu.make_async_copy(dense_hbm.at[k], at, weight_sem.at[1 if k and k % 2 == 0 else 0]).start()

    lists_in.wait()
    with scope("s_hots"):
        for i in range(graph):
            list_hot[:, i * cap:(i + 1) * cap] = one_hot(rows, lists_ref[0, i:i + 1, :])
        in_in.wait()
        if kept:
            def keep_in(at):
                in_hot[:, at] = in_part(at)

            tiles(keep_in)
    with scope("s_across"):
        for j in range(pieces):
            sum0.across(j)
    up_in.wait()
    state_copy(1).start()
    out_in.wait()
    live_in.wait()
    if kept:
        def keep_out(at):
            out_hot[:, at] = out_part(at)

        with scope("s_outhot"):
            tiles(keep_out)

    basis_in.wait()
    bw_in.wait()
    depth = basis_ref.shape[0]
    pad = basis_stack.shape[0] // 3
    with scope("s_angles"):
        bw_high, bw_low = halves(bw_ref[...])
        bw_stack[...] = jnp.zeros_like(bw_stack)
        bw_stack[0:depth] = bw_high
        bw_stack[pad:pad + depth] = bw_high
        bw_stack[2 * pad:2 * pad + depth] = bw_low

        def angles(at):
            high, low = halves(basis_ref[:, at])
            basis_stack[:, at] = jnp.zeros((3 * pad, tile), bf16)
            basis_stack[0:depth, at] = high
            basis_stack[pad:pad + depth, at] = low
            basis_stack[2 * pad:2 * pad + depth, at] = high
            angle[:, at] = dot(bw_stack[...], basis_stack[:, at], 0, 0)

        tiles(angles)

    pltpu.make_async_copy(weight, weight, weight_sem.at[0]).wait()
    if feeds:
        pltpu.make_async_copy(joint.at[:, :, own_cols], joint.at[:, :, own_cols], weight_sem.at[1]).wait()
    if feeds:
        enter(0, 0).start()
    up_copy(0).start()
    if feeds:
        enter(0, 1).start()
    step_rows = min(slot_total, 512)
    own = pl.ds(pl.multiple_of(g * cap, cap), cap)
    span = pl.ds(0, slot_total - cap)
    most = xc_recv.shape[0] // 2
    going = [exchange(0, j, piece(to_a, j, cap), piece(from_a, j, cap), from_a.at[j, span]) for j in range(pieces)]
    back = [exchange(1, most + j, piece(to_b, j, cap), piece(from_b, j, cap), from_b.at[j, span])
            for j in range(pieces)]

    def pick_piece(j):
        def pick(i, _):
            at = pl.ds(pl.multiple_of(i * step_rows, step_rows), step_rows)
            to_a[j, at, :] = dot(list_hot[:, at], full_a[j], 0, 0).astype(bf16)
            return 0

        sum0.done(j)
        lax.fori_loop(0, slot_total // step_rows, pick, 0)
        going[j][0]()
        from_a[j, own] = to_a[j, own]

    with scope("s_home"):
        for j in range(pieces):
            sum0.home(j)
            pick_piece(j)
    for which in range(2):
        for i in local[1:]:
            early(which, i).start()
    sum0.drain()

    for j in range(pieces):
        with scope("s_gowait%d" % j):
            going[j][1]()
        slots[...] = jnp.zeros_like(slots)
        received = from_a[j].astype(f32).T.astype(bf16)

        def trips(at):
            source = in_hot[:, at] if kept else in_part(at)
            value = dot(received, source) * angle[j * lane:(j + 1) * lane, at]
            target = out_hot[:, at] if kept else out_part(at)
            slots[...] += dot(target, value.astype(bf16), 1, 1)

        with scope("s_trips%d" % j):
            tiles(trips)
        to_b[j] = slots[...].astype(bf16)
        back[j][0]()
        from_b[j, own] = to_b[j, own]
    with scope("s_early0"):
        early_relay(0)

    def add_up(j):
        for index in range(mp):
            rest = dot(full_b[j], ups[index, j * lane:(j + 1) * lane, :])
            partial[index] = (states[index].astype(f32) if j == 0 else partial[index]) + rest

    for j in range(pieces):
        with scope("s_backwait%d" % j):
            back[j][1]()
        part_b[j] = dot(list_hot[...], from_b[j]).astype(bf16)
        sum1.into(j)
        if j == 0:
            with scope("s_upbeside"):
                up_beside()
        if j + 1 < pieces:
            sum1.across(j)
    with scope("s_sum1"):
        sum1.across(pieces - 1)
        with scope("s_early1"):
            up_home()
        with scope("s_feedspread"):
            for f in range(1, feeds):
                enter(f, 0).start()
            if feeds:
                for far in range(2):
                    enter(0, far).wait_recv()
                    near(0, far, 2 - far).start()
                    near(0, far, 1 + far).start()
        for j in range(pieces - 2):
            sum1.home(j)
        early_finish(0)
        early_finish(1)
        if pieces > 1:
            sum1.home(pieces - 2)
        for j in range(pieces - 2):
            sum1.done(j)
            add_up(j)
        with scope("s_lasthome"):
            sum1.home(pieces - 1)

    starts, sizes = chunks_of(half)
    order = [(h, t) for t in range(len(sizes)) for h in (0, 1)]

    def chunk(c):
        side, t = c
        start = side * half + starts[t]
        return pl.ds(start if isinstance(side, int) else pl.multiple_of(start, half // 2), sizes[t])

    def chunk_id(c):
        return c[0] * len(sizes) + c[1]

    def act_copy(layer, parity, c, which):
        bit, off = plan[which]
        at = acts.at[layer - 1, other_of(off), chunk(c)]
        return pltpu.make_async_remote_copy(
            src_ref=at, dst_ref=at,
            send_sem=act_send.at[parity, chunk_id(c)], recv_sem=act_recv.at[parity, chunk_id(c), 0 if which in relays_from else 1],
            device_id={"mp": flip(m, bit)}, device_id_type=MESH)

    def send(layer, parity, c):
        for i in local:
            act_copy(layer, parity, c, i).start()

    def relay(layer, parity, c):
        for i in relayed:
            first = brings[plan[i][1]]
            if [j for j in relayed if brings[plan[j][1]] == first][0] == i:
                act_copy(layer, parity, c, first).wait_recv()
            act_copy(layer, parity, c, i).start()

    def finish(layer, parity, c):
        at = acts.at[layer - 1, pl.ds(0, len(plan) - len(relays_from)), chunk(c)]
        pltpu.make_async_remote_copy(
            src_ref=at, dst_ref=at, send_sem=act_send.at[parity, chunk_id(c)],
            recv_sem=act_recv.at[parity, chunk_id(c), 1],
            device_id={"mp": flip(m, 1)}, device_id_type=MESH).wait_recv()

    def sent(layer, parity, c):
        at = acts.at[layer - 1, pl.ds(0, mp - 1), chunk(c)]
        pltpu.make_async_remote_copy(
            src_ref=at, dst_ref=at, send_sem=act_send.at[parity, chunk_id(c)], recv_sem=act_recv.at[parity, chunk_id(c), 0],
            device_id={"mp": flip(m, 1)}, device_id_type=MESH).wait_send()

    def product(k, at, held_weight):
        rows_in = jnp.concatenate([acts[k - 1, index, at, :] for index in range(mp)], axis=1)
        return silu(dot(rows_in, held_weight[...]))

    def core_copy(layer, c, i):
        at = acts.at[layer - 1, (m, across_y)[i], chunk(c)]
        return pltpu.make_async_remote_copy(
            src_ref=at, dst_ref=at, send_sem=core_send.at[chunk_id(c)], recv_sem=core_recv.at[chunk_id(c)],
            device_id={"mp": flip(m, 1)}, device_id_type=MESH)

    def core_both(layer, c):
        at = acts.at[layer - 1, pl.ds(0, 2), chunk(c)]
        return pltpu.make_async_remote_copy(
            src_ref=at, dst_ref=at, send_sem=core_send.at[chunk_id(c)], recv_sem=core_recv.at[chunk_id(c)],
            device_id={"mp": flip(m, 1)}, device_id_type=MESH)

    def core_sent(layer, c):
        core_both(layer, c).wait_send()

    late = range(max(pieces - 2, 0), pieces)
    late_up = pl.ds(late[0] * lane, len(late) * lane)
    with scope("s_begin"):
        for spot in range(len(order)):
            c = (m % 2 if spot % 2 == 0 else 1 - m % 2), spot // 2
            at = chunk(c)
            if spot == 1:
                for j in late:
                    sum1.done(j)
            update_rows = jnp.concatenate([full_b[j, at] for j in late], axis=1)
            firsts = []
            for index in range(mp):
                before = partial[index, at] if pieces > 2 else states[index, at].astype(f32)
                first = before + dot(update_rows, ups[index, late_up, :])
                partial[index, at] = first
                firsts.append(first.astype(bf16))
            total = dot(jnp.concatenate(firsts, axis=1), weight[0])
            hidden[at, :] = partial[m, at]
            acts[0, m, at, :] = silu(total).astype(bf16)
            send(1, 0, c)
        if feeds:
            with scope("s_corner0"):
                for f in range(1, feeds):
                    enter(f, 0).wait_recv()
                    hop(f).start()
        sum1.drain()
        arrived(from_a.at[:, span], 0, 0).wait_send()
        arrived(from_b.at[:, span], 1, 0).wait_send()
        for which in range(2):
            early_sent(which)
        pltpu.make_async_remote_copy(
            src_ref=ups.at[m], dst_ref=ups.at[m], send_sem=up_send, recv_sem=up_recv.at[0],
            device_id={"mp": across_y}, device_id_type=MESH).wait_send()
    atom_in.wait()
    atom_rows = min(atoms, 256)
    parts, part_lane = table.shape[0], table.shape[2]

    def columns(p):
        return slice(p * part_lane, (p + 1) * part_lane)

    def collect(c):
        at = chunk(c)
        stacked = jnp.concatenate(halves(hidden[at, :]), axis=0)

        def one(i, _):
            here_rows = pl.ds(pl.multiple_of(i * atom_rows, atom_rows), atom_rows)
            ids = one_hot(atom_rows, atom_ref[:, at] - i * atom_rows)
            total = dot(jnp.concatenate([ids, ids], axis=1), stacked)
            for p in range(parts):
                sums = total[:, columns(p)]
                if c != order[0]:
                    sums += atoms_own[p, here_rows]
                atoms_own[p, here_rows] = sums
                if c == order[-1]:
                    atoms_to[p, here_rows] = sums.astype(bf16)
            return 0

        lax.fori_loop(0, atoms // atom_rows, one, 0)

    def update(l, c):
        at = chunk(c)
        value = (hidden[at, :] + product(2 * l + 1, at, weight.at[1 + l])) * inv_root_two
        hidden[at, :] = value
        return value.astype(bf16)

    with scope("s_layer0"):
        with scope("s_l0rel"):
            relay(1, 0, order[0])
        if feeds:
            for far in range(2):
                feed_corner(0, far)
        with scope("s_feedrest0"):
            for f in range(1, feeds):
                near(f, 0, 2).start()
                near(f, 0, 1).start()
        for spot, c in enumerate(order):
            with scope("s_l0fin%d" % spot):
                finish(1, 0, c)
            with scope("s_l0rel%d" % spot):
                if spot + 1 < len(order):
                    relay(1, 0, order[spot + 1])
            if spot + 1 == len(order) and layers > 1:
                with scope("s_l1rel"):
                    relay(2, 1, order[0])
            value = update(0, c)
            if layers > 1:
                acts[1, m, chunk(c), :] = value
                send(2, 1, c)
            with scope("s_l0feed%d" % spot):
                if spot + 1 == len(order):
                    for f in range(1, feeds):
                        hop(f).wait_recv()
                        near(f, 1, 1).start()
                        near(f, 1, 2).start()
                        feed_corner(f, 0)

    def layer_step(l, _):
        k, parity, f = 2 * l, l % 2, l - 1

        def second(c):
            core_both(k + 1, c).wait_recv()
            value = update(l, c)

            @pl.when(l + 1 < layers)
            def _():
                sent(k, 1 - parity, c)
                acts[k + 1, m, chunk(c), :] = value
                send(k + 2, 1 - parity, c)

            @pl.when(l + 1 == layers)
            def _():
                collect(c)

        with scope("s_feedwait"):
            feed_ready(f)
        def opening(c):
            at = chunk(c)

            @pl.when(l > 1)
            def _():
                core_sent(k - 1, c)

            both = product(k, at, joint.at[f]).astype(bf16)
            acts[k, m, at, :] = both[:, :width]
            acts[k, across_y, at, :] = both[:, width:]
            for i in range(2):
                core_copy(k + 1, c, i).start()

        for spot in range(0, len(order), 2):
            one, two = order[spot:spot + 2]
            with scope("s_finA%d" % spot):
                finish(k, parity, one)
            with scope("s_relA%d" % spot):
                relay(k, parity, two)
            opening(one)
            with scope("s_finB%d" % spot):
                finish(k, parity, two)
            opening(two)
            with scope("s_secA%d" % spot):
                second(one)
            with scope("s_relB%d" % spot):
                if spot + 2 < len(order):
                    relay(k, parity, order[spot + 2])

                    @pl.when(l == 1)
                    def _():
                        for later in range(1, feeds):
                            feed_corner(later, 1)
                else:
                    @pl.when(l + 1 < layers)
                    def _():
                        relay(k + 2, 1 - parity, order[0])
            with scope("s_secB%d" % spot):
                second(two)
        return 0

    with scope("s_layers"):
        lax.fori_loop(1, layers, layer_step, 0)

    here = pl.ds(pl.multiple_of(g * ATOM_DEV, ATOM_DEV), ATOM_DEV)
    atom_span = pl.ds(0, atoms - ATOM_DEV)
    gathers = [exchange(0, p, piece(atoms_to, p, ATOM_DEV), piece(atoms_from, p, ATOM_DEV),
                        atoms_from.at[p, atom_span]) for p in range(parts)]
    spreads = [exchange(1, most + p, lambda peer, p=p: piece(table, p, ATOM_DEV)(g),
                        piece(table, p, ATOM_DEV), table.at[p, atom_span]) for p in range(parts)]

    if layers == 1:
        for c in order:
            collect(c)
    for p in range(parts):
        gathers[p][0]()
    for p in range(parts):
        atoms_from[p, here] = jnp.zeros((ATOM_DEV, part_lane), bf16)
    for c in order:
        sent(1, (layers - 1) % 2, c)
        if layers > 1:
            sent(1, layers % 2, c)
            core_sent(1, c)
    feed_sent()
    for p in range(parts):
        with scope("s_atomwait%d" % p):
            gathers[p][1]()

        def add(i, total):
            return total + atoms_from[p, pl.ds(pl.multiple_of(i * ATOM_DEV, ATOM_DEV), ATOM_DEV)].astype(f32)

        total = lax.fori_loop(0, graph, add, atoms_own[p, here])
        mine_out = silu(atom_scale * total).astype(bf16)
        table[p, here] = mine_out
        spreads[p][0]()
        atom_out_ref[:, columns(p)] = mine_out
    arrived(atoms_from.at[:, atom_span], 0, 0).wait_send()
    for p in range(parts):
        with scope("s_spreadwait%d" % p):
            spreads[p][1]()

        def spread(i, total):
            at = pl.ds(pl.multiple_of(i * atom_rows, atom_rows), atom_rows)
            return total + dot(one_hot(atom_rows, atom_ref[...] - i * atom_rows), table[p, at], 0, 0)

        total = lax.fori_loop(0, atoms // atom_rows, spread, hidden[:, columns(p)])
        edge_out_ref[:, columns(p)] = total.astype(bf16)
    arrived(table.at[:, atom_span], 1, 0).wait_send()


def hand_on(edge_ref, atom_ref, edge_out_ref, atom_out_ref, sem):
    edge = pltpu.make_async_copy(edge_ref, edge_out_ref, sem.at[0])
    atom = pltpu.make_async_copy(atom_ref, atom_out_ref, sem.at[1])
    edge.start()
    atom.start()
    edge.wait()
    atom.wait()


def local(graph, mp, edge_state, down_weight, basis, basis_weight, up_weight, dense_weight,
          send_rows, trip_in, trip_out, trip_live, edge_atom):
    rows, width = edge_state.shape
    trip = down_weight.shape[1]
    slot_total = graph * send_rows.shape[2]
    triplets = trip_in.shape[0]
    maps = dense_weight.shape[0] * dense_weight.shape[1]
    tile = 2048 if slot_total <= 512 else 128
    atoms = graph * ATOM_DEV
    feeds = dense_weight.shape[0] - 1
    chunks = 2 * len(chunks_of(rows // 2)[1])
    stages = mp.bit_length()
    extra = max(stages - 2, 1)
    half = rows // 2
    vmem = pltpu.VMEM
    pieces = trip // 128 if trip % 128 == 0 else 1
    lane = trip // pieces
    pad = -(-basis.shape[0] // 16) * 16
    hot_bytes = 2 * 2 * slot_total * triplets
    hots = [vmem((slot_total, triplets), bf16)] * 2 if hot_bytes <= 2 ** 24 else [None, None]
    reduce_bufs = [
        vmem((pieces, rows, lane), bf16), vmem((pieces, half, lane), bf16), vmem((pieces, extra, half, lane), bf16),
        vmem((pieces, extra, half, lane), bf16), vmem((pieces, rows, lane), bf16),
    ]
    dma = pltpu.SemaphoreType.DMA
    spec = pl.BlockSpec(memory_space=pltpu.VMEM)
    operands = [
        edge_state, down_weight, basis, basis_weight, up_weight,
        dense_weight.reshape((maps,) + dense_weight.shape[2:]),
        send_rows, trip_in.reshape(1, triplets), trip_out.reshape(1, triplets),
        trip_live.reshape(1, triplets), edge_atom.reshape(1, rows),
    ]
    inputs = [vmem(a.shape, a.dtype) for i, a in enumerate(operands) if i not in (0, 4, 5)]
    parts = width // 128 if width % 128 == 0 else 1
    atom_buf = (parts, atoms, width // parts)
    body = functools.partial(kernel, graph, mp, tile)
    before = [
        *inputs, dma((len(inputs) + 2,)),
        vmem((mp, rows, width), bf16), vmem((mp, trip, width), bf16), dma((2,)), dma((2, 2)), dma(()), dma((2,)),
        vmem((dense_weight.shape[0] + 1,) + dense_weight.shape[2:], bf16),
        vmem((feeds, dense_weight.shape[2], 2 * width), bf16), dma((2,)), dma((feeds,)), dma((feeds, 2)), dma((feeds, 2, 2)),
        dma((chunks,)), dma((chunks,)),
        *reduce_bufs, *reduce_bufs,
        dma((2, stages)), dma((2, pieces, stages)),
        *[vmem((pieces, slot_total, lane), bf16)] * 4,
        dma((2,)), dma((2 * max(pieces, parts),)),
        vmem((rows, slot_total), bf16), vmem((3 * pad, triplets), bf16), vmem((3 * pad, trip), bf16),
        vmem((trip, triplets), f32), vmem((slot_total, lane), f32),
    ]
    if hots[0] is None:
        hots, kept_body, at = [], body, len(operands) + 2 + len(before)
        body = lambda *refs: kept_body(*refs[:at], None, None, *refs[at:])
    outs = pl.pallas_call(
        body,
        out_shape=(
            pltpu.VMEM((rows, width), bf16),
            pltpu.VMEM((ATOM_DEV, width), bf16),
        ),
        in_specs=[pl.BlockSpec(memory_space=pl.ANY)] * len(operands),
        out_specs=(spec, spec),
        scratch_shapes=[
            *before, *hots,
            vmem((maps - 1, mp, rows, width), bf16), vmem((mp, rows, width), f32), vmem((rows, width), f32),
            dma((2, chunks)), dma((2, chunks, 2)),
            vmem(atom_buf, f32), vmem(atom_buf, bf16), vmem(atom_buf, bf16), vmem(atom_buf, bf16),
        ],
        compiler_params=pltpu.CompilerParams(
            collective_id=0, has_side_effects=True, vmem_limit_bytes=64000 * 1024
        ),
        name="edge_block",
    )(*operands)
    outs = [pltpu.with_memory_space_constraint(o, pltpu.VMEM) for o in outs]
    return pl.pallas_call(
        hand_on,
        out_shape=tuple(jax.ShapeDtypeStruct(o.shape, o.dtype) for o in outs),
        in_specs=[spec] * 2,
        out_specs=[pl.BlockSpec(memory_space=pl.ANY)] * 2,
        scratch_shapes=[dma((2,))],
        name="hand_on",
    )(*outs)


def solution(mesh):
    in_specs = (
        P("graph", "mp"),
        P("mp", None),
        P(None, ("graph", "mp")),
        P(),
        P(None, "mp"),
        P(None, None, None, "mp"),
        P("graph", "mp", None),
        P(("graph", "mp")),
        P(("graph", "mp")),
        P(("graph", "mp")),
        P("graph"),
    )
    out_specs = (P("graph", "mp"), P("graph", "mp"))
    body = functools.partial(local, mesh.shape["graph"], mesh.shape["mp"])
    return jax.shard_map(body, mesh=mesh, in_specs=in_specs, out_specs=out_specs, check_vma=False)
```
